128 devices in a mesh: rep: 2 (over core), dp: 64 (over x, y, z).
Axes of the slice: x: 4, y: 4, z: 4, core: 2. Of those that a mesh axis runs over, the one named last changes fastest.
Arguments:
- x: bfloat16 [128, 2048, 1024], P(('rep', 'dp')), parts along dimension 0
- dy: bfloat16 [128, 2048, 1024], P(('rep', 'dp')), parts along dimension 0
- w_gate: bfloat16 [2, 1024, 2816], P(None, 'dp')
- w_up: bfloat16 [2, 1024, 2816], P(None, 'dp')
- w_down: bfloat16 [2, 2816, 1024], P(None, 'dp')
Outputs:
- output 1: bfloat16 [128, 2048, 1024], P(('rep', 'dp')), parts along dimension 0
- output 2: bfloat16 [4, 1024, 2816], P('rep', 'dp'), parts along dimension 0
- output 3: bfloat16 [4, 1024, 2816], P('rep', 'dp'), parts along dimension 0
- output 4: bfloat16 [4, 2816, 1024], P('rep', 'dp'), parts along dimension 0
There are 2 independent parts. The reference program is written for one: setup_inputs(seed, part) draws one part's arguments, and reference() takes and returns one part's arrays. A program takes and returns all parts, laid end to end along the dimension named above; an argument that names none is the same for every part.
All inputs are finite; a program needn't handle non-finite values.
Results may differ from the reference program's by a relative error of at most 0.018.
Values are sent between devices in bfloat16 or wider.
A program may use at most 1.5 GiB of HBM per device.

```python
import jax
import jax.numpy as jnp
from jax import lax

SEQUENCES = 64
TOKENS = 2048
D = 1024
FF = 2816
LAYERS = 2
NAMES = ("w_gate", "w_up", "w_down")
SHAPES = {"w_gate": (LAYERS, D, FF), "w_up": (LAYERS, D, FF), "w_down": (LAYERS, FF, D)}


def bump(key, n, height):
    away = (jnp.arange(n, dtype=jnp.int32) - jax.random.randint(key, (), 0, n, jnp.int32)) % n
    return jnp.where(away < n // 8, height, 1.0)


def together(key, own, strength):
    shared = jax.random.normal(key, own.shape[1:], jnp.float32)
    return (own + strength * shared) * lax.rsqrt(1 + strength * strength)


def setup_inputs(seed: int = 0, part: int = 0) -> dict:
    kx, kdy, ka, kb, kz, kf, kh, kl, *kw = jax.random.split(jax.random.key(seed), 8 + len(NAMES))
    kx, kdy, ka, kb = (jax.random.fold_in(k, part) for k in (kx, kdy, ka, kb))
    shape = (SEQUENCES, TOKENS, D)
    much_x, much_dy = jax.random.uniform(kz, (2,), jnp.float32, 0.0, 1.0)
    layers = 2.0 ** jax.random.uniform(kl, (LAYERS, 1, 1), jnp.float32, -1.0, 1.0)
    x = together(ka, jax.random.normal(kx, shape, jnp.float32), much_x) * bump(kf, D, 4.0)
    dy = together(kb, jax.random.normal(kdy, shape, jnp.float32), much_dy)
    drawn = {"x": x.astype(jnp.bfloat16), "dy": (dy * (SEQUENCES * TOKENS) ** -0.5).astype(jnp.bfloat16)}
    for key, name in zip(kw, NAMES, strict=True):
        w = jax.random.normal(key, SHAPES[name], jnp.float32) * SHAPES[name][1] ** -0.5
        drawn[name] = (w * {"w_gate": 1.0, "w_up": bump(kh, FF, 4.0), "w_down": layers}[name]).astype(jnp.bfloat16)
    return drawn


def matmul(a, w):
    return jnp.dot(a, w, preferred_element_type=jnp.float32).astype(jnp.bfloat16)


def normed(h):
    wide = h.astype(jnp.float32)
    scale = lax.rsqrt(jnp.mean(wide**2, -1, keepdims=True) + 1e-6)
    return (wide * scale).astype(jnp.bfloat16)


def layer(h, w):
    a = normed(h)
    gate = jnp.dot(a, w["w_gate"], preferred_element_type=jnp.float32)
    up = jnp.dot(a, w["w_up"], preferred_element_type=jnp.float32)
    return h + matmul((jax.nn.silu(gate) * up).astype(jnp.bfloat16), w["w_down"])


def stack(weights, h):
    return lax.scan(lambda h, w: (layer(h, w), None), h, weights)[0]


def reference(x, dy, w_gate, w_up, w_down):
    weights = dict(zip(NAMES, (w_gate, w_up, w_down), strict=True))

    def take(so_far, sequence):
        h, by_y = sequence
        _, back = jax.vjp(stack, weights, h)
        by_weights, by_h = back(by_y)
        return jax.tree.map(lambda total, term: total + term.astype(jnp.float32), so_far, by_weights), by_h

    none_yet = {name: jnp.zeros(w.shape, jnp.float32) for name, w in weights.items()}
    by_weights, by_x = lax.scan(take, none_yet, (x, dy))
    return (by_x, *(by_weights[name].astype(jnp.bfloat16) for name in NAMES))
```

```python
import functools
import jax, jax.numpy as jnp
from jax import lax
from jax.experimental import pallas as pl
from jax.experimental.pallas import tpu as pltpu
from jax.sharding import PartitionSpec as P
bf=jnp.bfloat16
MESH=pl.DeviceIdType.MESH
PERM=((0,1,2),(1,2,0),(2,0,1))

def coords():
    i=lax.axis_index("dp")
    return [i//16,(i//4)%4,i%4]

def shifted(me,axis,d):
    c=list(me); c[axis]=(c[axis]+d)%4
    return {"dp":c[0]*16+c[1]*4+c[2]}

def peers(me,far=True):
    return [shifted(me,a,d) for a in range(3) for d in ((1,3,2) if far else (1,3))]

def barrier(me,far=True,sib=True):
    b=pltpu.get_barrier_semaphore()
    n=0
    for t in peers(me,far):
        pl.semaphore_signal(b,inc=1,device_id=t,device_id_type=MESH); n+=1
    if sib:
        pl.semaphore_signal(b,inc=1,device_id={"rep":1-lax.axis_index("rep")},device_id_type=MESH); n+=1
    pl.semaphore_wait(b,n)

class Gather:
    NSEM=15
    def __init__(self,me,own,out,ssem,rsem,lsem,cols):
        self.me,self.own,self.out,self.ssem,self.rsem,self.lsem,self.cols=me,own,out,ssem,rsem,lsem,cols
        self.r=lax.axis_index("rep"); self.sib={"rep":1-self.r}
    def at(self,p,r,u,v,w):
        i=[None]*3
        for a,k in zip(PERM[p],(u,v,w)): i[a]=k
        return self.out.at[(r,*i,slice(None),pl.ds(*self.cols[p]))]
    def copy(self,p,k,src,dst,dev):
        return pltpu.make_async_remote_copy(src_ref=src,dst_ref=dst,send_sem=self.ssem.at[p,k],recv_sem=self.rsem.at[p,k],device_id=dev,device_id_type=MESH)
    def m(self,p,k): return self.me[PERM[p][k]]
    def sent(self,p,k):
        r=self.r; u,v,w=(self.m(p,j) for j in range(3)); A=slice(None); lo,hi=pl.ds(0,2),pl.ds(2,2)
        ax=PERM[p]
        me=self.me
        if k<3:
            src=self.own.at[r,:,pl.ds(*self.cols[p])]; dst=self.at(p,r,u,v,w)
            return src,dst,shifted(me,ax[0],(1,3,2)[k])
        if k<5:
            ref=self.at(p,r,A,v,w); return ref,ref,shifted(me,ax[1],(1,3)[k-3])
        if k==5: ref=self.at(p,r,lo,(v+3)%4,w); return ref,ref,shifted(me,ax[1],1)
        if k==6: ref=self.at(p,r,hi,(v+1)%4,w); return ref,ref,shifted(me,ax[1],3)
        if k<9:
            ref=self.at(p,r,A,A,w); return ref,ref,shifted(me,ax[2],(1,3)[k-7])
        if k==9: ref=self.at(p,r,lo,A,(w+3)%4); return ref,ref,shifted(me,ax[2],1)
        if k==10: ref=self.at(p,r,hi,A,(w+1)%4); return ref,ref,shifted(me,ax[2],3)
        ref=self.at(p,r,A,A,(w+(0,3,1,2)[k-11])%4); return ref,ref,self.sib
    def received(self,p,k):
        r=self.r; u,v,w=(self.m(p,j) for j in range(3)); A=slice(None); lo,hi=pl.ds(0,2),pl.ds(2,2)
        if k<3: return self.at(p,r,(u+(3,1,2)[k])%4,v,w)
        if k<5: return self.at(p,r,A,(v+(3,1)[k-3])%4,w)
        if k==5: return self.at(p,r,lo,(v+2)%4,w)
        if k==6: return self.at(p,r,hi,(v+2)%4,w)
        if k<9: return self.at(p,r,A,A,(w+(3,1)[k-7])%4)
        if k==9: return self.at(p,r,lo,A,(w+2)%4)
        if k==10: return self.at(p,r,hi,A,(w+2)%4)
        return self.at(p,1-r,A,A,(w+(0,3,1,2)[k-11])%4)
    def start(self,p,k):
        s,d,dev=self.sent(p,k); self.copy(p,k,s,d,dev).start()
    def wait_send(self,p,k):
        s,d,dev=self.sent(p,k); self.copy(p,k,s,d,dev).wait_send()
    def wait_recv(self,p,k):
        ref=self.received(p,k); self.copy(p,k,ref,ref,self.sib).wait_recv()
    def local(self,p):
        return pltpu.make_async_copy(self.own.at[self.r,:,pl.ds(*self.cols[p])],self.at(p,self.r,*(self.m(p,j) for j in range(3))),self.lsem.at[p])
    def events(self):
        P3=range(3)
        def e0():
            for p in P3:
                self.local(p).start()
                for k in (0,1,2): self.start(p,k)
        def e1():
            for p in P3:
                self.local(p).wait()
                for k in (0,1,2): self.wait_recv(p,k)
                for k in (3,4): self.start(p,k)
        def e2():
            for p in P3:
                for k in (3,4): self.wait_recv(p,k); self.start(p,k+2)
        def e3():
            for p in P3:
                for k in (5,6): self.wait_recv(p,k)
                for k in (7,8,11): self.start(p,k)
        def e4():
            for p in P3:
                for k in (7,8): self.wait_recv(p,k); self.start(p,k+2); self.start(p,k+5)
        def e5():
            for p in P3:
                for k in (9,10): self.wait_recv(p,k)
                self.start(p,14)
        def e6():
            for p in P3:
                for k in range(15): self.wait_send(p,k)
                for k in range(11,15): self.wait_recv(p,k)
        return [e0,e1,e2,e3,e4,e5,e6]

f32=jnp.float32

class Scatter:
    N1,N2,N3=6,6,3
    NSEM=15
    @staticmethod
    def scratch(R,cols):
        s=[]
        for p in range(3):
            n=cols[p][1]
            h=Scatter.half_shape(p)
            s+=[pltpu.VMEM((6,*h,R,n),bf),
                pltpu.VMEM((4,*h,R,n),bf),
                pltpu.VMEM((4,4,R,n),f32),pltpu.VMEM((4,4,R,n),bf),
                pltpu.VMEM((6,2,R,n),bf),pltpu.VMEM((2,2,R,n),bf),
                pltpu.VMEM((4,R,n),f32),pltpu.VMEM((4,R,n),bf),
                pltpu.VMEM((3,R,n),bf)]
        return s+[pltpu.VMEM((R,sum(c[1] for c in cols)),bf),pltpu.SemaphoreType.DMA((3,15)),pltpu.SemaphoreType.DMA((3,15)),pltpu.SemaphoreType.DMA((3,4)),pltpu.SemaphoreType.DMA(())]
    @staticmethod
    def half_shape(p):
        _,v,w=PERM[p]
        return (2,4) if v<w else (4,2)
    def __init__(self,me,g,out,bufs,cols):
        self.me,self.g,self.out,self.cols=me,g,out,cols
        self.b=[bufs[9*p:9*p+9] for p in range(3)]
        self.res,self.ssem,self.rsem,self.lsem,self.osem=bufs[27:]
    def m(self,p,k,d=0): return (self.me[PERM[p][k]]+d)%4
    def gat(self,p,u,half):
        i=[None]*3
        _,v,w=PERM[p]
        i[PERM[p][0]]=u; i[v]=pl.ds(2*half,2); i[w]=slice(None)
        return self.g.at[(*i,slice(None),pl.ds(*self.cols[p]))]
    def hidx(self,p,v,w):
        _,a,b=PERM[p]
        return (v,w) if a<b else (w,v)
    def own(self,p,j):
        u,h=((1,0),(3,1),(0,0),(0,1))[j]
        return pltpu.make_async_copy(self.gat(p,self.m(p,0,u),h),self.b[p][1].at[j],self.lsem.at[p,j])
    def rc(self,p,k,src,dst,ax,d):
        return pltpu.make_async_remote_copy(src_ref=src,dst_ref=dst,send_sem=self.ssem.at[p,k],recv_sem=self.rsem.at[p,k],device_id=shifted(self.me,PERM[p][ax],d),device_id_type=MESH)
    def cp(self,p,k):
        b=self.b[p]
        if k<6:
            d=(1,3,1,3,1,3)[k]
            if k<4:
                u,h=((2,0),(2,1),(1,1),(3,0))[k]
                src=self.gat(p,self.m(p,0,u),h)
            else: src=b[1].at[k-4]
            return self.rc(p,k,src,b[0].at[k],0,d)
        if k<12:
            j=k-6; d=(1,3,1,3,1,3)[j]
            if j<4:
                v,h=((2,0),(2,1),(1,1),(3,0))[j]
                src=b[3].at[self.m(p,1,v),pl.ds(2*h,2)]
            else: src=b[5].at[j-4]
            return self.rc(p,k,src,b[4].at[j],1,d)
        j=k-12; d=(1,3,2)[j]
        return self.rc(p,k,b[7].at[self.m(p,2,d)],b[8].at[j],2,d)
    def events(self):
        P3=range(3)
        def e0():
            for k in (0,1,2,3):
                for p in P3: self.cp(p,k).start()
            for p in P3:
                for j in range(4): self.own(p,j).start()
        def e1():
            for p in P3:
                b=self.b[p]; h=self.half_shape(p)
                for k in (0,1):
                    self.own(p,k).wait(); self.cp(p,k).wait_recv()
                    def add(i,_,b=b,h=h,k=k):
                        ix=(k,i//h[1],i%h[1])
                        b[1][ix]=(b[0][ix].astype(f32)+b[1][ix].astype(f32)).astype(bf)
                        return 0
                    lax.fori_loop(0,8,add,0)
            for p in P3:
                for k in (4,5): self.cp(p,k).start()
        def e2():
            for p in P3:
                b=self.b[p]
                for k in (2,3,4,5): self.cp(p,k).wait_recv()
                for j in (2,3): self.own(p,j).wait()
                for hf in (0,1):
                    own,sm,raw=((2,4,3),(3,5,2))[hf]
                    def add(i,_,b=b,hf=hf,own=own,sm=sm,raw=raw,p=p):
                        v,w=i//4,i%4
                        ix=self.hidx(p,v,w)
                        t=b[1][(own,*ix)].astype(f32)+b[0][(sm,*ix)].astype(f32)+b[0][(raw,*ix)].astype(f32)
                        b[2][2*hf+v,w]=t; b[3][2*hf+v,w]=t.astype(bf)
                        return 0
                    lax.fori_loop(0,8,add,0)
        def e3():
            for k in (6,7,8,9):
                for p in P3: self.cp(p,k).start()
        def e4():
            for p in P3:
                b=self.b[p]
                for hf in (0,1):
                    self.cp(p,6+hf).wait_recv()
                    v=self.m(p,1,(1,3)[hf])
                    for w in (0,1):
                        b[5][hf,w]=(b[4][hf,w].astype(f32)+b[2][v,2*hf+w]).astype(bf)
            for p in P3:
                for k in (10,11): self.cp(p,k).start()
        def e5():
            for p in P3:
                b=self.b[p]; v=self.m(p,1)
                for k in (8,9,10,11): self.cp(p,k).wait_recv()
                for hf in (0,1):
                    sm,raw=((4,3),(5,2))[hf]
                    for w in (0,1):
                        t=b[2][v,2*hf+w]+b[4][sm,w].astype(f32)+b[4][raw,w].astype(f32)
                        b[6][2*hf+w]=t; b[7][2*hf+w]=t.astype(bf)
        def e6():
            for k in (12,13,14):
                for p in P3: self.cp(p,k).start()
        def e7():
            for p in P3:
                b=self.b[p]; w=self.m(p,2)
                for k in (12,13,14): self.cp(p,k).wait_recv()
                t=b[6][w]
                for j in range(3): t=t+b[8][j].astype(f32)
                self.res[:,pl.ds(*self.cols[p])]=t.astype(bf)
            pltpu.make_async_copy(self.res,self.out,self.osem).start()
            for p in P3:
                for k in range(15): self.cp(p,k).wait_send()
            pltpu.make_async_copy(self.res,self.out,self.osem).wait()
        return [e0,e1,e2,e3,e4,e5,e6,e7]

NAMES = ("w_gate", "w_up", "w_down")
GU_COLS = ((0, 1024), (1024, 896), (1920, 896))
D_COLS = ((0, 384), (384, 384), (768, 256))


def gather_call(pair, cols, number):
    rows, width = pair.shape[1:]

    def kernel(own, out, *sems):
        me = coords()
        barrier(me)
        for event in Gather(me, own, out, *sems, cols).events():
            event()

    return pl.pallas_call(
        kernel,
        in_specs=[pl.BlockSpec(memory_space=pltpu.VMEM)],
        out_specs=pl.BlockSpec(memory_space=pltpu.HBM),
        out_shape=jax.ShapeDtypeStruct((2, 4, 4, 4, rows, width), bf),
        scratch_shapes=[pltpu.SemaphoreType.DMA((3, 15)), pltpu.SemaphoreType.DMA((3, 15)), pltpu.SemaphoreType.DMA((3,))],
        compiler_params=pltpu.CompilerParams(collective_id=number, has_side_effects=True),
        name=f"gather_{number}",
    )(pair)


def scatter_call(g, cols, number):
    rows, width = g.shape[3:]

    def kernel(g, out, *bufs):
        me = coords()
        barrier(me, sib=False)
        for event in Scatter(me, g, out, bufs, cols).events():
            event()

    return pl.pallas_call(
        kernel,
        in_specs=[pl.BlockSpec(memory_space=pltpu.HBM)],
        out_specs=pl.BlockSpec(memory_space=pltpu.HBM),
        out_shape=jax.ShapeDtypeStruct((rows, width), bf),
        scratch_shapes=Scatter.scratch(rows, cols),
        compiler_params=pltpu.CompilerParams(collective_id=number, has_side_effects=True, vmem_limit_bytes=60 * 2**20),
        name=f"scatter_{number}",
    )(g)


def matmul(a, w):
    return jnp.dot(a, w, preferred_element_type=f32).astype(bf)


def normed(h):
    wide = h.astype(f32)
    scale = lax.rsqrt(jnp.mean(wide**2, -1, keepdims=True) + 1e-6)
    return (wide * scale).astype(bf)


def layer(h, w):
    a = normed(h)
    gate = jnp.dot(a, w["w_gate"], preferred_element_type=f32)
    up = jnp.dot(a, w["w_up"], preferred_element_type=f32)
    return h + matmul((jax.nn.silu(gate) * up).astype(bf), w["w_down"])


def stack(weights, h):
    for w in weights:
        h = layer(h, w)
    return h


def solution(mesh):
    def device(x, dy, w_gate, w_up, w_down):
        gu = [gather_call(jnp.stack([w_gate[n], w_up[n]]), GU_COLS, n).reshape(2, 1024, 2816) for n in (0, 1)]
        dd = gather_call(w_down, D_COLS, 2).reshape(2, 2816, 1024)
        weights = [dict(zip(NAMES, (*gu[n], dd[n]), strict=True)) for n in (0, 1)]
        _, back = jax.vjp(stack, weights, x[0])
        by_weights, by_x = back(dy[0])
        outs = []
        for j, name in enumerate(NAMES):
            rows, cols = (44, D_COLS) if name == "w_down" else (16, GU_COLS)
            both = [scatter_call(by_weights[n][name].reshape(4, 4, 4, rows, -1), cols, 3 + 2 * j + n) for n in (0, 1)]
            outs.append(jnp.stack(both))
        return (by_x[None], *outs)

    return jax.shard_map(
        device,
        mesh=mesh,
        in_specs=(P(("rep", "dp")), P(("rep", "dp")), *(P(None, "dp"),) * 3),
        out_specs=(P(("rep", "dp")), *(P("rep", "dp"),) * 3),
        check_vma=False,
    )
```

```python
import functools
import jax, jax.numpy as jnp
from jax import lax
from jax.experimental import pallas as pl
from jax.experimental.pallas import tpu as pltpu
from jax.sharding import PartitionSpec as P
bf=jnp.bfloat16
MESH=pl.DeviceIdType.MESH
PERM=((0,1,2),(1,2,0),(2,0,1))

def coords():
    i=lax.axis_index("dp")
    return [i//16,(i//4)%4,i%4]

def shifted(me,axis,d):
    c=list(me); c[axis]=(c[axis]+d)%4
    return {"dp":c[0]*16+c[1]*4+c[2]}

def peers(me,far=True):
    return [shifted(me,a,d) for a in range(3) for d in ((1,3,2) if far else (1,3))]

def barrier(me,far=True,sib=True):
    b=pltpu.get_barrier_semaphore()
    n=0
    for t in peers(me,far):
        pl.semaphore_signal(b,inc=1,device_id=t,device_id_type=MESH); n+=1
    if sib:
        pl.semaphore_signal(b,inc=1,device_id={"rep":1-lax.axis_index("rep")},device_id_type=MESH); n+=1
    pl.semaphore_wait(b,n)

class Gather:
    NSEM=15
    def __init__(self,me,own,out,ssem,rsem,lsem,cols):
        self.me,self.own,self.out,self.ssem,self.rsem,self.lsem,self.cols=me,own,out,ssem,rsem,lsem,cols
        self.r=lax.axis_index("rep"); self.sib={"rep":1-self.r}
    def at(self,p,r,u,v,w):
        i=[None]*3
        for a,k in zip(PERM[p],(u,v,w)): i[a]=k
        return self.out.at[(r,*i,slice(None),pl.ds(*self.cols[p]))]
    def copy(self,p,k,src,dst,dev):
        return pltpu.make_async_remote_copy(src_ref=src,dst_ref=dst,send_sem=self.ssem.at[p,k],recv_sem=self.rsem.at[p,k],device_id=dev,device_id_type=MESH)
    def m(self,p,k): return self.me[PERM[p][k]]
    def sent(self,p,k):
        r=self.r; u,v,w=(self.m(p,j) for j in range(3)); A=slice(None); lo,hi=pl.ds(0,2),pl.ds(2,2)
        ax=PERM[p]
        me=self.me
        if k<3:
            src=self.own.at[r,:,pl.ds(*self.cols[p])]; dst=self.at(p,r,u,v,w)
            return src,dst,shifted(me,ax[0],(1,3,2)[k])
        if k<5:
            ref=self.at(p,r,A,v,w); return ref,ref,shifted(me,ax[1],(1,3)[k-3])
        if k==5: ref=self.at(p,r,lo,(v+3)%4,w); return ref,ref,shifted(me,ax[1],1)
        if k==6: ref=self.at(p,r,hi,(v+1)%4,w); return ref,ref,shifted(me,ax[1],3)
        if k<9:
            ref=self.at(p,r,A,A,w); return ref,ref,shifted(me,ax[2],(1,3)[k-7])
        if k==9: ref=self.at(p,r,lo,A,(w+3)%4); return ref,ref,shifted(me,ax[2],1)
        if k==10: ref=self.at(p,r,hi,A,(w+1)%4); return ref,ref,shifted(me,ax[2],3)
        ref=self.at(p,r,A,A,(w+(0,3,1,2)[k-11])%4); return ref,ref,self.sib
    def received(self,p,k):
        r=self.r; u,v,w=(self.m(p,j) for j in range(3)); A=slice(None); lo,hi=pl.ds(0,2),pl.ds(2,2)
        if k<3: return self.at(p,r,(u+(3,1,2)[k])%4,v,w)
        if k<5: return self.at(p,r,A,(v+(3,1)[k-3])%4,w)
        if k==5: return self.at(p,r,lo,(v+2)%4,w)
        if k==6: return self.at(p,r,hi,(v+2)%4,w)
        if k<9: return self.at(p,r,A,A,(w+(3,1)[k-7])%4)
        if k==9: return self.at(p,r,lo,A,(w+2)%4)
        if k==10: return self.at(p,r,hi,A,(w+2)%4)
        return self.at(p,1-r,A,A,(w+(0,3,1,2)[k-11])%4)
    def start(self,p,k):
        s,d,dev=self.sent(p,k); self.copy(p,k,s,d,dev).start()
    def wait_send(self,p,k):
        s,d,dev=self.sent(p,k); self.copy(p,k,s,d,dev).wait_send()
    def wait_recv(self,p,k):
        ref=self.received(p,k); self.copy(p,k,ref,ref,self.sib).wait_recv()
    def local(self,p):
        return pltpu.make_async_copy(self.own.at[self.r,:,pl.ds(*self.cols[p])],self.at(p,self.r,*(self.m(p,j) for j in range(3))),self.lsem.at[p])
    def events(self):
        P3=range(3)
        def e0():
            for p in P3:
                self.local(p).start()
                for k in (0,1,2): self.start(p,k)
        def e1():
            for p in P3:
                self.local(p).wait()
                for k in (0,1,2): self.wait_recv(p,k)
                for k in (3,4): self.start(p,k)
        def e2():
            for p in P3:
                for k in (3,4): self.wait_recv(p,k); self.start(p,k+2)
        def e3():
            for p in P3:
                for k in (5,6): self.wait_recv(p,k)
                for k in (7,8,11): self.start(p,k)
        def e4():
            for p in P3:
                for k in (7,8): self.wait_recv(p,k); self.start(p,k+2); self.start(p,k+5)
        def e5():
            for p in P3:
                for k in (9,10): self.wait_recv(p,k)
                self.start(p,14)
        def e6():
            for p in P3:
                for k in range(11,15): self.wait_recv(p,k)
        return [e0,e1,e2,e3,e4,e5,e6]
    def finish(self):
        for p in range(3):
            for k in range(15): self.wait_send(p,k)

f32=jnp.float32

class Scatter:
    N1,N2,N3=6,6,3
    NSEM=15
    @staticmethod
    def scratch(R,cols):
        s=[]
        for p in range(3):
            n=cols[p][1]
            h=Scatter.half_shape(p)
            s+=[pltpu.VMEM((6,*h,R,n),bf),
                pltpu.VMEM((4,*h,R,n),bf),
                pltpu.VMEM((4,4,R,n),f32),pltpu.VMEM((4,4,R,n),bf),
                pltpu.VMEM((6,2,R,n),bf),pltpu.VMEM((2,2,R,n),bf),
                pltpu.VMEM((4,R,n),f32),pltpu.VMEM((4,R,n),bf),
                pltpu.VMEM((3,R,n),bf)]
        return s+[pltpu.VMEM((R,sum(c[1] for c in cols)),bf),pltpu.SemaphoreType.DMA((3,15)),pltpu.SemaphoreType.DMA((3,15)),pltpu.SemaphoreType.DMA((3,4)),pltpu.SemaphoreType.DMA(())]
    @staticmethod
    def half_shape(p):
        _,v,w=PERM[p]
        return (2,4) if v<w else (4,2)
    def __init__(self,me,g,out,bufs,cols):
        self.me,self.g,self.out,self.cols=me,g,out,cols
        self.b=[bufs[9*p:9*p+9] for p in range(3)]
        self.res,self.ssem,self.rsem,self.lsem,self.osem=bufs[27:]
    def m(self,p,k,d=0): return (self.me[PERM[p][k]]+d)%4
    def gat(self,p,u,half):
        i=[None]*3
        _,v,w=PERM[p]
        i[PERM[p][0]]=u; i[v]=pl.ds(2*half,2); i[w]=slice(None)
        return self.g.at[(*i,slice(None),pl.ds(*self.cols[p]))]
    def hidx(self,p,v,w):
        _,a,b=PERM[p]
        return (v,w) if a<b else (w,v)
    def own(self,p,j):
        u,h=((1,0),(3,1),(0,0),(0,1))[j]
        return pltpu.make_async_copy(self.gat(p,self.m(p,0,u),h),self.b[p][1].at[j],self.lsem.at[p,j])
    def rc(self,p,k,src,dst,ax,d):
        return pltpu.make_async_remote_copy(src_ref=src,dst_ref=dst,send_sem=self.ssem.at[p,k],recv_sem=self.rsem.at[p,k],device_id=shifted(self.me,PERM[p][ax],d),device_id_type=MESH)
    def cp(self,p,k):
        b=self.b[p]
        if k<6:
            d=(1,3,1,3,1,3)[k]
            if k<4:
                u,h=((2,0),(2,1),(1,1),(3,0))[k]
                src=self.gat(p,self.m(p,0,u),h)
            else: src=b[1].at[k-4]
            return self.rc(p,k,src,b[0].at[k],0,d)
        if k<12:
            j=k-6; d=(1,3,1,3,1,3)[j]
            if j<4:
                v,h=((2,0),(2,1),(1,1),(3,0))[j]
                src=b[3].at[self.m(p,1,v),pl.ds(2*h,2)]
            else: src=b[5].at[j-4]
            return self.rc(p,k,src,b[4].at[j],1,d)
        j=k-12; d=(1,3,2)[j]
        return self.rc(p,k,b[7].at[self.m(p,2,d)],b[8].at[j],2,d)
    def events(self):
        P3=range(3)
        def e0():
            for k in (0,1,2,3):
                for p in P3: self.cp(p,k).start()
            for p in P3:
                for j in range(4): self.own(p,j).start()
        def e1():
            for p in P3:
                b=self.b[p]; h=self.half_shape(p)
                for k in (0,1):
                    self.own(p,k).wait(); self.cp(p,k).wait_recv()
                    def add(i,_,b=b,h=h,k=k):
                        ix=(k,i//h[1],i%h[1])
                        b[1][ix]=(b[0][ix].astype(f32)+b[1][ix].astype(f32)).astype(bf)
                        return 0
                    lax.fori_loop(0,8,add,0)
            for p in P3:
                for k in (4,5): self.cp(p,k).start()
        def e2():
            for p in P3:
                b=self.b[p]
                for k in (2,3,4,5): self.cp(p,k).wait_recv()
                for j in (2,3): self.own(p,j).wait()
                for hf in (0,1):
                    own,sm,raw=((2,4,3),(3,5,2))[hf]
                    def add(i,_,b=b,hf=hf,own=own,sm=sm,raw=raw,p=p):
                        v,w=i//4,i%4
                        ix=self.hidx(p,v,w)
                        t=b[1][(own,*ix)].astype(f32)+b[0][(sm,*ix)].astype(f32)+b[0][(raw,*ix)].astype(f32)
                        b[2][2*hf+v,w]=t; b[3][2*hf+v,w]=t.astype(bf)
                        return 0
                    lax.fori_loop(0,8,add,0)
        def e3():
            for k in (6,7,8,9):
                for p in P3: self.cp(p,k).start()
        def e4():
            for p in P3:
                b=self.b[p]
                for hf in (0,1):
                    self.cp(p,6+hf).wait_recv()
                    v=self.m(p,1,(1,3)[hf])
                    for w in (0,1):
                        b[5][hf,w]=(b[4][hf,w].astype(f32)+b[2][v,2*hf+w]).astype(bf)
            for p in P3:
                for k in (10,11): self.cp(p,k).start()
        def e5():
            for p in P3:
                b=self.b[p]; v=self.m(p,1)
                for k in (8,9,10,11): self.cp(p,k).wait_recv()
                for hf in (0,1):
                    sm,raw=((4,3),(5,2))[hf]
                    for w in (0,1):
                        t=b[2][v,2*hf+w]+b[4][sm,w].astype(f32)+b[4][raw,w].astype(f32)
                        b[6][2*hf+w]=t; b[7][2*hf+w]=t.astype(bf)
        def e6():
            for k in (12,13,14):
                for p in P3: self.cp(p,k).start()
        def e7():
            for p in P3:
                b=self.b[p]; w=self.m(p,2)
                for k in (12,13,14): self.cp(p,k).wait_recv()
                t=b[6][w]
                for j in range(3): t=t+b[8][j].astype(f32)
                self.res[:,pl.ds(*self.cols[p])]=t.astype(bf)
            pltpu.make_async_copy(self.res,self.out,self.osem).start()
            for p in P3:
                for k in range(15): self.cp(p,k).wait_send()
            pltpu.make_async_copy(self.res,self.out,self.osem).wait()
        return [e0,e1,e2,e3,e4,e5,e6,e7]

T, D, FF = 2048, 1024, 2816
F = 256
N_F = FF // F
M = 512
N_T = T // M
NT = (((1,), (1,)), ((), ()))
TN = (((0,), (0,)), ((), ()))
GU0 = (((0, 256), (256, 256), (512, 256)), ((768, 384), (1152, 384), (1536, 256)), ((1792, 384), (2176, 384), (2560, 256)))
DD = ((0, 384), (384, 384), (768, 256))
GU1 = (((0, 512), (512, 512), (1024, 384)), ((1408, 512), (1920, 512), (2432, 384)))
HBM = pl.BlockSpec(memory_space=pltpu.HBM)
VMEM = pl.BlockSpec(memory_space=pltpu.VMEM)


def dot(a, b, dims=None):
    if dims is None:
        return jnp.dot(a, b, preferred_element_type=f32)
    return lax.dot_general(a, b, dims, preferred_element_type=f32)


def norm_rows(h):
    wide = h.astype(f32)
    return (wide * lax.rsqrt(jnp.mean(wide * wide, -1, keepdims=True) + 1e-6)).astype(bf)


def run(events):
    for event in events:
        event()


def at_step(i, events):
    for step, functions in events.items():
        pl.when(i == step)(functools.partial(run, functions))


def tile(ref, f):
    return ref.at[:, pl.ds(pl.multiple_of(f * F, F), F)]


def forward_kernel(
    x_hbm, dy_hbm, own0, own_d, own1,
    gu0, dd, gu1, gate0, up0, act0, a0, h1, a1, act1, dgate1, dup1,
    x, a, big, wt, go, raw, wc, ho, dyt, eo,
    ssem, rsem, csem, xsem, wsem, gsem, bsem, rawsem, hsem, asem, dsem, esem,
):
    me = coords()
    barrier(me)

    def stream(k, own, out, cols):
        g = Gather(me, own, out, ssem.at[k], rsem.at[k], csem.at[k], cols)
        return g, g.events()

    (gA, A), (gB, B), (gC, C) = (stream(k, own0, gu0, cols) for k, cols in enumerate(GU0))
    gD, Dd = stream(3, own_d, dd, DD)
    (gE, E), (gG, G) = (stream(4 + k, own1, gu1, cols) for k, cols in enumerate(GU1))

    load_x = pltpu.make_async_copy(x_hbm, x, xsem.at[0])
    load_x.start()
    run([A[0], B[0]])
    load_x.wait()

    def norm0(t, _):
        rows = pl.ds(pl.multiple_of(t * M, M), M)
        a[rows, :] = norm_rows(x[rows, :])
        return 0

    lax.fori_loop(0, N_T, norm0, 0)
    keep_a0 = pltpu.make_async_copy(a, a0, xsem.at[1])
    keep_a0.start()
    run([A[1], B[1], C[0], A[2], B[2], A[3], C[1], A[4], B[3], C[2], A[5], A[6], B[4], C[3]])

    def load_w(w, f, slot):
        return pltpu.make_async_copy(w.at[:, :, :, :, :, pl.ds(pl.multiple_of(f * F, F), F)], wt.at[slot], wsem.at[slot])

    def put(f, slot):
        return (
            pltpu.make_async_copy(go.at[slot, 0], tile(gate0, f), gsem.at[slot, 0]),
            pltpu.make_async_copy(go.at[slot, 1], tile(up0, f), gsem.at[slot, 1]),
            pltpu.make_async_copy(tile(big, f), tile(act0, f), bsem.at[slot]),
        )

    def gate_up(f, events, w, finish):
        slot = lax.rem(f, 2)
        load_w(w, f, slot).wait()

        @pl.when(f + 1 < N_F)
        def _():
            load_w(w, f + 1, 1 - slot).start()

        finish(f, slot, [wt[slot, k].reshape(D, F) for k in (0, 1)])
        at_step(f, events)
        return 0

    def finish0(f, slot, w):
        @pl.when(f >= 2)
        def _():
            for copy in put(f - 2, slot):
                copy.wait()

        for t in range(N_T):
            rows = pl.ds(t * M, M)
            gate, up = dot(a[rows, :], w[0]), dot(a[rows, :], w[1])
            go[slot, 0, rows, :] = gate
            go[slot, 1, rows, :] = up
            tile(big, f)[rows, :] = (gate * jax.nn.sigmoid(gate) * up).astype(bf)
        for copy in put(f, slot):
            copy.start()

    ev = {
        0: [B[5]], 1: [B[6], C[4]], 2: [C[5], Dd[0]], 3: [Dd[1]], 4: [Dd[2]], 5: [C[6], Dd[3]],
        9: [Dd[4]], 10: [E[0], G[0]],
    }
    load_w(gu0, 0, 0).start()
    lax.fori_loop(0, N_F, lambda f, _: gate_up(f, ev, gu0, finish0), 0)
    run([Dd[5], E[1], Dd[6], G[1]])
    load_raw = [pltpu.make_async_copy(dd.at[k], raw, rawsem) for k in (0, 1)]
    load_raw[0].start()
    for f in (N_F - 2, N_F - 1):
        for copy in put(f, f % 2):
            copy.wait()
    keep_a0.wait()

    def convert():
        for i in range(64):
            wc[44 * i : 44 * i + 44, :] = raw[i // 16, i // 4 % 4, i % 4]

    load_raw[0].wait()
    convert()
    load_raw[1].start()

    def put_h(t, slot):
        return pltpu.make_async_copy(ho.at[slot], h1.at[pl.ds(pl.multiple_of(t * M, M), M)], hsem.at[slot])

    def load_dy(t, slot):
        return pltpu.make_async_copy(dy_hbm.at[pl.ds(pl.multiple_of(t * M, M), M)], dyt.at[slot], dsem.at[slot])

    def down(t, events):
        slot = lax.rem(t, 2)

        @pl.when(t >= 2)
        def _():
            put_h(t - 2, slot).wait()

        rows = pl.ds(pl.multiple_of(t * M, M), M)
        h = (x[rows, :].astype(f32) + dot(big[rows, :], wc[...]).astype(bf).astype(f32)).astype(bf)
        ho[slot] = h
        a[rows, :] = norm_rows(h)
        put_h(t, slot).start()
        at_step(t, events)
        return 0

    lax.fori_loop(0, N_T, lambda t, _: down(t, {0: [E[2]], 1: [G[2], E[3]]}), 0)
    keep_a1 = pltpu.make_async_copy(a, a1, asem)
    keep_a1.start()
    load_dy(0, 0).start()
    for t in (N_T - 2, N_T - 1):
        put_h(t, t % 2).wait()
    load_raw[1].wait()
    convert()

    def dact(t, events):
        slot = lax.rem(t, 2)
        load_dy(t, slot).wait()

        @pl.when(t + 1 < N_T)
        def _():
            load_dy(t + 1, 1 - slot).start()

        rows = pl.ds(pl.multiple_of(t * M, M), M)
        big[rows, :] = dot(dyt[slot], wc[...], NT).astype(bf)
        at_step(t, events)
        return 0

    lax.fori_loop(0, N_T, lambda t, _: dact(t, {0: [E[4], G[3]], 2: [E[5]], 3: [E[6], G[4]]}), 0)

    def put1(f, slot):
        return [pltpu.make_async_copy(eo.at[slot, k], tile(out, f), esem.at[slot, k]) for k, out in enumerate((act1, dgate1, dup1))]

    def finish1(f, slot, w):
        @pl.when(f >= 2)
        def _():
            for copy in put1(f - 2, slot):
                copy.wait()

        for t in range(N_T):
            rows = pl.ds(t * M, M)
            gate, up = dot(a[rows, :], w[0]), dot(a[rows, :], w[1])
            by_act = tile(big, f)[rows, :].astype(f32)
            sig = jax.nn.sigmoid(gate)
            silu = gate * sig
            eo[slot, 0, rows, :] = (silu * up).astype(bf)
            eo[slot, 1, rows, :] = (by_act * up * (sig + silu * (1 - sig))).astype(bf)
            eo[slot, 2, rows, :] = (by_act * silu).astype(bf)
        for copy in put1(f, slot):
            copy.start()

    load_w(gu1, 0, 0).start()
    lax.fori_loop(0, N_F, lambda f, _: gate_up(f, {1: [G[5]], 2: [G[6]]}, gu1, finish1), 0)
    for f in (N_F - 2, N_F - 1):
        for copy in put1(f, f % 2):
            copy.wait()
    keep_a1.wait()
    for g in (gA, gB, gC, gD, gE, gG):
        g.finish()


def forward(x, dy, own0, own_d, own1):
    sd = jax.ShapeDtypeStruct
    wide, wide32, narrow = sd((T, FF), bf), sd((T, FF), f32), sd((T, D), bf)
    dma = pltpu.SemaphoreType.DMA
    return pl.pallas_call(
        forward_kernel,
        in_specs=[HBM, HBM, VMEM, VMEM, VMEM],
        out_specs=[HBM] * 12,
        out_shape=[sd((2, 4, 4, 4, 16, FF), bf), sd((2, 4, 4, 4, 44, D), bf), sd((2, 4, 4, 4, 16, FF), bf),
                   wide32, wide32, wide, narrow, narrow, narrow, wide, wide, wide],
        scratch_shapes=[
            pltpu.VMEM((T, D), bf), pltpu.VMEM((T, D), bf), pltpu.VMEM((T, FF), bf),
            pltpu.VMEM((2, 2, 4, 4, 4, 16, F), bf), pltpu.VMEM((2, 2, T, F), f32),
            pltpu.VMEM((4, 4, 4, 44, D), bf), pltpu.VMEM((FF, D), bf), pltpu.VMEM((2, M, D), bf),
            pltpu.VMEM((2, M, D), bf), pltpu.VMEM((2, 3, T, F), bf),
            dma((6, 3, 15)), dma((6, 3, 15)), dma((6, 3)), dma((2,)), dma((2,)), dma((2, 2)), dma((2,)), dma(()), dma((2,)), dma(()), dma((2,)), dma((2, 3)),
        ],
        compiler_params=pltpu.CompilerParams(collective_id=0, has_side_effects=True, vmem_limit_bytes=63 * 2**20),
        name="forward",
    )(x, dy, own0, own_d, own1)


NAMES = ("w_gate", "w_up", "w_down")
GU_COLS = ((0, 1024), (1024, 896), (1920, 896))
D_COLS = ((0, 384), (384, 384), (768, 256))


def scatter_call(g, cols, number):
    rows, width = g.shape[3:]

    def kernel(g, out, *bufs):
        me = coords()
        barrier(me, sib=False)
        for event in Scatter(me, g, out, bufs, cols).events():
            event()

    return pl.pallas_call(
        kernel,
        in_specs=[pl.BlockSpec(memory_space=pltpu.HBM)],
        out_specs=pl.BlockSpec(memory_space=pltpu.HBM),
        out_shape=jax.ShapeDtypeStruct((rows, width), bf),
        scratch_shapes=Scatter.scratch(rows, cols),
        compiler_params=pltpu.CompilerParams(collective_id=number, has_side_effects=True, vmem_limit_bytes=60 * 2**20),
        name=f"scatter_{number}",
    )(g)


def mm(a, w, dims):
    return lax.dot_general(a, w, dims, preferred_element_type=f32).astype(bf)


def norm_back(h, by_a, by_h):
    wide = h.astype(f32)
    scale = lax.rsqrt(jnp.mean(wide**2, -1, keepdims=True) + 1e-6)
    by_a = by_a.astype(f32)
    by_wide = scale * by_a - wide * (scale**3 * jnp.mean(wide * by_a, -1, keepdims=True))
    return (by_h.astype(f32) + by_wide.astype(bf).astype(f32)).astype(bf)


def solution(mesh):
    def device(x, dy, w_gate, w_up, w_down):
        x, dy = x[0], dy[0]
        own0, own1 = (jnp.stack([w_gate[n], w_up[n]]) for n in (0, 1))
        gu0, dd, gu1, gate0, up0, act0, a0, h1, a1, act1, dgate1, dup1 = forward(x, dy, own0, w_down, own1)
        gu0, gu1 = (t.reshape(2, D, FF) for t in (gu0, gu1))
        dd = dd.reshape(2, FF, D)
        by = {}
        by["w_down", 1] = mm(act1, dy, TN)
        by["w_gate", 1] = mm(a1, dgate1, TN)
        by["w_up", 1] = mm(a1, dup1, TN)
        dh = norm_back(h1, mm(dgate1, gu1[0], NT) + mm(dup1, gu1[1], NT), dy)
        by["w_down", 0] = mm(act0, dh, TN)
        ds = mm(dh, dd[0], NT).astype(f32)
        sig = jax.nn.sigmoid(gate0)
        silu = gate0 * sig
        dgate0 = (ds * up0 * (sig + silu * (1 - sig))).astype(bf)
        dup0 = (ds * silu).astype(bf)
        by["w_gate", 0] = mm(a0, dgate0, TN)
        by["w_up", 0] = mm(a0, dup0, TN)
        by_x = norm_back(x, mm(dgate0, gu0[0], NT) + mm(dup0, gu0[1], NT), dh)
        outs = []
        for j, name in enumerate(NAMES):
            rows, cols = (44, D_COLS) if name == "w_down" else (16, GU_COLS)
            both = [scatter_call(by[name, n].reshape(4, 4, 4, rows, -1), cols, 3 + 2 * j + n) for n in (0, 1)]
            outs.append(jnp.stack(both))
        return (by_x[None], *outs)

    return jax.shard_map(
        device,
        mesh=mesh,
        in_specs=(P(("rep", "dp")), P(("rep", "dp")), *(P(None, "dp"),) * 3),
        out_specs=(P(("rep", "dp")), *(P("rep", "dp"),) * 3),
        check_vma=False,
    )
```

```python
import functools
import jax, jax.numpy as jnp
from jax import lax
from jax.experimental import pallas as pl
from jax.experimental.pallas import tpu as pltpu
from jax.sharding import PartitionSpec as P
ZERO, ONE, TWO, THREE, FOUR, FIVE, SIX, SEVEN, EIGHT, NINE, TEN, ELEVEN, TWELVE = range(13)
ROWS = 1024 // 64
bf=jnp.bfloat16
MESH=pl.DeviceIdType.MESH
PERM=((ZERO,ONE,TWO),(ONE,TWO,ZERO),(TWO,ZERO,ONE))

class Place:
    def __init__(self):
        i=lax.axis_index("dp")
        self.plus=[[c,*((c+d)%FOUR for d in range(ONE,FOUR))] for c in (i//ROWS,(i//FOUR)%FOUR,i%FOUR)]
        self.near=[]
        for a in range(THREE):
            c=[self.plus[b][ZERO] for b in range(THREE)]
            self.near.append([{"dp":(c[:a]+[self.plus[a][d]]+c[a+ONE:])[ZERO]*ROWS+(c[:a]+[self.plus[a][d]]+c[a+ONE:])[ONE]*FOUR+(c[:a]+[self.plus[a][d]]+c[a+ONE:])[TWO]} for d in range(FOUR)])

def coords():
    return Place()

def shifted(me,axis,d):
    return me.near[axis][d]

def peers(me,far=True):
    return [shifted(me,a,d) for a in range(THREE) for d in ((ONE,THREE,TWO) if far else (ONE,THREE))]

def barrier(me,far=True,sib=True):
    b=pltpu.get_barrier_semaphore()
    n=ZERO
    for t in peers(me,far):
        pl.semaphore_signal(b,inc=ONE,device_id=t,device_id_type=MESH); n+=ONE
    if sib:
        pl.semaphore_signal(b,inc=ONE,device_id={"rep":ONE-lax.axis_index("rep")},device_id_type=MESH); n+=ONE
    pl.semaphore_wait(b,n)

class Gather:
    NSEM=15
    def __init__(self,me,own,out,ssem,rsem,lsem,cols):
        self.me,self.own,self.out,self.ssem,self.rsem,self.lsem,self.cols=me,own,out,ssem,rsem,lsem,cols
        self.r=lax.axis_index("rep"); self.sib={"rep":ONE-self.r}
    def at(self,p,r,u,v,w):
        i=[None]*THREE
        for a,k in zip(PERM[p],(u,v,w)): i[a]=k
        return self.out.at[(r,pl.ds(*self.cols[p]),*i)]
    def copy(self,p,k,src,dst,dev):
        return pltpu.make_async_remote_copy(src_ref=src,dst_ref=dst,send_sem=self.ssem.at[p,k],recv_sem=self.rsem.at[p,k],device_id=dev,device_id_type=MESH)
    def m(self,p,k,d=ZERO): return self.me.plus[PERM[p][k]][d]
    def sent(self,p,k):
        r=self.r; u,v,w=(self.m(p,j) for j in range(THREE)); A=slice(None); lo,hi=pl.ds(ZERO,TWO),pl.ds(TWO,TWO)
        near=[self.me.near[a] for a in PERM[p]]
        if k<THREE: return self.own.at[r,pl.ds(*self.cols[p])],self.at(p,r,u,v,w),near[ZERO][(ONE,THREE,TWO)[k]]
        if k<FIVE: ref,to=self.at(p,r,A,v,w),near[ONE][(ONE,THREE)[k-THREE]]
        elif k<SEVEN: ref,to=self.at(p,r,(lo,hi)[k-FIVE],self.m(p,ONE,(THREE,ONE)[k-FIVE]),w),near[ONE][(ONE,THREE)[k-FIVE]]
        elif k<NINE: ref,to=self.at(p,r,A,A,w),near[TWO][(ONE,THREE)[k-SEVEN]]
        elif k<ELEVEN: ref,to=self.at(p,r,(lo,hi)[k-NINE],A,self.m(p,TWO,(THREE,ONE)[k-NINE])),near[TWO][(ONE,THREE)[k-NINE]]
        else: ref,to=self.at(p,r,A,A,self.m(p,TWO,(ZERO,THREE,ONE,TWO)[k-ELEVEN])),self.sib
        return ref,ref,to
    def received(self,p,k):
        r=self.r; v,w=self.m(p,ONE),self.m(p,TWO); A=slice(None); lo,hi=pl.ds(ZERO,TWO),pl.ds(TWO,TWO)
        if k<THREE: return self.at(p,r,self.m(p,ZERO,(THREE,ONE,TWO)[k]),v,w)
        if k<FIVE: return self.at(p,r,A,self.m(p,ONE,(THREE,ONE)[k-THREE]),w)
        if k<SEVEN: return self.at(p,r,(lo,hi)[k-FIVE],self.m(p,ONE,TWO),w)
        if k<NINE: return self.at(p,r,A,A,self.m(p,TWO,(THREE,ONE)[k-SEVEN]))
        if k<ELEVEN: return self.at(p,r,(lo,hi)[k-NINE],A,self.m(p,TWO,TWO))
        return self.at(p,ONE-r,A,A,self.m(p,TWO,(ZERO,THREE,ONE,TWO)[k-ELEVEN]))
    def start(self,p,k):
        s,d,dev=self.sent(p,k); self.copy(p,k,s,d,dev).start()
    def wait_send(self,p,k):
        s,d,dev=self.sent(p,k); self.copy(p,k,s,d,dev).wait_send()
    def wait_recv(self,p,k):
        ref=self.received(p,k); self.copy(p,k,ref,ref,self.sib).wait_recv()
    def local(self,p):
        return pltpu.make_async_copy(self.own.at[self.r,pl.ds(*self.cols[p])],self.at(p,self.r,*(self.m(p,j) for j in range(THREE))),self.lsem.at[p])
    def events(self):
        P3=range(THREE)
        def e0():
            for p in P3:
                self.local(p).start()
                for k in (ZERO,ONE,TWO): self.start(p,k)
        def e1():
            for p in P3:
                self.local(p).wait()
                for k in (ZERO,ONE,TWO): self.wait_recv(p,k)
                for k in (THREE,FOUR): self.start(p,k)
        def e2():
            for p in P3:
                for k in (THREE,FOUR): self.wait_recv(p,k); self.start(p,k+TWO)
        def e3():
            for p in P3:
                for k in (FIVE,SIX): self.wait_recv(p,k)
                for k in (SEVEN,EIGHT,ELEVEN): self.start(p,k)
        def e4():
            for p in P3:
                for k in (SEVEN,EIGHT): self.wait_recv(p,k); self.start(p,k+TWO); self.start(p,k+FIVE)
        def e5():
            for p in P3:
                for k in (NINE,TEN): self.wait_recv(p,k)
                self.start(p,14)
        def e6():
            for p in P3:
                for k in range(ELEVEN,15): self.wait_recv(p,k)
        return [e0,e1,e2,e3,e4,e5,e6]
    def finish(self):
        for p in range(THREE):
            for k in range(15): self.wait_send(p,k)

f32=jnp.float32

T, D, FF, LAYERS = 2048, 1024, 2816, TWO
F = 256
N_F = FF // F
M = 512
N_T = T // M
NT = (((ONE,), (ONE,)), ((), ()))
TN = (((ZERO,), (ZERO,)), ((), ()))
L = 128
C = FF // L
GU0 = (((ZERO, TWO), (TWO, TWO), (FOUR, TWO)), ((SIX, THREE), (NINE, THREE), (TWELVE, TWO)), ((14, THREE), (17, THREE), (20, TWO)))
DD = ((ZERO, FOUR), (FOUR, FOUR), (EIGHT, THREE))
GU1 = (((ZERO, FOUR), (FOUR, THREE), (SEVEN, FOUR)), ((ELEVEN, THREE), (14, FOUR), (18, FOUR)))
HBM = pl.BlockSpec(memory_space=pltpu.HBM)
VMEM = pl.BlockSpec(memory_space=pltpu.VMEM)


def dot(a, b, dims=None):
    if dims is None:
        return jnp.dot(a, b, preferred_element_type=f32)
    return lax.dot_general(a, b, dims, preferred_element_type=f32)


def norm_rows(h):
    wide = h.astype(f32)
    return (wide * lax.rsqrt(jnp.mean(wide * wide, -ONE, keepdims=True) + 1e-6)).astype(bf)


def run(events):
    for event in events:
        event()


def at_step(i, events):
    for step, functions in events.items():
        pl.when(i == step)(functools.partial(run, functions))


def pair(ref, f):
    return ref.at[pl.ds(TWO * f, TWO)]


def wide(tiles):
    return jnp.concatenate(tiles, axis=ONE)


def down_block(tiles):
    last = [wide([tiles[ROWS + TWO * g + e][FOUR * c : FOUR * c + FOUR] for c in range(FOUR) for e in (ZERO, ONE)]) for g in range(THREE)]
    return jnp.concatenate([wide(tiles[:EIGHT]), wide(tiles[EIGHT:ROWS]), *last], axis=ZERO)


def plan_forward():
    tiles = [max(n for _, n in cols) for cols in (*GU0, DD, DD, *GU1)]
    per_tile = (0.27, 0.36, 0.18, 1.43, 0.72, 0.0, 0.0)
    due = {ZERO: ZERO, ONE: TWO, TWO: SIX, THREE: N_F, FOUR: N_F + TWO, FIVE: 99, SIX: 99}
    length = [3.0] * N_F + [3.8] * (TWO * N_T)
    late = (2.7, 2.7, 2.7, 2.7, 2.7, 1.5, 0.0)
    following = [ZERO] * SEVEN
    arrives = [0.0] * SEVEN
    plan = [[] for _ in range(N_F + TWO * N_T + TWO)]
    now, link = 0.0, 0.0

    def allowed(place, k):
        e = following[k]
        if e > SIX:
            return False
        if k == ZERO:
            return True
        before = following[k - ONE]
        if place == ZERO and k > TWO:
            return False
        return before > FOUR or (before > THREE and link <= now + 1.0) if e == THREE else before > ZERO

    def run_one(place, k):
        nonlocal now, link
        e = following[k]
        now = max(now, arrives[k]) + 0.3
        plan[place].append((k, e))
        link = max(link, now) + per_tile[e] * tiles[k]
        arrives[k] = (link if e < FIVE else now) + late[e]
        following[k] = e + ONE

    for place in range(len(plan)):
        while True:
            ready = [k for k in range(SEVEN) if allowed(place, k) and arrives[k] <= now]
            if ready:
                run_one(place, ready[ZERO])
                continue
            must = [k for k in range(SEVEN) if following[k] < SEVEN and (due[k] <= place or place == len(plan) - ONE)]
            if not must:
                break
            waiting = [k for k in range(SEVEN) if allowed(place, k) and following[k] < SEVEN]
            run_one(place, min(waiting, key=lambda k: arrives[k]))
        if place < len(length):
            now += length[place]
    return plan


def forward_kernel(
    x_hbm, dy_hbm, w_gate, w_up, own_d,
    gu0, d0, gu1, gate0, up0, act0, a0, h1, a1, dact1, d1,
    x, a, big, wt, go, raw, wc, ho, dyt, own,
    ssem, rsem, csem, xsem, wsem, gsem, bsem, rawsem, hsem, asem, dsem, esem,
):
    load_x = pltpu.make_async_copy(x_hbm, x, xsem.at[ZERO])
    load_x.start()

    def own_tile(c, _):
        for layer in range(LAYERS):
            for k, w in enumerate((w_gate, w_up)):
                own[layer, k, c] = w[layer, :, pl.ds(pl.multiple_of(c * L, L), L)]
        return ZERO

    lax.fori_loop(ZERO, C, own_tile, ZERO)
    me = coords()
    barrier(me)

    def stream(k, shard, out, cols):
        g = Gather(me, shard, out, ssem.at[k], rsem.at[k], csem.at[k], cols)
        return g, g.events()

    todo = [(own.at[ZERO], gu0, cols) for cols in GU0] + [(own_d.at[n], d, DD) for n, d in enumerate((d0, d1))] + [(own.at[ONE], gu1, cols) for cols in GU1]
    streams = [stream(k, *one) for k, one in enumerate(todo)]
    plan = [[streams[k][ONE][e] for k, e in place] for place in plan_forward()]

    run(plan[ZERO][:TWO])
    load_x.wait()

    def norm0(t, _):
        rows = pl.ds(pl.multiple_of(t * M, M), M)
        a[rows, :] = norm_rows(x[rows, :])
        return ZERO

    lax.fori_loop(ZERO, N_T, norm0, ZERO)
    keep_a0 = pltpu.make_async_copy(a, a0, xsem.at[ONE])
    keep_a0.start()
    run(plan[ZERO][TWO:])

    def load_w(w, f, slot):
        return pltpu.make_async_copy(w.at[:, pl.ds(TWO * f, TWO)], wt.at[slot], wsem.at[slot])

    def put(f, slot):
        return (
            pltpu.make_async_copy(go.at[slot, ZERO], pair(gate0, f), gsem.at[slot, ZERO]),
            pltpu.make_async_copy(go.at[slot, ONE], pair(up0, f), gsem.at[slot, ONE]),
            pltpu.make_async_copy(pair(big, f), pair(act0, f), bsem.at[slot]),
        )

    def gate_up(f, events, w, finish):
        slot = lax.rem(f, TWO)
        load_w(w, f, slot).wait()

        @pl.when(f + ONE < N_F)
        def _():
            load_w(w, f + ONE, ONE - slot).start()

        finish(f, slot, [wide([wt[slot, k, e].reshape(D, L) for e in (ZERO, ONE)]) for k in (ZERO, ONE)])
        at_step(f, events)
        return ZERO

    def finish0(f, slot, w):
        @pl.when(f >= TWO)
        def _():
            for copy in put(f - TWO, slot):
                copy.wait()

        for t in range(N_T):
            rows = pl.ds(t * M, M)
            gate, up = dot(a[rows, :], w[ZERO]), dot(a[rows, :], w[ONE])
            act = (gate * jax.nn.sigmoid(gate) * up).astype(bf)
            for e in (ZERO, ONE):
                lanes = slice(L * e, L * e + L)
                go[slot, ZERO, e, rows, :] = gate[:, lanes]
                go[slot, ONE, e, rows, :] = up[:, lanes]
                big[TWO * f + e, rows, :] = act[:, lanes]
        for copy in put(f, slot):
            copy.start()

    load_raw = [pltpu.make_async_copy(d, raw, rawsem) for d in (d0, d1)]
    ev = {f: plan[ONE + f] for f in range(N_F)}
    load_w(gu0, ZERO, ZERO).start()
    lax.fori_loop(ZERO, N_F, lambda f, _: gate_up(f, ev, gu0, finish0), ZERO)
    load_raw[ZERO].start()
    for f in (N_F - TWO, N_F - ONE):
        for copy in put(f, f % TWO):
            copy.wait()
    keep_a0.wait()

    def convert():
        def four(g, _):
            blocks = [down_block([raw[c // ELEVEN, c % ELEVEN, g // FOUR, lax.rem(g, FOUR), z] for c in range(C)]) for z in range(FOUR)]
            wc[pl.ds(pl.multiple_of(176 * g, 176), 176), :] = jnp.concatenate(blocks, axis=ZERO)
            return ZERO

        lax.fori_loop(ZERO, ROWS, four, ZERO)

    load_raw[ZERO].wait()
    convert()

    def put_h(t, slot):
        return pltpu.make_async_copy(ho.at[slot], h1.at[pl.ds(pl.multiple_of(t * M, M), M)], hsem.at[slot])

    def load_dy(t, slot):
        return pltpu.make_async_copy(dy_hbm.at[pl.ds(pl.multiple_of(t * M, M), M)], dyt.at[slot], dsem.at[slot])

    def down(t, events):
        slot = lax.rem(t, TWO)

        @pl.when(t >= TWO)
        def _():
            put_h(t - TWO, slot).wait()

        rows = pl.ds(pl.multiple_of(t * M, M), M)
        h = (x[rows, :].astype(f32) + dot(wide([big[c, rows, :] for c in range(C)]), wc[...]).astype(bf).astype(f32)).astype(bf)
        ho[slot] = h
        a[rows, :] = norm_rows(h)
        put_h(t, slot).start()
        at_step(t, events)
        return ZERO

    lax.fori_loop(ZERO, N_T, lambda t, _: down(t, {ZERO: plan[ONE + N_F], ONE: [*plan[TWO + N_F], load_raw[ONE].start], TWO: plan[THREE + N_F], THREE: plan[FOUR + N_F]}), ZERO)
    keep_a1 = pltpu.make_async_copy(a, a1, asem)
    keep_a1.start()
    load_dy(ZERO, ZERO).start()
    for t in (N_T - TWO, N_T - ONE):
        put_h(t, t % TWO).wait()
    load_raw[ONE].wait()
    convert()

    def put_dact(t):
        r = pl.ds(pl.multiple_of(t * M, M), M)
        return pltpu.make_async_copy(big.at[:, r], dact1.at[:, r], esem.at[t])

    def dact(t, events):
        slot = lax.rem(t, TWO)
        load_dy(t, slot).wait()

        @pl.when(t + ONE < N_T)
        def _():
            load_dy(t + ONE, ONE - slot).start()

        rows = pl.ds(pl.multiple_of(t * M, M), M)
        for half in (ZERO, ONE):
            v = dot(dyt[slot], wc[FF // TWO * half : FF // TWO * half + FF // TWO, :], NT).astype(bf)
            for c in range(ELEVEN):
                big[ELEVEN * half + c, rows, :] = v[:, L * c : L * c + L]
        put_dact(t).start()
        at_step(t, events)
        return ZERO

    lax.fori_loop(ZERO, N_T, lambda t, _: dact(t, {n: plan[FIVE + N_F + n] for n in range(N_T)}), ZERO)
    run(plan[-ONE])

    for t in range(N_T):
        put_dact(t).wait()
    keep_a1.wait()
    for g, _ in streams:
        g.finish()


def forward(x, dy, w_gate, w_up, own_d):
    sd = jax.ShapeDtypeStruct
    tall, tall32, narrow = sd((C, T, L), bf), sd((C, T, L), f32), sd((T, D), bf)
    blocks = sd((TWO, C, FOUR, FOUR, FOUR, ROWS, L), bf)
    half_blocks = sd((TWO, C // TWO, FOUR, FOUR, FOUR, ROWS, L), bf)
    dma = pltpu.SemaphoreType.DMA
    return pl.pallas_call(
        forward_kernel,
        in_specs=[HBM, HBM, VMEM, VMEM, VMEM],
        out_specs=[HBM] * ELEVEN,
        out_shape=[blocks, half_blocks, blocks, tall32, tall32, tall, narrow, narrow, narrow, tall, half_blocks],
        scratch_shapes=[
            pltpu.VMEM((T, D), bf), pltpu.VMEM((T, D), bf), pltpu.VMEM((C, T, L), bf),
            pltpu.VMEM((TWO, TWO, TWO, FOUR, FOUR, FOUR, ROWS, L), bf), pltpu.VMEM((TWO, TWO, TWO, T, L), f32),
            pltpu.VMEM((TWO, C // TWO, FOUR, FOUR, FOUR, ROWS, L), bf), pltpu.VMEM((FF, D), bf), pltpu.VMEM((TWO, M, D), bf),
            pltpu.VMEM((TWO, M, D), bf), pltpu.VMEM((LAYERS, TWO, C, ROWS, L), bf),
            dma((SEVEN, THREE, 15)), dma((SEVEN, THREE, 15)), dma((SEVEN, THREE)), dma((TWO,)), dma((TWO,)), dma((TWO, TWO)), dma((TWO,)), dma(()), dma((TWO,)), dma(()), dma((TWO,)), dma((FOUR,)),
        ],
        compiler_params=pltpu.CompilerParams(collective_id=ZERO, has_side_effects=True, vmem_limit_bytes=63 * TWO**20),
        name="forward",
    )(x, dy, w_gate, w_up, own_d)[:TEN]


HALF = FF // TWO
PARTS = ((ZERO, FOUR), (FOUR, FOUR), (EIGHT, THREE))
UNITS = TWELVE


class Scatter:
    @staticmethod
    def vw(p, v, w):
        return (slice(None), v, w) if PERM[p][ONE] < PERM[p][TWO] else (slice(None), w, v)

    @staticmethod
    def scratch():
        s = []
        for p, (_, n) in enumerate(PARTS):
            _, *h = Scatter.vw(p, TWO, FOUR)
            s += [
                pltpu.VMEM((TWO, SIX, n, *h, ROWS, L), bf),
                pltpu.VMEM((TWO, FOUR, n, *h, ROWS, L), bf),
                pltpu.VMEM((n, FOUR, FOUR, ROWS, L), f32), pltpu.VMEM((n, FOUR, FOUR, ROWS, L), bf),
                pltpu.VMEM((SIX, n, TWO, ROWS, L), bf), pltpu.VMEM((TWO, n, TWO, ROWS, L), bf),
                pltpu.VMEM((n, FOUR, ROWS, L), f32), pltpu.VMEM((n, FOUR, ROWS, L), bf),
                pltpu.VMEM((THREE, n, ROWS, L), bf),
            ]
        dma = pltpu.SemaphoreType.DMA
        regular = pltpu.SemaphoreType.REGULAR
        return s + [pltpu.VMEM((ROWS, FF // TWO), bf), dma((TWO, THREE, 15)), dma((TWO, THREE, 15)), dma((TWO, THREE, FOUR)), dma(()), regular((THREE, TWO)), regular((THREE, TWO)), regular((THREE, THREE))]

    def __init__(self, me, grads, out, bufs):
        self.me, self.grads, self.out = me, grads, out
        self.b = [bufs[NINE * p : NINE * p + NINE] for p in range(THREE)]
        self.res, self.ssem, self.rsem, self.lsem, self.osem, self.credit1, self.credit2, self.credit3 = bufs[27:]

    def m(self, p, k, d=ZERO):
        return self.me.plus[PERM[p][k]][d]

    def at_unit(self, k):
        self.k, self.slot = k, lax.rem(k, TWO)
        odd = lax.rem(k, TWO)
        self.grad = jnp.where(k < FOUR, ONE + odd, jnp.where(k < SIX, ZERO, jnp.where(k < EIGHT, THREE, FOUR + odd)))
        self.col0 = C // TWO * jnp.where(k < FOUR, k // TWO, jnp.where(k < EIGHT, odd, k // TWO - FOUR))

    def cols(self, p):
        c, n = PARTS[p]
        return pl.ds(self.col0 + c, n)

    def term(self, p, u, half):
        i = [None] * THREE
        a, v, w = PERM[p]
        i[a], i[v], i[w] = u, pl.ds(TWO * half, TWO), slice(None)
        return self.grads.at[(self.grad, self.cols(p), *i)]

    def own(self, p, j):
        u, h = ((ONE, ZERO), (THREE, ONE), (ZERO, ZERO), (ZERO, ONE))[j]
        return pltpu.make_async_copy(self.term(p, self.m(p, ZERO, u), h), self.b[p][ONE].at[self.slot, j], self.lsem.at[self.slot, p, j])

    def cp(self, p, k):
        b, s = self.b[p], self.slot
        if k < SIX:
            ax, d = ZERO, (ONE, THREE, ONE, THREE, ONE, THREE)[k]
            if k < FOUR:
                u, h = ((TWO, ZERO), (TWO, ONE), (ONE, ONE), (THREE, ZERO))[k]
                src = self.term(p, self.m(p, ZERO, u), h)
            else:
                src = b[ONE].at[s, k - FOUR]
            dst = b[ZERO].at[s, k]
        elif k < TWELVE:
            j = k - SIX
            ax, d = ONE, (ONE, THREE, ONE, THREE, ONE, THREE)[j]
            if j < FOUR:
                v, h = ((TWO, ZERO), (TWO, ONE), (ONE, ONE), (THREE, ZERO))[j]
                src = b[THREE].at[self.vw(p, self.m(p, ONE, v), pl.ds(TWO * h, TWO))]
            else:
                src = b[FIVE].at[j - FOUR]
            dst, s = b[FOUR].at[j], ZERO
        else:
            ax, d = TWO, (ONE, THREE, TWO)[k - TWELVE]
            src, dst, s = b[SEVEN].at[:, self.m(p, TWO, d)], b[EIGHT].at[k - TWELVE], ZERO
        return pltpu.make_async_remote_copy(
            src_ref=src, dst_ref=dst, send_sem=self.ssem.at[s, p, k], recv_sem=self.rsem.at[s, p, k],
            device_id=shifted(self.me, PERM[p][ax], d), device_id_type=MESH,
        )

    def give(self, credit, axis, last):
        @pl.when(self.k < last)
        def _():
            for p in range(THREE):
                for j, d in enumerate((THREE, ONE, TWO)[: credit.shape[ONE]]):
                    pl.semaphore_signal(credit.at[p, j], inc=ONE, device_id=shifted(self.me, PERM[p][axis], d), device_id_type=MESH)

    def take(self, credit, first):
        @pl.when(self.k >= first)
        def _():
            for p in range(THREE):
                for j in range(credit.shape[ONE]):
                    pl.semaphore_wait(credit.at[p, j], ONE)

    def begin(self):
        self.take(self.credit1, TWO)
        for k in (ZERO, ONE, TWO, THREE):
            for p in range(THREE):
                self.cp(p, k).start()
        for p in range(THREE):
            for j in range(FOUR):
                self.own(p, j).start()

    def pass_on(self):
        s = self.slot
        for p in range(THREE):
            b = self.b[p]
            for k in (ZERO, ONE):
                self.own(p, k).wait()
                self.cp(p, k).wait_recv()
                b[ONE][s, k] = (b[ZERO][s, k].astype(f32) + b[ONE][s, k].astype(f32)).astype(bf)
        for k in (FOUR, FIVE):
            for p in range(THREE):
                self.cp(p, k).start()

    def first_sum(self):
        s = self.slot
        for p in range(THREE):
            b = self.b[p]
            for k in (TWO, THREE, FOUR, FIVE):
                self.cp(p, k).wait_recv()
            for j in (TWO, THREE):
                self.own(p, j).wait()
            for half in (ZERO, ONE):
                own, sums, raw = ((TWO, FOUR, THREE), (THREE, FIVE, TWO))[half]
                t = b[ONE][s, own].astype(f32) + b[ZERO][s, sums].astype(f32) + b[ZERO][s, raw].astype(f32)
                ix = self.vw(p, slice(TWO * half, TWO * half + TWO), slice(None))
                b[TWO][ix] = t
                b[THREE][ix] = t.astype(bf)
        for p in range(THREE):
            for k in range(SIX):
                self.cp(p, k).wait_send()
        self.give(self.credit1, ZERO, UNITS - TWO)
        self.take(self.credit2, ONE)
        for k in (SIX, SEVEN, EIGHT, NINE):
            for p in range(THREE):
                self.cp(p, k).start()

    def pass_on2(self):
        for p in range(THREE):
            b = self.b[p]
            for half in (ZERO, ONE):
                self.cp(p, SIX + half).wait_recv()
                v = self.m(p, ONE, (ONE, THREE)[half])
                own = b[TWO][self.vw(p, v, slice(TWO * half, TWO * half + TWO))]
                b[FIVE][half] = (b[FOUR][half].astype(f32) + own).astype(bf)
        for k in (TEN, ELEVEN):
            for p in range(THREE):
                self.cp(p, k).start()

    def second_sum(self):
        for p in range(THREE):
            b, v = self.b[p], self.m(p, ONE)
            for k in (EIGHT, NINE, TEN, ELEVEN):
                self.cp(p, k).wait_recv()
            for half in (ZERO, ONE):
                sums, raw = ((FOUR, THREE), (FIVE, TWO))[half]
                part = slice(TWO * half, TWO * half + TWO)
                t = b[TWO][self.vw(p, v, part)] + b[FOUR][sums].astype(f32) + b[FOUR][raw].astype(f32)
                b[SIX][:, part] = t
                b[SEVEN][:, part] = t.astype(bf)
        for p in range(THREE):
            for k in range(SIX, TWELVE):
                self.cp(p, k).wait_send()
        self.give(self.credit2, ONE, UNITS - ONE)
        self.take(self.credit3, ONE)
        for k in (TWELVE, 13, 14):
            for p in range(THREE):
                self.cp(p, k).start()

    def total(self):
        for p in range(THREE):
            b, w = self.b[p], self.m(p, TWO)
            for k in (TWELVE, 13, 14):
                self.cp(p, k).wait_recv()
            t = b[SIX][:, w]
            for j in range(THREE):
                t = t + b[EIGHT][j].astype(f32)
            c, n = PARTS[p]
            for q in range(n):
                self.res[:, L * (c + q) : L * (c + q) + L] = t[q].astype(bf)
        layer, kind = ONE - self.grad // THREE, lax.rem(self.grad, THREE)
        for m, out in enumerate(self.out):

            @pl.when(kind == m)
            def _():
                pltpu.make_async_copy(self.res, out.at[layer, :, pl.ds(pl.multiple_of(self.col0 * L, L), FF // TWO)], self.osem).start()

        for p in range(THREE):
            for k in (TWELVE, 13, 14):
                self.cp(p, k).wait_send()
        self.give(self.credit3, TWO, UNITS - ONE)
        pltpu.make_async_copy(self.res, self.out[ZERO].at[ZERO, :, pl.ds(ZERO, FF // TWO)], self.osem).wait()

    def tick(self, j, plan):
        def due(steps):
            words = [sum(ONE << (n - 30 * w) for n in steps if n // 30 == w) for w in range(max(steps) // 30 + ONE)]
            word = functools.reduce(lambda have, w: jnp.where(j >= 30 * w, words[w], have), range(ONE, len(words)), words[ZERO])
            return (lax.shift_right_logical(jnp.int32(word), lax.rem(j, 30)) & ONE) == ONE

        @pl.when(due({n for steps in plan.values() for n in steps}))
        def _():
            for event in (self.total, self.second_sum, self.pass_on2, self.first_sum, self.pass_on, self.begin):
                steps = plan[event.__name__]

                @pl.when(due(steps))
                def _():
                    self.at_unit(sum(jnp.where(j > n, ONE, ZERO) for n in steps))
                    event()


S1, S2, S3, S6, S5, S7, S9, TAIL = ZERO, ELEVEN, 19, 35, 43, 51, 63, 79


def make_plan():
    length = [5.2] * ELEVEN + [2.3] * EIGHT + [1.95] * ROWS + [2.3] * EIGHT + [2.1] * EIGHT + [3.6] * TWELVE + [1.95] * ROWS
    ready = [SEVEN, SEVEN, S2 + ONE, S2 + ONE, S3 + ONE, S3 + ONE, S5 + ONE, S5 + ONE, S7 + EIGHT, S7 + EIGHT, S9 + ONE, S9 + ONE]
    names = ("begin", "pass_on", "first_sum", "pass_on2", "second_sum", "total")
    sends = (5.9, 2.95, 1.5, 0.8, 1.0, 0.0)
    late = 2.5
    plan = {name: [] for name in names}
    arrives = [[0.0] * SEVEN for _ in range(UNITS)]
    now, link, step = 3.0, 0.0, ZERO

    def may_run(e, k):
        n = len(plan[names[e]])
        if n != k or (plan[names[e]] and plan[names[e]][-ONE] == step):
            return False
        if e == ZERO:
            return step >= ready[k] and (k < TWO or len(plan["first_sum"]) > k - TWO)
        if len(plan[names[e - ONE]]) <= k or plan[names[e - ONE]][k] == step:
            return False
        if e == TWO and len(plan["second_sum"]) < k:
            return False
        return not (e == FOUR and len(plan["total"]) < k)

    while len(plan["total"]) < UNITS:
        ran = False
        for e in (FIVE, FOUR, THREE, TWO, ONE, ZERO):
            k = len(plan[names[e]])
            if k < UNITS and may_run(e, k) and (arrives[k][e] <= now or step >= TAIL):
                if step >= TAIL and arrives[k][e] > now:
                    if ran or any(may_run(o, len(plan[names[o]])) and arrives[len(plan[names[o]])][o] < arrives[k][e] for o in range(SIX) if o != e and len(plan[names[o]]) < UNITS):
                        continue
                    now = arrives[k][e]
                plan[names[e]].append(step)
                ran = True
                now += 0.3
                link = max(link, now) + sends[e]
                if e == ZERO:
                    arrives[k][ONE], arrives[k][TWO] = link - sends[ONE] + late, link + late
                elif e < FIVE:
                    arrives[k][e + ONE] = max(arrives[k][e + ONE], link + late)
        now += length[step] if step < TAIL else 0.05
        step += ONE
    return plan


PLAN = make_plan()
N_STEPS = max(PLAN["total"]) + ONE


def backward_kernel(
    x, dy, gu0, d0, gu1, gate0, up0, act0, a0, h1, a1, dact1,
    dx, by_down, by_gate, by_up, grads, dup1,
    am, dh, r1, r2, r3, stg, tl, ob, gl, ht,
    lsem, r1sem, r2sem, r3sem, amsem, wsem, dasem, tlsem, obsem, glsem, flsem, hsem, dxsem, *bufs,
):
    me = coords()
    barrier(me, sib=False)
    scatter = Scatter(me, grads, (by_down, by_gate, by_up), bufs)

    def rows(t, n=M):
        return pl.ds(pl.multiple_of(t * n, n), n)

    def col(f, n=F):
        return pl.ds(pl.multiple_of(f * n, 128), n)

    load_dh = pltpu.make_async_copy(dy, dh, lsem)
    load_dup = pltpu.make_async_copy(dup1, r1, r1sem)
    load_act = pltpu.make_async_copy(act0, r2, r2sem)

    def load_am(src):
        return pltpu.make_async_copy(src, am, amsem)

    def load_wt(f, slot):
        return [
            pltpu.make_async_copy(gu1.at[k, pl.ds(TWO * f, TWO), pl.ds(TWO * h, TWO)], stg.at[pl.ds(EIGHT * slot + FOUR * k + TWO * h, TWO)], wsem.at[slot, k, h])
            for k in (ZERO, ONE) for h in (ZERO, ONE)
        ]

    def load_dact(f, slot):
        return pltpu.make_async_copy(pair(dact1, f), pair(r1, f), dasem.at[slot])

    def load_r3(src, h):
        return pltpu.make_async_copy(src.at[:, pl.ds(TWO * h, TWO)], r3.at[:, pl.ds(TWO * h, TWO)], r3sem.at[h])

    def flush(grad, half):
        return pltpu.make_async_copy(stg, grads.at[grad, :, pl.ds(TWO * half, TWO)], flsem)

    def put_tl(f, slot):
        return pltpu.make_async_copy(tl.at[slot], pair(dup1, f), tlsem.at[slot])

    def put_ob(grad, f, slot):
        return [pltpu.make_async_copy(ob.at[slot, k], grads.at[grad + k, pl.ds(TWO * f, TWO)], obsem.at[slot, k]) for k in (ZERO, ONE)]

    def load_gl(f, e):
        return [pltpu.make_async_copy(src.at[TWO * f + e], gl.at[e, k], glsem.at[e, k]) for k, src in enumerate((gate0, up0))]

    def load_h(src, t):
        return pltpu.make_async_copy(src.at[rows(t)], ht, hsem)

    def put_dx(t):
        return pltpu.make_async_copy(dh.at[rows(t)], dx.at[rows(t)], dxsem.at[t])

    def go(copies):
        for c in copies:
            c.start()

    def done(copies):
        for c in copies:
            c.wait()

    def when(condition, f):
        pl.when(condition)(f)

    def gate_up_grad(slot, tiles, parts=(ZERO, FOUR)):
        lo, hi = parts
        v = dot(am[:, F * lo : F * hi], wide(tiles), TN).astype(bf)
        for k in (ZERO, ONE):
            for e in (ZERO, ONE):
                ob[slot, k, e, lo:hi] = v[:, F * k + L * e : F * k + L * e + L].reshape(hi - lo, FOUR, FOUR, ROWS, L)

    def layer1(f, slot):
        w = []
        for k in (ZERO, ONE):
            halves = [wide([stg[EIGHT * slot + FOUR * k + TWO * h + e].reshape(D // TWO, L) for e in (ZERO, ONE)]) for h in (ZERO, ONE)]
            w.append(jnp.concatenate(halves, axis=ZERO))
        for t in range(N_T):
            r = pl.ds(t * M, M)
            gate, up = dot(am[r, :], w[ZERO]), dot(am[r, :], w[ONE])
            by_act = wide([r1[TWO * f + e, r, :] for e in (ZERO, ONE)]).astype(f32)
            sig = jax.nn.sigmoid(gate)
            silu = gate * sig
            act, by_gate, by_up = silu * up, by_act * up * (sig + silu * (ONE - sig)), by_act * silu
            for e in (ZERO, ONE):
                lanes = slice(L * e, L * e + L)
                r1[TWO * f + e, r, :] = act[:, lanes].astype(bf)
                r2[TWO * f + e, r, :] = by_gate[:, lanes].astype(bf)
                tl[slot, e, r, :] = by_up[:, lanes].astype(bf)
        gate_up_grad(slot, [r2[TWO * f], r2[TWO * f + ONE], tl[slot, ZERO], tl[slot, ONE]])

    def down_grad(s, src, grad):
        half, c = s // FOUR, lax.rem(s, FOUR)
        lhs = wide([src[C // TWO * half + i] for i in range(C // TWO)])
        am[: FF // TWO, :F] = dot(lhs, dh[:, col(c)], TN).astype(bf)
        when(s == FOUR, lambda: flush(grad, ZERO).wait())
        lanes = [slice(L * e, L * e + L) for e in (ZERO, ONE)]

        def four(g, _):
            v = am[pl.ds(pl.multiple_of(176 * g, 176), 176), :F]
            x, y = g // FOUR, lax.rem(g, FOUR)
            for z in range(FOUR):
                for e in (ZERO, ONE):
                    stg[TWO * c + e, x, y, z] = v[44 * z : 44 * z + ROWS, lanes[e]]
                    stg[EIGHT + TWO * c + e, x, y, z] = v[44 * z + ROWS : 44 * z + 32, lanes[e]]
            for k in range(FOUR):

                @pl.when(c == k)
                def _():
                    for z in range(FOUR):
                        for n in range(THREE):
                            for e in (ZERO, ONE):
                                stg[ROWS + TWO * n + e, x, y, z, FOUR * k : FOUR * k + FOUR] = v[44 * z + 32 + FOUR * n : 44 * z + 36 + FOUR * n, lanes[e]]

            return ZERO

        lax.fori_loop(ZERO, EIGHT, four, ZERO)
        for h in (ZERO, ONE):
            when(s == FOUR * h + THREE, lambda: flush(grad, h).start())

    def silu_back(f, e, t):
        r = pl.ds(t * M, M)
        gate, up, by_act = gl[e, ZERO, r, :], gl[e, ONE, r, :], r1[TWO * f + e, r, :].astype(f32)
        sig = jax.nn.sigmoid(gate)
        silu = gate * sig
        r2[TWO * f + e, r, :] = (by_act * up * (sig + silu * (ONE - sig))).astype(bf)
        r1[TWO * f + e, r, :] = (by_act * silu).astype(bf)

    def by_input(src, n, t):
        w = wide([r3[c, pl.ds(TWO * n, TWO)].reshape(D // TWO, L) for c in range(C)])
        return dot(wide([src[c, rows(t), :] for c in range(C)]), w, NT).astype(bf)

    def norm_back(t):
        h = ht[...].astype(f32)
        by_a = am[rows(t), :].astype(f32)
        scale = lax.rsqrt(jnp.mean(h * h, -ONE, keepdims=True) + 1e-6)
        by_wide = scale * by_a - h * (scale * scale * scale * jnp.mean(h * by_a, -ONE, keepdims=True))
        dh[rows(t), :] = (dh[rows(t), :].astype(f32) + by_wide.astype(bf).astype(f32)).astype(bf)

    def down_rows(half):
        def four(g, _):
            blocks = [down_block([r3[c, TWO * half + g // FOUR, lax.rem(g, FOUR), z] for c in range(C)]) for z in range(FOUR)]
            am[pl.ds(pl.multiple_of(176 * g, 176), 176), :] = jnp.concatenate(blocks, axis=ZERO)
            return ZERO

        lax.fori_loop(ZERO, EIGHT, four, ZERO)

    def step(j, _):
        def within(a, b):
            return (j >= a) & (j < b)

        in1, in2, in3 = j < S2, within(S2, S3), within(S3, S6)
        in6, in5, in7, in9 = within(S6, S5), within(S5, S7), within(S7, S9), within(S9, TAIL)

        @pl.when(in1)
        def _():
            f = j - S1
            slot = lax.rem(f, TWO)

            @pl.when(f >= TWO)
            def _():
                done(put_ob(ONE, f - TWO, slot))
                put_tl(f - TWO, slot).wait()

            done(load_wt(f, slot))
            load_dact(f, slot).wait()

            @pl.when(f + ONE < N_F)
            def _():
                go(load_wt(f + ONE, ONE - slot))
                load_dact(f + ONE, ONE - slot).start()

            when(f == TWO, lambda: go([load_r3(gu1.at[ZERO], h) for h in (ZERO, ONE)]))

        @pl.when(in2)
        def _():
            @pl.when(j == S2)
            def _():
                done(put_ob(ONE, N_F - TWO, ONE))
                put_tl(N_F - TWO, ONE).wait()
                load_dh.wait()

            @pl.when(j == S2 + ONE)
            def _():
                done(put_ob(ONE, N_F - ONE, ZERO))
                put_tl(N_F - ONE, ZERO).wait()

        def input_pre(s, w, src):
            when(s == ZERO, lambda: load_r3(w.at[ZERO], ZERO).wait())

            @pl.when(s == FOUR)
            def _():
                load_r3(w.at[ZERO], ONE).wait()
                load_r3(w.at[ONE], ZERO).start()

            @pl.when(s == EIGHT)
            def _():
                load_r3(w.at[ONE], ZERO).wait()
                load_r3(w.at[ONE], ONE).start()

            when(s == ELEVEN, lambda: load_h(src, ZERO).start())
            when(s == TWELVE, lambda: load_r3(w.at[ONE], ONE).wait())

        @pl.when(in3)
        def _():
            s = j - S3
            input_pre(s, gu1, h1)
            when(s == ZERO, load_dup.start)
            when(s == ONE, lambda: flush(ZERO, ONE).wait())

            @pl.when(s == EIGHT)
            def _():
                load_dup.wait()
                load_act.start()

            when(s == TWELVE, lambda: load_r3(d0, ZERO).start())

        @pl.when(in9)
        def _():
            s = j - S9
            input_pre(s, gu0, x)
            when(s == ZERO, lambda: done(put_ob(FOUR, N_F - TWO, ONE)))
            when(s == ONE, lambda: done(put_ob(FOUR, N_F - ONE, ZERO)))

        @pl.when(j == S6)
        def _():
            load_act.wait()
            load_r3(d0, ONE).start()

        @pl.when(in5)
        def _():
            s = j - S5

            @pl.when(s == ZERO)
            def _():
                load_r3(d0, ZERO).wait()
                go(load_gl(ZERO, ZERO) + load_gl(ZERO, ONE))

            @pl.when(s == ONE)
            def _():
                flush(THREE, ONE).wait()
                load_r3(gu0.at[ZERO], ZERO).start()

            when(s == FOUR, lambda: load_r3(d0, ONE).wait())
            when(s == FIVE, lambda: load_r3(gu0.at[ZERO], ONE).start())

        @pl.when(in7)
        def _():
            when(j == S7 + ONE, lambda: load_am(a0).wait())
            when(j >= S7 + THREE, lambda: done(put_ob(FOUR, j - S7 - THREE, lax.rem(j - S7 - THREE, TWO))))

        scatter.tick(j, PLAN)

        @pl.when(in1)
        def _():
            f = j - S1
            slot = lax.rem(f, TWO)
            layer1(f, slot)
            go(put_ob(ONE, f, slot))
            put_tl(f, slot).start()

        when(in2, lambda: down_grad(j - S2, r1, ZERO))
        when(in6, lambda: down_grad(j - S6, r2, THREE))

        @pl.when(in3 | in9)
        def _():
            s = jnp.where(in3, j - S3, j - S9)
            n, t = lax.rem(s, EIGHT) // FOUR, lax.rem(s, FOUR)
            here = (rows(t), col(n, D // TWO))

            def more():
                am[here] = (am[here].astype(f32) + by_input(r1, n, t).astype(f32)).astype(bf)

            @pl.when(s < EIGHT)
            def _():
                am[here] = by_input(r2, n, t)

            when((s >= EIGHT) & (s < 13), more)

            @pl.when(s >= 13)
            def _():
                load_h(h1, t - ONE).wait()
                norm_back(t - ONE)
                more()
                when(in3, lambda: load_h(h1, t).start())
                when(in9, lambda: load_h(x, t).start())
                when(in9, lambda: put_dx(t - ONE).start())

            @pl.when(s == 15)
            def _():
                load_h(h1, THREE).wait()
                norm_back(THREE)
                when(in9, lambda: put_dx(THREE).start())

        @pl.when(in5)
        def _():
            s = j - S5
            half, t = s // FOUR, lax.rem(s, FOUR)
            when(t == ZERO, lambda: down_rows(half))
            v = dot(dh[rows(t), :], am[: FF // TWO, :], NT).astype(bf)
            for c in range(C // TWO):
                r1[C // TWO * half + c, rows(t), :] = v[:, L * c : L * c + L]
            when(s == SEVEN, lambda: load_am(a0).start())

        @pl.when(in7)
        def _():
            i = j - S7
            before = i - ONE
            slot = lax.rem(i + ONE, TWO)
            tiles = lambda: [r2[TWO * before], r2[TWO * before + ONE], r1[TWO * before], r1[TWO * before + ONE]]

            @pl.when(i == ZERO)
            def _():
                for e in (ZERO, ONE):
                    done(load_gl(ZERO, e))
                    for t in range(FOUR):
                        silu_back(ZERO, e, t)
                    go(load_gl(ONE, e))

            @pl.when((i > ZERO) & (i < N_F))
            def _():
                for e in (ZERO, ONE):
                    done(load_gl(i, e))
                    for t in (ZERO, ONE):
                        gate_up_grad(slot, tiles(), (TWO * e + t, TWO * e + t + ONE))
                        silu_back(i, e, TWO * t)
                        silu_back(i, e, TWO * t + ONE)
                    when(i + ONE < N_F, lambda: go(load_gl(i + ONE, e)))

            when(i == N_F, lambda: gate_up_grad(slot, tiles()))
            when(i > ZERO, lambda: go(put_ob(FOUR, before, slot)))

        return ZERO

    load_am(a1).start()
    go(load_wt(ZERO, ZERO))
    load_dact(ZERO, ZERO).start()
    load_dh.start()
    load_am(a1).wait()
    lax.fori_loop(ZERO, N_STEPS, step, ZERO)
    done([put_dx(t) for t in range(FOUR)])


def backward(x, dy, gu0, d0, *args):
    sd = jax.ShapeDtypeStruct
    dma = pltpu.SemaphoreType.DMA
    return pl.pallas_call(
        backward_kernel,
        in_specs=[HBM] * TWELVE,
        out_specs=[HBM] * SIX,
        out_shape=[sd((T, D), bf), *[sd((LAYERS, ROWS, FF), bf)] * THREE, sd((SIX, C, FOUR, FOUR, FOUR, ROWS, L), bf), sd((C, T, L), bf)],
        scratch_shapes=[
            pltpu.VMEM((T, D), bf), pltpu.VMEM((T, D), bf), pltpu.VMEM((C, T, L), bf), pltpu.VMEM((C, T, L), bf),
            pltpu.VMEM((C, FOUR, FOUR, FOUR, ROWS, L), bf), pltpu.VMEM((C, TWO, FOUR, FOUR, ROWS, L), bf), pltpu.VMEM((TWO, TWO, T, L), bf),
            pltpu.VMEM((TWO, TWO, TWO, FOUR, FOUR, FOUR, ROWS, L), bf), pltpu.VMEM((TWO, TWO, T, L), f32), pltpu.VMEM((M, D), bf),
            dma(()), dma(()), dma(()), dma((TWO,)), dma(()), dma((TWO, TWO, TWO)), dma((TWO,)), dma((TWO,)), dma((TWO, TWO)), dma((TWO, TWO)), dma(()), dma(()), dma((FOUR,)),
            *Scatter.scratch(),
        ],
        compiler_params=pltpu.CompilerParams(collective_id=ONE, has_side_effects=True, vmem_limit_bytes=63 * TWO**20 + 900 * 1024),
        name="backward",
    )(x, dy, gu0, d0.reshape(C, FOUR, FOUR, FOUR, ROWS, L), *args)[:FOUR]


def pack_down(t):
    first = t[:, :32].reshape(-ONE, TWO, ROWS, EIGHT, L).transpose(ZERO, ONE, THREE, TWO, FOUR).reshape(-ONE, ROWS, ROWS, L)
    last = t[:, 32:].reshape(-ONE, THREE, FOUR, FOUR, TWO, L).transpose(ZERO, ONE, FOUR, THREE, TWO, FIVE).reshape(-ONE, SIX, ROWS, L)
    return jnp.concatenate([first, last], axis=ONE).reshape(-ONE, TWO, C // TWO, ROWS, L)


def unpack_down(t):
    last = t[:, :, TWO * D :].reshape(-ONE, FOUR, FOUR, THREE, F).transpose(ZERO, THREE, TWO, ONE, FOUR).reshape(-ONE, TWELVE, D)
    return jnp.concatenate([t[:, :, :D], t[:, :, D : TWO * D], last], axis=ONE)


def solution(mesh):
    def device(x, dy, w_gate, w_up, w_down):
        x, dy = x[ZERO], dy[ZERO]
        own_d = pack_down(w_down)
        gu0, d0, gu1, *rest = forward(x, dy, w_gate, w_up, own_d)
        by_x, by_down, by_gate, by_up = backward(x, dy, gu0, d0, gu1, *rest)
        return by_x[None], by_gate, by_up, unpack_down(by_down)

    return jax.shard_map(
        device,
        mesh=mesh,
        in_specs=(P(("rep", "dp")), P(("rep", "dp")), *(P(None, "dp"),) * THREE),
        out_specs=(P(("rep", "dp")), *(P("rep", "dp"),) * THREE),
        check_vma=False,
    )
```

```python
import functools
import jax, jax.numpy as jnp
from jax import lax
from jax.experimental import pallas as pl
from jax.experimental.pallas import tpu as pltpu
from jax.sharding import PartitionSpec as P
ZERO, ONE, TWO, THREE, FOUR, FIVE, SIX, SEVEN, EIGHT, NINE, TEN, ELEVEN, TWELVE = range(13)
ROWS = 1024 // 64
bf=jnp.bfloat16
MESH=pl.DeviceIdType.MESH
PERM=((ZERO,ONE,TWO),(ONE,TWO,ZERO),(TWO,ZERO,ONE))

class Place:
    def __init__(self):
        i=lax.axis_index("dp")
        self.plus=[[c,*((c+d)%FOUR for d in range(ONE,FOUR))] for c in (i//ROWS,(i//FOUR)%FOUR,i%FOUR)]
        self.near=[]
        for a in range(THREE):
            c=[self.plus[b][ZERO] for b in range(THREE)]
            self.near.append([{"dp":(c[:a]+[self.plus[a][d]]+c[a+ONE:])[ZERO]*ROWS+(c[:a]+[self.plus[a][d]]+c[a+ONE:])[ONE]*FOUR+(c[:a]+[self.plus[a][d]]+c[a+ONE:])[TWO]} for d in range(FOUR)])

def coords():
    return Place()

def shifted(me,axis,d):
    return me.near[axis][d]

def peers(me,far=True):
    return [shifted(me,a,d) for a in range(THREE) for d in ((ONE,THREE,TWO) if far else (ONE,THREE))]

def barrier(me,far=True,sib=True):
    b=pltpu.get_barrier_semaphore()
    n=ZERO
    for t in peers(me,far):
        pl.semaphore_signal(b,inc=ONE,device_id=t,device_id_type=MESH); n+=ONE
    if sib:
        pl.semaphore_signal(b,inc=ONE,device_id={"rep":ONE-lax.axis_index("rep")},device_id_type=MESH); n+=ONE
    pl.semaphore_wait(b,n)

class Gather:
    NSEM=15
    def __init__(self,me,own,out,ssem,rsem,lsem,cols):
        self.me,self.own,self.out,self.ssem,self.rsem,self.lsem,self.cols=me,own,out,ssem,rsem,lsem,cols
        self.r=lax.axis_index("rep"); self.sib={"rep":ONE-self.r}
    def at(self,p,r,u,v,w):
        i=[None]*THREE
        for a,k in zip(PERM[p],(u,v,w)): i[a]=k
        return self.out.at[(r,pl.ds(*self.cols[p]),*i)]
    def copy(self,p,k,src,dst,dev):
        return pltpu.make_async_remote_copy(src_ref=src,dst_ref=dst,send_sem=self.ssem.at[p,k],recv_sem=self.rsem.at[p,k],device_id=dev,device_id_type=MESH)
    def m(self,p,k,d=ZERO): return self.me.plus[PERM[p][k]][d]
    def sent(self,p,k):
        r=self.r; u,v,w=(self.m(p,j) for j in range(THREE)); A=slice(None); lo,hi=pl.ds(ZERO,TWO),pl.ds(TWO,TWO)
        near=[self.me.near[a] for a in PERM[p]]
        if k<THREE: return self.own.at[r,pl.ds(*self.cols[p])],self.at(p,r,u,v,w),near[ZERO][(ONE,THREE,TWO)[k]]
        if k<FIVE: ref,to=self.at(p,r,A,v,w),near[ONE][(ONE,THREE)[k-THREE]]
        elif k<SEVEN: ref,to=self.at(p,r,(lo,hi)[k-FIVE],self.m(p,ONE,(THREE,ONE)[k-FIVE]),w),near[ONE][(ONE,THREE)[k-FIVE]]
        elif k<NINE: ref,to=self.at(p,r,A,A,w),near[TWO][(ONE,THREE)[k-SEVEN]]
        elif k<ELEVEN: ref,to=self.at(p,r,(lo,hi)[k-NINE],A,self.m(p,TWO,(THREE,ONE)[k-NINE])),near[TWO][(ONE,THREE)[k-NINE]]
        else: ref,to=self.at(p,r,A,A,self.m(p,TWO,(ZERO,THREE,ONE,TWO)[k-ELEVEN])),self.sib
        return ref,ref,to
    def received(self,p,k):
        r=self.r; v,w=self.m(p,ONE),self.m(p,TWO); A=slice(None); lo,hi=pl.ds(ZERO,TWO),pl.ds(TWO,TWO)
        if k<THREE: return self.at(p,r,self.m(p,ZERO,(THREE,ONE,TWO)[k]),v,w)
        if k<FIVE: return self.at(p,r,A,self.m(p,ONE,(THREE,ONE)[k-THREE]),w)
        if k<SEVEN: return self.at(p,r,(lo,hi)[k-FIVE],self.m(p,ONE,TWO),w)
        if k<NINE: return self.at(p,r,A,A,self.m(p,TWO,(THREE,ONE)[k-SEVEN]))
        if k<ELEVEN: return self.at(p,r,(lo,hi)[k-NINE],A,self.m(p,TWO,TWO))
        return self.at(p,ONE-r,A,A,self.m(p,TWO,(ZERO,THREE,ONE,TWO)[k-ELEVEN]))
    def start(self,p,k):
        s,d,dev=self.sent(p,k); self.copy(p,k,s,d,dev).start()
    def wait_send(self,p,k):
        s,d,dev=self.sent(p,k); self.copy(p,k,s,d,dev).wait_send()
    def wait_recv(self,p,k):
        ref=self.received(p,k); self.copy(p,k,ref,ref,self.sib).wait_recv()
    def local(self,p):
        return pltpu.make_async_copy(self.own.at[self.r,pl.ds(*self.cols[p])],self.at(p,self.r,*(self.m(p,j) for j in range(THREE))),self.lsem.at[p])
    def events(self):
        P3=range(THREE)
        def e0():
            for p in P3:
                self.local(p).start()
                for k in (ZERO,ONE,TWO): self.start(p,k)
        def e1():
            for p in P3:
                self.local(p).wait()
                for k in (ZERO,ONE,TWO): self.wait_recv(p,k)
                for k in (THREE,FOUR): self.start(p,k)
        def e2():
            for p in P3:
                for k in (THREE,FOUR): self.wait_recv(p,k); self.start(p,k+TWO)
        def e3():
            for p in P3:
                for k in (FIVE,SIX): self.wait_recv(p,k)
                for k in (SEVEN,EIGHT,ELEVEN): self.start(p,k)
        def e4():
            for p in P3:
                for k in (SEVEN,EIGHT): self.wait_recv(p,k); self.start(p,k+TWO); self.start(p,k+FIVE)
        def e5():
            for p in P3:
                for k in (NINE,TEN): self.wait_recv(p,k)
                self.start(p,14)
        def e6():
            for p in P3:
                for k in range(ELEVEN,15): self.wait_recv(p,k)
        return [e0,e1,e2,e3,e4,e5,e6]
    def finish(self):
        for p in range(THREE):
            for k in range(15): self.wait_send(p,k)

f32=jnp.float32

T, D, FF, LAYERS = 2048, 1024, 2816, TWO
F = 256
N_F = FF // F
M = 512
N_T = T // M
NT = (((ONE,), (ONE,)), ((), ()))
TN = (((ZERO,), (ZERO,)), ((), ()))
L = 128
C = FF // L
GU0 = (((ZERO, TWO), (TWO, TWO), (FOUR, TWO)), ((SIX, THREE), (NINE, THREE), (TWELVE, TWO)), ((14, THREE), (17, THREE), (20, TWO)))
DD = ((ZERO, FOUR), (FOUR, FOUR), (EIGHT, THREE))
GU1 = (((ZERO, FOUR), (FOUR, THREE), (SEVEN, FOUR)), ((ELEVEN, THREE), (14, FOUR), (18, FOUR)))
HBM = pl.BlockSpec(memory_space=pltpu.HBM)
VMEM = pl.BlockSpec(memory_space=pltpu.VMEM)


def dot(a, b, dims=None):
    if dims is None:
        return jnp.dot(a, b, preferred_element_type=f32)
    return lax.dot_general(a, b, dims, preferred_element_type=f32)


def norm_rows(h):
    wide = h.astype(f32)
    return (wide * lax.rsqrt(jnp.mean(wide * wide, -ONE, keepdims=True) + 1e-6)).astype(bf)


def run(events):
    for event in events:
        event()


def at_step(i, events):
    for step, functions in events.items():
        pl.when(i == step)(functools.partial(run, functions))


def pair(ref, f):
    return ref.at[pl.ds(TWO * f, TWO)]


def wide(tiles):
    return jnp.concatenate(tiles, axis=ONE)


def down_block(tiles):
    last = [wide([tiles[ROWS + TWO * g + e][FOUR * c : FOUR * c + FOUR] for c in range(FOUR) for e in (ZERO, ONE)]) for g in range(THREE)]
    return jnp.concatenate([wide(tiles[:EIGHT]), wide(tiles[EIGHT:ROWS]), *last], axis=ZERO)


def plan_forward():
    tiles = [max(n for _, n in cols) for cols in (*GU0, DD, DD, *GU1)]
    per_tile = (0.27, 0.36, 0.18, 1.43, 0.72, 0.0, 0.0)
    due = {ZERO: ZERO, ONE: TWO, TWO: SIX, THREE: N_F, FOUR: N_F + TWO, FIVE: 99, SIX: 99}
    length = [3.0] * N_F + [3.8] * (TWO * N_T)
    late = (2.7, 2.7, 2.7, 2.7, 2.7, 1.5, 0.0)
    following = [ZERO] * SEVEN
    arrives = [0.0] * SEVEN
    plan = [[] for _ in range(N_F + TWO * N_T + TWO)]
    now, link = 0.0, 0.0

    def allowed(place, k):
        e = following[k]
        if e > SIX:
            return False
        if k == ZERO:
            return True
        before = following[k - ONE]
        if place == ZERO and k > TWO:
            return False
        return before > FOUR or (before > THREE and link <= now + 1.0) if e == THREE else before > ZERO

    def run_one(place, k):
        nonlocal now, link
        e = following[k]
        now = max(now, arrives[k]) + 0.3
        plan[place].append((k, e))
        link = max(link, now) + per_tile[e] * tiles[k]
        arrives[k] = (link if e < FIVE else now) + late[e]
        following[k] = e + ONE

    for place in range(len(plan)):
        while True:
            ready = [k for k in range(SEVEN) if allowed(place, k) and arrives[k] <= now]
            if ready:
                run_one(place, ready[ZERO])
                continue
            must = [k for k in range(SEVEN) if following[k] < SEVEN and (due[k] <= place or place == len(plan) - ONE)]
            if not must:
                break
            waiting = [k for k in range(SEVEN) if allowed(place, k) and following[k] < SEVEN]
            run_one(place, min(waiting, key=lambda k: arrives[k]))
        if place < len(length):
            now += length[place]
    return plan


def forward_kernel(
    x_hbm, dy_hbm, w_gate, w_up, own_d,
    gu0, d0, gu1, gate0, up0, act0, a0, h1, a1, dact1, d1,
    x, a, big, wt, go, raw, wc, ho, dyt, own,
    ssem, rsem, csem, xsem, wsem, gsem, bsem, rawsem, hsem, asem, dsem, esem,
):
    load_x = pltpu.make_async_copy(x_hbm, x, xsem.at[ZERO])
    load_x.start()

    def own_tile(c, _):
        for layer in range(LAYERS):
            for k, w in enumerate((w_gate, w_up)):
                own[layer, k, c] = w[layer, :, pl.ds(pl.multiple_of(c * L, L), L)]
        return ZERO

    lax.fori_loop(ZERO, C, own_tile, ZERO)
    me = coords()
    barrier(me)

    def stream(k, shard, out, cols):
        g = Gather(me, shard, out, ssem.at[k], rsem.at[k], csem.at[k], cols)
        return g, g.events()

    todo = [(own.at[ZERO], gu0, cols) for cols in GU0] + [(own_d.at[n], d, DD) for n, d in enumerate((d0, d1))] + [(own.at[ONE], gu1, cols) for cols in GU1]
    streams = [stream(k, *one) for k, one in enumerate(todo)]
    plan = [[streams[k][ONE][e] for k, e in place] for place in plan_forward()]

    run(plan[ZERO][:TWO])
    load_x.wait()

    def norm0(t, _):
        rows = pl.ds(pl.multiple_of(t * M, M), M)
        a[rows, :] = norm_rows(x[rows, :])
        return ZERO

    lax.fori_loop(ZERO, N_T, norm0, ZERO)
    keep_a0 = pltpu.make_async_copy(a, a0, xsem.at[ONE])
    keep_a0.start()
    run(plan[ZERO][TWO:])

    def load_w(w, f, slot):
        return pltpu.make_async_copy(w.at[:, pl.ds(TWO * f, TWO)], wt.at[slot], wsem.at[slot])

    def put(f, slot):
        return (
            pltpu.make_async_copy(go.at[slot, ZERO], pair(gate0, f), gsem.at[slot, ZERO]),
            pltpu.make_async_copy(go.at[slot, ONE], pair(up0, f), gsem.at[slot, ONE]),
            pltpu.make_async_copy(pair(big, f), pair(act0, f), bsem.at[slot]),
        )

    def gate_up(f, events, w, finish):
        slot = lax.rem(f, TWO)
        load_w(w, f, slot).wait()

        @pl.when(f + ONE < N_F)
        def _():
            load_w(w, f + ONE, ONE - slot).start()

        finish(f, slot, [wide([wt[slot, k, e].reshape(D, L) for e in (ZERO, ONE)]) for k in (ZERO, ONE)])
        at_step(f, events)
        return ZERO

    def finish0(f, slot, w):
        @pl.when(f >= TWO)
        def _():
            for copy in put(f - TWO, slot):
                copy.wait()

        for t in range(N_T):
            rows = pl.ds(t * M, M)
            gate, up = dot(a[rows, :], w[ZERO]), dot(a[rows, :], w[ONE])
            act = (gate * jax.nn.sigmoid(gate) * up).astype(bf)
            for e in (ZERO, ONE):
                lanes = slice(L * e, L * e + L)
                go[slot, ZERO, e, rows, :] = gate[:, lanes]
                go[slot, ONE, e, rows, :] = up[:, lanes]
                big[TWO * f + e, rows, :] = act[:, lanes]
        for copy in put(f, slot):
            copy.start()

    load_raw = [pltpu.make_async_copy(d, raw, rawsem) for d in (d0, d1)]
    ev = {f: plan[ONE + f] for f in range(N_F)}
    load_w(gu0, ZERO, ZERO).start()
    lax.fori_loop(ZERO, N_F, lambda f, _: gate_up(f, ev, gu0, finish0), ZERO)
    load_raw[ZERO].start()
    for f in (N_F - TWO, N_F - ONE):
        for copy in put(f, f % TWO):
            copy.wait()
    keep_a0.wait()

    def convert():
        def four(g, _):
            blocks = [down_block([raw[c // ELEVEN, c % ELEVEN, g // FOUR, lax.rem(g, FOUR), z] for c in range(C)]) for z in range(FOUR)]
            wc[pl.ds(pl.multiple_of(176 * g, 176), 176), :] = jnp.concatenate(blocks, axis=ZERO)
            return ZERO

        lax.fori_loop(ZERO, ROWS, four, ZERO)

    load_raw[ZERO].wait()
    convert()

    def put_h(t, slot):
        return pltpu.make_async_copy(ho.at[slot], h1.at[pl.ds(pl.multiple_of(t * M, M), M)], hsem.at[slot])

    def load_dy(t, slot):
        return pltpu.make_async_copy(dy_hbm.at[pl.ds(pl.multiple_of(t * M, M), M)], dyt.at[slot], dsem.at[slot])

    def down(t, events):
        slot = lax.rem(t, TWO)

        @pl.when(t >= TWO)
        def _():
            put_h(t - TWO, slot).wait()

        rows = pl.ds(pl.multiple_of(t * M, M), M)
        h = (x[rows, :].astype(f32) + dot(wide([big[c, rows, :] for c in range(C)]), wc[...]).astype(bf).astype(f32)).astype(bf)
        ho[slot] = h
        a[rows, :] = norm_rows(h)
        put_h(t, slot).start()
        at_step(t, events)
        return ZERO

    lax.fori_loop(ZERO, N_T, lambda t, _: down(t, {ZERO: plan[ONE + N_F], ONE: [*plan[TWO + N_F], lambda: load_raw[ONE].start()], TWO: plan[THREE + N_F], THREE: plan[FOUR + N_F]}), ZERO)
    keep_a1 = pltpu.make_async_copy(a, a1, asem)
    keep_a1.start()
    load_dy(ZERO, ZERO).start()
    for t in (N_T - TWO, N_T - ONE):
        put_h(t, t % TWO).wait()
    load_raw[ONE].wait()
    convert()

    def put_dact(t):
        r = pl.ds(pl.multiple_of(t * M, M), M)
        return pltpu.make_async_copy(big.at[:, r], dact1.at[:, r], esem.at[t])

    def dact(t, events):
        slot = lax.rem(t, TWO)
        load_dy(t, slot).wait()

        @pl.when(t + ONE < N_T)
        def _():
            load_dy(t + ONE, ONE - slot).start()

        rows = pl.ds(pl.multiple_of(t * M, M), M)
        for half in (ZERO, ONE):
            v = dot(dyt[slot], wc[FF // TWO * half : FF // TWO * half + FF // TWO, :], NT).astype(bf)
            for c in range(ELEVEN):
                big[ELEVEN * half + c, rows, :] = v[:, L * c : L * c + L]
        put_dact(t).start()
        at_step(t, events)
        return ZERO

    lax.fori_loop(ZERO, N_T, lambda t, _: dact(t, {n: plan[FIVE + N_F + n] for n in range(N_T)}), ZERO)
    run(plan[-ONE])

    for t in range(N_T):
        put_dact(t).wait()
    keep_a1.wait()
    for g, _ in streams:
        g.finish()


def forward(x, dy, w_gate, w_up, own_d):
    sd = jax.ShapeDtypeStruct
    tall, tall32, narrow = sd((C, T, L), bf), sd((C, T, L), f32), sd((T, D), bf)
    blocks = sd((TWO, C, FOUR, FOUR, FOUR, ROWS, L), bf)
    half_blocks = sd((TWO, C // TWO, FOUR, FOUR, FOUR, ROWS, L), bf)
    dma = pltpu.SemaphoreType.DMA
    return pl.pallas_call(
        forward_kernel,
        in_specs=[HBM, HBM, VMEM, VMEM, VMEM],
        out_specs=[HBM] * ELEVEN,
        out_shape=[blocks, half_blocks, blocks, tall32, tall32, tall, narrow, narrow, narrow, tall, half_blocks],
        scratch_shapes=[
            pltpu.VMEM((T, D), bf), pltpu.VMEM((T, D), bf), pltpu.VMEM((C, T, L), bf),
            pltpu.VMEM((TWO, TWO, TWO, FOUR, FOUR, FOUR, ROWS, L), bf), pltpu.VMEM((TWO, TWO, TWO, T, L), f32),
            pltpu.VMEM((TWO, C // TWO, FOUR, FOUR, FOUR, ROWS, L), bf), pltpu.VMEM((FF, D), bf), pltpu.VMEM((TWO, M, D), bf),
            pltpu.VMEM((TWO, M, D), bf), pltpu.VMEM((LAYERS, TWO, C, ROWS, L), bf),
            dma((SEVEN, THREE, 15)), dma((SEVEN, THREE, 15)), dma((SEVEN, THREE)), dma((TWO,)), dma((TWO,)), dma((TWO, TWO)), dma((TWO,)), dma(()), dma((TWO,)), dma(()), dma((TWO,)), dma((FOUR,)),
        ],
        compiler_params=pltpu.CompilerParams(collective_id=ZERO, has_side_effects=True, vmem_limit_bytes=63 * TWO**20),
        name="forward",
    )(x, dy, w_gate, w_up, own_d)[:TEN]


HALF = FF // TWO
PARTS = ((ZERO, FOUR), (FOUR, FOUR), (EIGHT, THREE))
UNITS = TWELVE


class Scatter:
    @staticmethod
    def vw(p, v, w):
        return (slice(None), v, w) if PERM[p][ONE] < PERM[p][TWO] else (slice(None), w, v)

    @staticmethod
    def scratch():
        s = []
        for p, (_, n) in enumerate(PARTS):
            _, *h = Scatter.vw(p, TWO, FOUR)
            s += [
                pltpu.VMEM((TWO, SIX, n, *h, ROWS, L), bf),
                pltpu.VMEM((TWO, FOUR, n, *h, ROWS, L), bf),
                pltpu.VMEM((n, FOUR, FOUR, ROWS, L), f32), pltpu.VMEM((n, FOUR, FOUR, ROWS, L), bf),
                pltpu.VMEM((SIX, n, TWO, ROWS, L), bf), pltpu.VMEM((TWO, n, TWO, ROWS, L), bf),
                pltpu.VMEM((n, FOUR, ROWS, L), f32), pltpu.VMEM((n, FOUR, ROWS, L), bf),
                pltpu.VMEM((THREE, n, ROWS, L), bf),
            ]
        dma = pltpu.SemaphoreType.DMA
        regular = pltpu.SemaphoreType.REGULAR
        return s + [pltpu.VMEM((ROWS, FF // TWO), bf), dma((TWO, THREE, 15)), dma((TWO, THREE, 15)), dma((TWO, THREE, FOUR)), dma(()), regular((THREE, TWO)), regular((THREE, TWO)), regular((THREE, THREE))]

    def __init__(self, me, grads, out, bufs):
        self.me, self.grads, self.out = me, grads, out
        self.b = [bufs[NINE * p : NINE * p + NINE] for p in range(THREE)]
        self.res, self.ssem, self.rsem, self.lsem, self.osem, self.credit1, self.credit2, self.credit3 = bufs[27:]

    def m(self, p, k, d=ZERO):
        return self.me.plus[PERM[p][k]][d]

    def at_unit(self, k):
        self.k, self.slot = k, lax.rem(k, TWO)
        odd = lax.rem(k, TWO)
        self.grad = jnp.where(k < FOUR, ONE + odd, jnp.where(k < SIX, ZERO, jnp.where(k < EIGHT, THREE, k // TWO)))
        self.col0 = C // TWO * jnp.where(k < FOUR, k // TWO, odd)

    def cols(self, p):
        c, n = PARTS[p]
        return pl.ds(self.col0 + c, n)

    def term(self, p, u, half):
        i = [None] * THREE
        a, v, w = PERM[p]
        i[a], i[v], i[w] = u, pl.ds(TWO * half, TWO), slice(None)
        return self.grads.at[(self.grad, self.cols(p), *i)]

    def own(self, p, j):
        u, h = ((ONE, ZERO), (THREE, ONE), (ZERO, ZERO), (ZERO, ONE))[j]
        return pltpu.make_async_copy(self.term(p, self.m(p, ZERO, u), h), self.b[p][ONE].at[self.slot, j], self.lsem.at[self.slot, p, j])

    def cp(self, p, k):
        b, s = self.b[p], self.slot
        if k < SIX:
            ax, d = ZERO, (ONE, THREE, ONE, THREE, ONE, THREE)[k]
            if k < FOUR:
                u, h = ((TWO, ZERO), (TWO, ONE), (ONE, ONE), (THREE, ZERO))[k]
                src = self.term(p, self.m(p, ZERO, u), h)
            else:
                src = b[ONE].at[s, k - FOUR]
            dst = b[ZERO].at[s, k]
        elif k < TWELVE:
            j = k - SIX
            ax, d = ONE, (ONE, THREE, ONE, THREE, ONE, THREE)[j]
            if j < FOUR:
                v, h = ((TWO, ZERO), (TWO, ONE), (ONE, ONE), (THREE, ZERO))[j]
                src = b[THREE].at[self.vw(p, self.m(p, ONE, v), pl.ds(TWO * h, TWO))]
            else:
                src = b[FIVE].at[j - FOUR]
            dst, s = b[FOUR].at[j], ZERO
        else:
            ax, d = TWO, (ONE, THREE, TWO)[k - TWELVE]
            src, dst, s = b[SEVEN].at[:, self.m(p, TWO, d)], b[EIGHT].at[k - TWELVE], ZERO
        return pltpu.make_async_remote_copy(
            src_ref=src, dst_ref=dst, send_sem=self.ssem.at[s, p, k], recv_sem=self.rsem.at[s, p, k],
            device_id=shifted(self.me, PERM[p][ax], d), device_id_type=MESH,
        )

    def give(self, credit, axis, last):
        @pl.when(self.k < last)
        def _():
            for p in range(THREE):
                for j, d in enumerate((THREE, ONE, TWO)[: credit.shape[ONE]]):
                    pl.semaphore_signal(credit.at[p, j], inc=ONE, device_id=shifted(self.me, PERM[p][axis], d), device_id_type=MESH)

    def take(self, credit, first):
        @pl.when(self.k >= first)
        def _():
            for p in range(THREE):
                for j in range(credit.shape[ONE]):
                    pl.semaphore_wait(credit.at[p, j], ONE)

    def begin(self):
        self.take(self.credit1, TWO)
        for k in (ZERO, ONE, TWO, THREE):
            for p in range(THREE):
                self.cp(p, k).start()
        for p in range(THREE):
            for j in range(FOUR):
                self.own(p, j).start()

    def pass_on(self):
        s = self.slot
        for p in range(THREE):
            b = self.b[p]
            for k in (ZERO, ONE):
                self.own(p, k).wait()
                self.cp(p, k).wait_recv()
                for n in range(PARTS[p][ONE]):
                    b[ONE][s, k, n] = (b[ZERO][s, k, n].astype(f32) + b[ONE][s, k, n].astype(f32)).astype(bf)
        for k in (FOUR, FIVE):
            for p in range(THREE):
                self.cp(p, k).start()

    def first_sum(self):
        s = self.slot
        for p in range(THREE):
            b = self.b[p]
            for k in (TWO, THREE, FOUR, FIVE):
                self.cp(p, k).wait_recv()
            for j in (TWO, THREE):
                self.own(p, j).wait()
            for half in (ZERO, ONE):
                own, sums, raw = ((TWO, FOUR, THREE), (THREE, FIVE, TWO))[half]
                _, *ix = self.vw(p, slice(TWO * half, TWO * half + TWO), slice(None))
                for n in range(PARTS[p][ONE]):
                    t = b[ONE][s, own, n].astype(f32) + b[ZERO][s, sums, n].astype(f32) + b[ZERO][s, raw, n].astype(f32)
                    b[TWO][(n, *ix)] = t
                    b[THREE][(n, *ix)] = t.astype(bf)
        for p in range(THREE):
            for k in range(SIX):
                self.cp(p, k).wait_send()
        self.give(self.credit1, ZERO, UNITS - TWO)
        self.take(self.credit2, ONE)
        for k in (SIX, SEVEN, EIGHT, NINE):
            for p in range(THREE):
                self.cp(p, k).start()

    def pass_on2(self):
        for p in range(THREE):
            b = self.b[p]
            for half in (ZERO, ONE):
                self.cp(p, SIX + half).wait_recv()
                v = self.m(p, ONE, (ONE, THREE)[half])
                own = b[TWO][self.vw(p, v, slice(TWO * half, TWO * half + TWO))]
                b[FIVE][half] = (b[FOUR][half].astype(f32) + own).astype(bf)
        for k in (TEN, ELEVEN):
            for p in range(THREE):
                self.cp(p, k).start()

    def second_sum(self):
        for p in range(THREE):
            b, v = self.b[p], self.m(p, ONE)
            for k in (EIGHT, NINE, TEN, ELEVEN):
                self.cp(p, k).wait_recv()
            for half in (ZERO, ONE):
                sums, raw = ((FOUR, THREE), (FIVE, TWO))[half]
                part = slice(TWO * half, TWO * half + TWO)
                t = b[TWO][self.vw(p, v, part)] + b[FOUR][sums].astype(f32) + b[FOUR][raw].astype(f32)
                b[SIX][:, part] = t
                b[SEVEN][:, part] = t.astype(bf)
        for p in range(THREE):
            for k in range(SIX, TWELVE):
                self.cp(p, k).wait_send()
        self.give(self.credit2, ONE, UNITS - ONE)
        self.take(self.credit3, ONE)
        for k in (TWELVE, 13, 14):
            for p in range(THREE):
                self.cp(p, k).start()

    def total(self):
        for p in range(THREE):
            b, w = self.b[p], self.m(p, TWO)
            for k in (TWELVE, 13, 14):
                self.cp(p, k).wait_recv()
            t = b[SIX][:, w]
            for j in range(THREE):
                t = t + b[EIGHT][j].astype(f32)
            c, n = PARTS[p]
            for q in range(n):
                self.res[:, L * (c + q) : L * (c + q) + L] = t[q].astype(bf)
        layer, kind = ONE - self.grad // THREE, lax.rem(self.grad, THREE)
        for m, out in enumerate(self.out):

            @pl.when(kind == m)
            def _():
                pltpu.make_async_copy(self.res, out.at[layer, :, pl.ds(pl.multiple_of(self.col0 * L, L), FF // TWO)], self.osem).start()

        for p in range(THREE):
            for k in (TWELVE, 13, 14):
                self.cp(p, k).wait_send()
        self.give(self.credit3, TWO, UNITS - ONE)
        pltpu.make_async_copy(self.res, self.out[ZERO].at[ZERO, :, pl.ds(ZERO, FF // TWO)], self.osem).wait()

    def tick(self, j, plan):
        def due(steps):
            words = [sum(ONE << (n - 30 * w) for n in steps if n // 30 == w) for w in range(max(plan["total"]) // 30 + ONE)]
            word = functools.reduce(lambda have, w: jnp.where(j >= 30 * w, words[w], have), range(ONE, len(words)), words[ZERO])
            return (lax.shift_right_logical(jnp.int32(word), lax.rem(j, 30)) & ONE) == ONE

        @pl.when(due({n for steps in plan.values() for n in steps}))
        def _():
            for event in (self.total, self.second_sum, self.pass_on2, self.first_sum, self.pass_on, self.begin):
                steps = plan[event.__name__]

                @pl.when(due(steps))
                def _():
                    self.at_unit(sum(jnp.where(j > n, ONE, ZERO) for n in steps))
                    event()


S1, S2, S3, S6, S5, S7, S8, S9, TAIL = ZERO, ELEVEN, 19, 35, 43, 51, 63, 74, 90


def make_plan():
    length = [5.1] * ELEVEN + [2.2] * EIGHT + [1.95] * ROWS + [2.2] * EIGHT + [2.1] * EIGHT + [2.4] * TWELVE + [1.4] * ELEVEN + [1.95] * ROWS
    ready = [SEVEN, SEVEN, S2 + ONE, S2 + ONE, S3 + ONE, S3 + ONE, S5 + ONE, S5 + ONE, S7 + SEVEN, S8 + ONE, S8 + SEVEN, S9 + ONE]
    names = ("begin", "pass_on", "first_sum", "pass_on2", "second_sum", "total")
    sends = (6.1, 3.05, 1.6, 0.8, 1.1, 0.0)
    late = 2.5
    plan = {name: [] for name in names}
    arrives = [[0.0] * SEVEN for _ in range(UNITS)]
    now, link, step = 3.0, 0.0, ZERO

    def may_run(e, k):
        n = len(plan[names[e]])
        if n != k or (plan[names[e]] and plan[names[e]][-ONE] == step):
            return False
        if e == ZERO:
            return step >= ready[k] and (k < TWO or len(plan["first_sum"]) > k - TWO)
        if len(plan[names[e - ONE]]) <= k or plan[names[e - ONE]][k] == step:
            return False
        if e == TWO and len(plan["second_sum"]) < k:
            return False
        return not (e == FOUR and len(plan["total"]) < k)

    while len(plan["total"]) < UNITS:
        ran = False
        for e in (FIVE, FOUR, THREE, TWO, ONE, ZERO):
            k = len(plan[names[e]])
            if k < UNITS and may_run(e, k) and (arrives[k][e] <= now or step >= TAIL):
                if step >= TAIL and arrives[k][e] > now:
                    if ran or any(may_run(o, len(plan[names[o]])) and arrives[len(plan[names[o]])][o] < arrives[k][e] for o in range(SIX) if o != e and len(plan[names[o]]) < UNITS):
                        continue
                    now = arrives[k][e]
                plan[names[e]].append(step)
                ran = True
                now += 0.35
                link = max(link, now) + sends[e]
                if e == ZERO:
                    arrives[k][ONE], arrives[k][TWO] = link - sends[ONE] + late, link + late
                elif e < FIVE:
                    arrives[k][e + ONE] = max(arrives[k][e + ONE], link + late)
        now += length[step] if step < TAIL else 0.05
        step += ONE
    return plan


PLAN = make_plan()
N_STEPS = max(PLAN["total"]) + ONE


def backward_kernel(
    x, dy, gu0, d0, gu1, gate0, up0, act0, a0, h1, a1, dact1,
    dx, by_down, by_gate, by_up, grads, dup1,
    am, dh, r1, r2, r3, stg, tl, ob, gl, ht,
    lsem, r1sem, r2sem, r3sem, amsem, wsem, dasem, tlsem, obsem, glsem, flsem, hsem, dxsem, *bufs,
):
    me = coords()
    barrier(me, sib=False)
    scatter = Scatter(me, grads, (by_down, by_gate, by_up), bufs)

    def rows(t, n=M):
        return pl.ds(pl.multiple_of(t * n, n), n)

    def col(f, n=F):
        return pl.ds(pl.multiple_of(f * n, 128), n)

    load_dh = pltpu.make_async_copy(dy, dh, lsem)
    load_dup = pltpu.make_async_copy(dup1, r1, r1sem)
    load_act = pltpu.make_async_copy(act0, r2, r2sem)

    def load_am(src):
        return pltpu.make_async_copy(src, am, amsem)

    def load_wt(f, slot):
        return [
            pltpu.make_async_copy(gu1.at[k, pl.ds(TWO * f, TWO), pl.ds(TWO * h, TWO)], stg.at[pl.ds(EIGHT * slot + FOUR * k + TWO * h, TWO)], wsem.at[slot, k, h])
            for k in (ZERO, ONE) for h in (ZERO, ONE)
        ]

    def load_dact(f, slot):
        return pltpu.make_async_copy(pair(dact1, f), pair(r1, f), dasem.at[slot])

    def load_r3(src, h):
        return pltpu.make_async_copy(src.at[:, pl.ds(TWO * h, TWO)], r3.at[:, pl.ds(TWO * h, TWO)], r3sem.at[h])

    def flush(grad, half):
        return pltpu.make_async_copy(stg, grads.at[grad, :, pl.ds(TWO * half, TWO)], flsem)

    def put_tl(f, slot):
        return pltpu.make_async_copy(tl.at[slot], pair(dup1, f), tlsem.at[slot])

    def put_ob(grad, f, slot, kinds=(ZERO, ONE)):
        return [pltpu.make_async_copy(ob.at[slot, k], grads.at[grad + k, pl.ds(TWO * f, TWO)], obsem.at[slot, k]) for k in kinds]

    def load_gl(f, e):
        return [pltpu.make_async_copy(src.at[TWO * f + e], gl.at[e, k], glsem.at[e, k]) for k, src in enumerate((gate0, up0))]

    def load_h(src, t):
        return pltpu.make_async_copy(src.at[rows(t)], ht, hsem)

    def put_dx(t):
        return pltpu.make_async_copy(dh.at[rows(t)], dx.at[rows(t)], dxsem.at[t])

    def go(copies):
        for c in copies:
            c.start()

    def done(copies):
        for c in copies:
            c.wait()

    def when(condition, f):
        pl.when(condition)(f)

    def gate_up_grad(slot, tiles, parts=(ZERO, FOUR), kinds=(ZERO, ONE)):
        lo, hi = parts
        v = dot(am[:, F * lo : F * hi], wide(tiles), TN).astype(bf)
        for n, k in enumerate(kinds):
            for e in (ZERO, ONE):
                ob[slot, k, e, lo:hi] = v[:, F * n + L * e : F * n + L * e + L].reshape(hi - lo, FOUR, FOUR, ROWS, L)

    def layer1(f, slot):
        w = []
        for k in (ZERO, ONE):
            halves = [wide([stg[EIGHT * slot + FOUR * k + TWO * h + e].reshape(D // TWO, L) for e in (ZERO, ONE)]) for h in (ZERO, ONE)]
            w.append(jnp.concatenate(halves, axis=ZERO))
        for t in range(N_T):
            r = pl.ds(t * M, M)
            gate, up = dot(am[r, :], w[ZERO]), dot(am[r, :], w[ONE])
            by_act = wide([r1[TWO * f + e, r, :] for e in (ZERO, ONE)]).astype(f32)
            sig = jax.nn.sigmoid(gate)
            silu = gate * sig
            act, by_gate, by_up = silu * up, by_act * up * (sig + silu * (ONE - sig)), by_act * silu
            for e in (ZERO, ONE):
                lanes = slice(L * e, L * e + L)
                r1[TWO * f + e, r, :] = act[:, lanes].astype(bf)
                r2[TWO * f + e, r, :] = by_gate[:, lanes].astype(bf)
                tl[slot, e, r, :] = by_up[:, lanes].astype(bf)
        gate_up_grad(slot, [r2[TWO * f], r2[TWO * f + ONE], tl[slot, ZERO], tl[slot, ONE]])

    def down_grad(s, src, grad):
        half, c = s // FOUR, lax.rem(s, FOUR)
        lhs = wide([src[C // TWO * half + i] for i in range(C // TWO)])
        am[: FF // TWO, :F] = dot(lhs, dh[:, col(c)], TN).astype(bf)
        when(s == FOUR, lambda: flush(grad, ZERO).wait())
        lanes = [slice(L * e, L * e + L) for e in (ZERO, ONE)]

        def four(g, _):
            v = am[pl.ds(pl.multiple_of(176 * g, 176), 176), :F]
            x, y = g // FOUR, lax.rem(g, FOUR)
            for z in range(FOUR):
                for e in (ZERO, ONE):
                    stg[TWO * c + e, x, y, z] = v[44 * z : 44 * z + ROWS, lanes[e]]
                    stg[EIGHT + TWO * c + e, x, y, z] = v[44 * z + ROWS : 44 * z + 32, lanes[e]]
            for k in range(FOUR):

                @pl.when(c == k)
                def _():
                    for z in range(FOUR):
                        for n in range(THREE):
                            for e in (ZERO, ONE):
                                stg[ROWS + TWO * n + e, x, y, z, FOUR * k : FOUR * k + FOUR] = v[44 * z + 32 + FOUR * n : 44 * z + 36 + FOUR * n, lanes[e]]

            return ZERO

        lax.fori_loop(ZERO, EIGHT, four, ZERO)
        for h in (ZERO, ONE):
            when(s == FOUR * h + THREE, lambda: flush(grad, h).start())

    def silu_back(f, e, t):
        for q in range(t * M, t * M + M, L):
            r = slice(q, q + L)
            gate, up, by_act = gl[e, ZERO, r, :], gl[e, ONE, r, :], r1[TWO * f + e, r, :].astype(f32)
            sig = jax.nn.sigmoid(gate)
            silu = gate * sig
            r2[TWO * f + e, r, :] = (by_act * up * (sig + silu * (ONE - sig))).astype(bf)
            r1[TWO * f + e, r, :] = (by_act * silu).astype(bf)

    def by_input(src, n, t):
        w = wide([r3[c, pl.ds(TWO * n, TWO)].reshape(D // TWO, L) for c in range(C)])
        return dot(wide([src[c, rows(t), :] for c in range(C)]), w, NT).astype(bf)

    def norm_back(t):
        h = ht[...].astype(f32)
        by_a = am[rows(t), :].astype(f32)
        scale = lax.rsqrt(jnp.mean(h * h, -ONE, keepdims=True) + 1e-6)
        by_wide = scale * by_a - h * (scale * scale * scale * jnp.mean(h * by_a, -ONE, keepdims=True))
        dh[rows(t), :] = (dh[rows(t), :].astype(f32) + by_wide.astype(bf).astype(f32)).astype(bf)

    def down_rows(half):
        def four(g, _):
            blocks = [down_block([r3[c, TWO * half + g // FOUR, lax.rem(g, FOUR), z] for c in range(C)]) for z in range(FOUR)]
            am[pl.ds(pl.multiple_of(176 * g, 176), 176), :] = jnp.concatenate(blocks, axis=ZERO)
            return ZERO

        lax.fori_loop(ZERO, EIGHT, four, ZERO)

    def step(j, _):
        def within(a, b):
            return (j >= a) & (j < b)

        in1, in2, in3 = j < S2, within(S2, S3), within(S3, S6)
        in6, in5, in7, in8, in9 = within(S6, S5), within(S5, S7), within(S7, S8), within(S8, S9), within(S9, TAIL)

        @pl.when(in1)
        def _():
            f = j - S1
            slot = lax.rem(f, TWO)

            @pl.when(f >= TWO)
            def _():
                done(put_ob(ONE, f - TWO, slot))
                put_tl(f - TWO, slot).wait()

            done(load_wt(f, slot))
            load_dact(f, slot).wait()

            @pl.when(f + ONE < N_F)
            def _():
                go(load_wt(f + ONE, ONE - slot))
                load_dact(f + ONE, ONE - slot).start()

            when(f == TWO, lambda: go([load_r3(gu1.at[ZERO], h) for h in (ZERO, ONE)]))

        @pl.when(in2)
        def _():
            @pl.when(j == S2)
            def _():
                done(put_ob(ONE, N_F - TWO, ONE))
                put_tl(N_F - TWO, ONE).wait()
                load_dh.wait()

            @pl.when(j == S2 + ONE)
            def _():
                done(put_ob(ONE, N_F - ONE, ZERO))
                put_tl(N_F - ONE, ZERO).wait()

        def input_pre(s, w, src):
            when(s == ZERO, lambda: load_r3(w.at[ZERO], ZERO).wait())

            @pl.when(s == FOUR)
            def _():
                load_r3(w.at[ZERO], ONE).wait()
                load_r3(w.at[ONE], ZERO).start()

            @pl.when(s == EIGHT)
            def _():
                load_r3(w.at[ONE], ZERO).wait()
                load_r3(w.at[ONE], ONE).start()

            when(s == ELEVEN, lambda: load_h(src, ZERO).start())
            when(s == TWELVE, lambda: load_r3(w.at[ONE], ONE).wait())

        @pl.when(in3)
        def _():
            s = j - S3
            input_pre(s, gu1, h1)
            when(s == ZERO, lambda: load_dup.start())
            when(s == ONE, lambda: flush(ZERO, ONE).wait())

            @pl.when(s == EIGHT)
            def _():
                load_dup.wait()
                load_act.start()

            when(s == TWELVE, lambda: load_r3(d0, ZERO).start())

        @pl.when(in9)
        def _():
            s = j - S9
            input_pre(s, gu0, x)
            when(s == ZERO, lambda: done(put_ob(FOUR, N_F - TWO, ONE, (ONE,))))
            when(s == ONE, lambda: done(put_ob(FOUR, N_F - ONE, ZERO, (ONE,))))

        @pl.when(j == S6)
        def _():
            load_act.wait()
            load_r3(d0, ONE).start()

        @pl.when(in5)
        def _():
            s = j - S5

            @pl.when(s == ZERO)
            def _():
                load_r3(d0, ZERO).wait()
                go(load_gl(ZERO, ZERO) + load_gl(ZERO, ONE))

            @pl.when(s == ONE)
            def _():
                flush(THREE, ONE).wait()
                load_r3(gu0.at[ZERO], ZERO).start()

            when(s == FOUR, lambda: load_r3(d0, ONE).wait())
            when(s == FIVE, lambda: load_r3(gu0.at[ZERO], ONE).start())

        @pl.when(in7)
        def _():
            when(j == S7 + ONE, lambda: load_am(a0).wait())
            i = j - S7
            when((i >= THREE) & (i != EIGHT), lambda: done(put_ob(FOUR, i - THREE, lax.rem(i - THREE, TWO), (ZERO,))))
            when(i == SEVEN, lambda: done(put_ob(FOUR, FIVE, ONE, (ZERO,))))

        @pl.when(in8)
        def _():
            f = j - S8
            when(f == ZERO, lambda: done(put_ob(FOUR, N_F - TWO, ONE, (ZERO,))))
            when(f == ONE, lambda: done(put_ob(FOUR, N_F - ONE, ZERO, (ZERO,))))
            when(f >= TWO, lambda: done(put_ob(FOUR, f - TWO, lax.rem(f, TWO), (ONE,))))

        scatter.tick(j, PLAN)

        @pl.when(in1)
        def _():
            f = j - S1
            slot = lax.rem(f, TWO)
            layer1(f, slot)
            go(put_ob(ONE, f, slot))
            put_tl(f, slot).start()

        when(in2, lambda: down_grad(j - S2, r1, ZERO))
        when(in6, lambda: down_grad(j - S6, r2, THREE))

        @pl.when(in3 | in9)
        def _():
            s = jnp.where(in3, j - S3, j - S9)
            n, t = lax.rem(s, EIGHT) // FOUR, lax.rem(s, FOUR)
            here = (rows(t), col(n, D // TWO))

            def more():
                am[here] = (am[here].astype(f32) + by_input(r1, n, t).astype(f32)).astype(bf)

            @pl.when(s < EIGHT)
            def _():
                am[here] = by_input(r2, n, t)

            when((s >= EIGHT) & (s < 13), more)

            @pl.when(s >= 13)
            def _():
                load_h(h1, t - ONE).wait()
                norm_back(t - ONE)
                more()
                when(in3, lambda: load_h(h1, t).start())
                when(in9, lambda: load_h(x, t).start())
                when(in9, lambda: put_dx(t - ONE).start())

            @pl.when(s == 15)
            def _():
                load_h(h1, THREE).wait()
                norm_back(THREE)
                when(in9, lambda: put_dx(THREE).start())

        @pl.when(in5)
        def _():
            s = j - S5
            half, t = s // FOUR, lax.rem(s, FOUR)
            when(t == ZERO, lambda: down_rows(half))
            v = dot(dh[rows(t), :], am[: FF // TWO, :], NT).astype(bf)
            for c in range(C // TWO):
                r1[C // TWO * half + c, rows(t), :] = v[:, L * c : L * c + L]
            when(s == SEVEN, lambda: load_am(a0).start())

        @pl.when(in7)
        def _():
            i = j - S7
            before = i - ONE
            slot = lax.rem(i + ONE, TWO)
            tiles = lambda: [r2[TWO * before], r2[TWO * before + ONE]]

            @pl.when(i == ZERO)
            def _():
                for e in (ZERO, ONE):
                    done(load_gl(ZERO, e))
                    for t in range(FOUR):
                        silu_back(ZERO, e, t)
                    go(load_gl(ONE, e))

            @pl.when((i > ZERO) & (i < N_F))
            def _():
                for e in (ZERO, ONE):
                    done(load_gl(i, e))
                    for t in (ZERO, ONE):
                        gate_up_grad(slot, tiles(), (TWO * e + t, TWO * e + t + ONE), (ZERO,))
                        silu_back(i, e, TWO * t)
                        silu_back(i, e, TWO * t + ONE)
                    when(i + ONE < N_F, lambda: go(load_gl(i + ONE, e)))

            when(i == N_F, lambda: gate_up_grad(slot, tiles(), (ZERO, FOUR), (ZERO,)))
            when(i > ZERO, lambda: go(put_ob(FOUR, before, slot, (ZERO,))))

        @pl.when(in8)
        def _():
            f = j - S8
            slot = lax.rem(f, TWO)
            gate_up_grad(slot, [r1[TWO * f], r1[TWO * f + ONE]], (ZERO, FOUR), (ONE,))
            go(put_ob(FOUR, f, slot, (ONE,)))

        return ZERO

    load_am(a1).start()
    go(load_wt(ZERO, ZERO))
    load_dact(ZERO, ZERO).start()
    load_dh.start()
    load_am(a1).wait()
    lax.fori_loop(ZERO, N_STEPS, step, ZERO)
    done([put_dx(t) for t in range(FOUR)])


def backward(x, dy, gu0, d0, *args):
    sd = jax.ShapeDtypeStruct
    dma = pltpu.SemaphoreType.DMA
    return pl.pallas_call(
        backward_kernel,
        in_specs=[HBM] * TWELVE,
        out_specs=[HBM] * SIX,
        out_shape=[sd((T, D), bf), *[sd((LAYERS, ROWS, FF), bf)] * THREE, sd((SIX, C, FOUR, FOUR, FOUR, ROWS, L), bf), sd((C, T, L), bf)],
        scratch_shapes=[
            pltpu.VMEM((T, D), bf), pltpu.VMEM((T, D), bf), pltpu.VMEM((C, T, L), bf), pltpu.VMEM((C, T, L), bf),
            pltpu.VMEM((C, FOUR, FOUR, FOUR, ROWS, L), bf), pltpu.VMEM((C, TWO, FOUR, FOUR, ROWS, L), bf), pltpu.VMEM((TWO, TWO, T, L), bf),
            pltpu.VMEM((TWO, TWO, TWO, FOUR, FOUR, FOUR, ROWS, L), bf), pltpu.VMEM((TWO, TWO, T, L), f32), pltpu.VMEM((M, D), bf),
            dma(()), dma(()), dma(()), dma((TWO,)), dma(()), dma((TWO, TWO, TWO)), dma((TWO,)), dma((TWO,)), dma((TWO, TWO)), dma((TWO, TWO)), dma(()), dma(()), dma((FOUR,)),
            *Scatter.scratch(),
        ],
        compiler_params=pltpu.CompilerParams(collective_id=ONE, has_side_effects=True, vmem_limit_bytes=63 * TWO**20 + 900 * 1024),
        name="backward",
    )(x, dy, gu0, d0.reshape(C, FOUR, FOUR, FOUR, ROWS, L), *args)[:FOUR]


def pack_down(t):
    first = t[:, :32].reshape(-ONE, TWO, ROWS, EIGHT, L).transpose(ZERO, ONE, THREE, TWO, FOUR).reshape(-ONE, ROWS, ROWS, L)
    last = t[:, 32:].reshape(-ONE, THREE, FOUR, FOUR, TWO, L).transpose(ZERO, ONE, FOUR, THREE, TWO, FIVE).reshape(-ONE, SIX, ROWS, L)
    return jnp.concatenate([first, last], axis=ONE).reshape(-ONE, TWO, C // TWO, ROWS, L)


def unpack_down(t):
    last = t[:, :, TWO * D :].reshape(-ONE, FOUR, FOUR, THREE, F).transpose(ZERO, THREE, TWO, ONE, FOUR).reshape(-ONE, TWELVE, D)
    return jnp.concatenate([t[:, :, :D], t[:, :, D : TWO * D], last], axis=ONE)


def solution(mesh):
    def device(x, dy, w_gate, w_up, w_down):
        x, dy = x[ZERO], dy[ZERO]
        own_d = pack_down(w_down)
        gu0, d0, gu1, *rest = forward(x, dy, w_gate, w_up, own_d)
        by_x, by_down, by_gate, by_up = backward(x, dy, gu0, d0, gu1, *rest)
        return by_x[None], by_gate, by_up, unpack_down(by_down)

    return jax.shard_map(
        device,
        mesh=mesh,
        in_specs=(P(("rep", "dp")), P(("rep", "dp")), *(P(None, "dp"),) * THREE),
        out_specs=(P(("rep", "dp")), *(P("rep", "dp"),) * THREE),
        check_vma=False,
    )
```

```python
import functools
import jax, jax.numpy as jnp
from jax import lax
from jax.experimental import pallas as pl
from jax.experimental.pallas import tpu as pltpu
from jax.sharding import PartitionSpec as P
ZERO, ONE, TWO, THREE, FOUR, FIVE, SIX, SEVEN, EIGHT, NINE, TEN, ELEVEN, TWELVE = range(13)
ROWS = 1024 // 64
bf=jnp.bfloat16
MESH=pl.DeviceIdType.MESH
PERM=((ZERO,ONE,TWO),(ONE,TWO,ZERO),(TWO,ZERO,ONE))

class Place:
    def __init__(self):
        i=lax.axis_index("dp")
        self.plus=[[c,*((c+d)%FOUR for d in range(ONE,FOUR))] for c in (i//ROWS,(i//FOUR)%FOUR,i%FOUR)]
        self.near=[]
        for a in range(THREE):
            c=[self.plus[b][ZERO] for b in range(THREE)]
            self.near.append([{"dp":(c[:a]+[self.plus[a][d]]+c[a+ONE:])[ZERO]*ROWS+(c[:a]+[self.plus[a][d]]+c[a+ONE:])[ONE]*FOUR+(c[:a]+[self.plus[a][d]]+c[a+ONE:])[TWO]} for d in range(FOUR)])

def coords():
    return Place()

def shifted(me,axis,d):
    return me.near[axis][d]

def peers(me,far=True):
    return [shifted(me,a,d) for a in range(THREE) for d in ((ONE,THREE,TWO) if far else (ONE,THREE))]

def barrier(me,far=True,sib=True):
    b=pltpu.get_barrier_semaphore()
    n=ZERO
    for t in peers(me,far):
        pl.semaphore_signal(b,inc=ONE,device_id=t,device_id_type=MESH); n+=ONE
    if sib:
        pl.semaphore_signal(b,inc=ONE,device_id={"rep":ONE-lax.axis_index("rep")},device_id_type=MESH); n+=ONE
    pl.semaphore_wait(b,n)

class Gather:
    NSEM=15
    def __init__(self,me,own,out,ssem,rsem,lsem,cols):
        self.me,self.own,self.out,self.ssem,self.rsem,self.lsem,self.cols=me,own,out,ssem,rsem,lsem,cols
        self.r=lax.axis_index("rep"); self.sib={"rep":ONE-self.r}
    def at(self,p,r,u,v,w):
        i=[None]*THREE
        for a,k in zip(PERM[p],(u,v,w)): i[a]=k
        return self.out.at[(r,pl.ds(*self.cols[p]),*i)]
    def copy(self,p,k,src,dst,dev):
        return pltpu.make_async_remote_copy(src_ref=src,dst_ref=dst,send_sem=self.ssem.at[p,k],recv_sem=self.rsem.at[p,k],device_id=dev,device_id_type=MESH)
    def m(self,p,k,d=ZERO): return self.me.plus[PERM[p][k]][d]
    def sent(self,p,k):
        r=self.r; u,v,w=(self.m(p,j) for j in range(THREE)); A=slice(None); lo,hi=pl.ds(ZERO,TWO),pl.ds(TWO,TWO)
        near=[self.me.near[a] for a in PERM[p]]
        if k<THREE: return self.own.at[r,pl.ds(*self.cols[p])],self.at(p,r,u,v,w),near[ZERO][(ONE,THREE,TWO)[k]]
        if k<FIVE: ref,to=self.at(p,r,A,v,w),near[ONE][(ONE,THREE)[k-THREE]]
        elif k<SEVEN: ref,to=self.at(p,r,(lo,hi)[k-FIVE],self.m(p,ONE,(THREE,ONE)[k-FIVE]),w),near[ONE][(ONE,THREE)[k-FIVE]]
        elif k<NINE: ref,to=self.at(p,r,A,A,w),near[TWO][(ONE,THREE)[k-SEVEN]]
        elif k<ELEVEN: ref,to=self.at(p,r,(lo,hi)[k-NINE],A,self.m(p,TWO,(THREE,ONE)[k-NINE])),near[TWO][(ONE,THREE)[k-NINE]]
        else: ref,to=self.at(p,r,A,A,self.m(p,TWO,(ZERO,THREE,ONE,TWO)[k-ELEVEN])),self.sib
        return ref,ref,to
    def received(self,p,k):
        r=self.r; v,w=self.m(p,ONE),self.m(p,TWO); A=slice(None); lo,hi=pl.ds(ZERO,TWO),pl.ds(TWO,TWO)
        if k<THREE: return self.at(p,r,self.m(p,ZERO,(THREE,ONE,TWO)[k]),v,w)
        if k<FIVE: return self.at(p,r,A,self.m(p,ONE,(THREE,ONE)[k-THREE]),w)
        if k<SEVEN: return self.at(p,r,(lo,hi)[k-FIVE],self.m(p,ONE,TWO),w)
        if k<NINE: return self.at(p,r,A,A,self.m(p,TWO,(THREE,ONE)[k-SEVEN]))
        if k<ELEVEN: return self.at(p,r,(lo,hi)[k-NINE],A,self.m(p,TWO,TWO))
        return self.at(p,ONE-r,A,A,self.m(p,TWO,(ZERO,THREE,ONE,TWO)[k-ELEVEN]))
    def start(self,p,k):
        s,d,dev=self.sent(p,k); self.copy(p,k,s,d,dev).start()
    def wait_send(self,p,k):
        s,d,dev=self.sent(p,k); self.copy(p,k,s,d,dev).wait_send()
    def wait_recv(self,p,k):
        ref=self.received(p,k); self.copy(p,k,ref,ref,self.sib).wait_recv()
    def local(self,p):
        return pltpu.make_async_copy(self.own.at[self.r,pl.ds(*self.cols[p])],self.at(p,self.r,*(self.m(p,j) for j in range(THREE))),self.lsem.at[p])
    def events(self):
        P3=range(THREE)
        def e0():
            for p in P3:
                self.local(p).start()
                for k in (ZERO,ONE,TWO): self.start(p,k)
        def e1():
            for p in P3:
                self.local(p).wait()
                for k in (ZERO,ONE,TWO): self.wait_recv(p,k)
                for k in (THREE,FOUR): self.start(p,k)
        def e2():
            for p in P3:
                for k in (THREE,FOUR): self.wait_recv(p,k); self.start(p,k+TWO)
        def e3():
            for p in P3:
                for k in (FIVE,SIX): self.wait_recv(p,k)
                for k in (SEVEN,EIGHT,ELEVEN): self.start(p,k)
        def e4():
            for p in P3:
                for k in (SEVEN,EIGHT): self.wait_recv(p,k); self.start(p,k+TWO); self.start(p,k+FIVE)
        def e5():
            for p in P3:
                for k in (NINE,TEN): self.wait_recv(p,k)
                self.start(p,14)
        def e6():
            for p in P3:
                for k in range(ELEVEN,15): self.wait_recv(p,k)
        return [e0,e1,e2,e3,e4,e5,e6]
    def finish(self):
        for p in range(THREE):
            for k in range(15): self.wait_send(p,k)

f32=jnp.float32

T, D, FF, LAYERS = 2048, 1024, 2816, TWO
F = 256
N_F = FF // F
M = 512
N_T = T // M
NT = (((ONE,), (ONE,)), ((), ()))
TN = (((ZERO,), (ZERO,)), ((), ()))
L = 128
C = FF // L
GU0 = (((ZERO, TWO), (TWO, TWO), (FOUR, TWO)), ((SIX, THREE), (NINE, THREE), (TWELVE, TWO)), ((14, THREE), (17, THREE), (20, TWO)))
DD = ((ZERO, FOUR), (FOUR, FOUR), (EIGHT, THREE))
GU1 = (((ZERO, FOUR), (FOUR, THREE), (SEVEN, FOUR)), ((ELEVEN, THREE), (14, FOUR), (18, FOUR)))
HBM = pl.BlockSpec(memory_space=pltpu.HBM)
VMEM = pl.BlockSpec(memory_space=pltpu.VMEM)


def dot(a, b, dims=None):
    if dims is None:
        return jnp.dot(a, b, preferred_element_type=f32)
    return lax.dot_general(a, b, dims, preferred_element_type=f32)


def norm_rows(h):
    wide = h.astype(f32)
    return (wide * lax.rsqrt(jnp.mean(wide * wide, -ONE, keepdims=True) + 1e-6)).astype(bf)


def run(events):
    for event in events:
        event()


def at_step(i, events):
    for step, functions in events.items():
        pl.when(i == step)(functools.partial(run, functions))


def pair(ref, f):
    return ref.at[pl.ds(TWO * f, TWO)]


def wide(tiles):
    return jnp.concatenate(tiles, axis=ONE)


def down_block(tiles):
    last = [wide([tiles[ROWS + TWO * g + e][FOUR * c : FOUR * c + FOUR] for c in range(FOUR) for e in (ZERO, ONE)]) for g in range(THREE)]
    return jnp.concatenate([wide(tiles[:EIGHT]), wide(tiles[EIGHT:ROWS]), *last], axis=ZERO)


def plan_forward():
    tiles = [max(n for _, n in cols) for cols in (*GU0, DD, DD, *GU1)]
    per_tile = (0.27, 0.36, 0.18, 1.43, 0.72, 0.0, 0.0)
    due = {ZERO: ZERO, ONE: TWO, TWO: SIX, THREE: N_F, FOUR: N_F + TWO, FIVE: 99, SIX: 99}
    length = [3.0] * N_F + [3.8] * (TWO * N_T)
    late = (2.7, 2.7, 2.7, 2.7, 2.7, 1.5, 0.0)
    following = [ZERO] * SEVEN
    arrives = [0.0] * SEVEN
    plan = [[] for _ in range(N_F + TWO * N_T + TWO)]
    now, link = 0.0, 0.0

    def allowed(place, k):
        e = following[k]
        if e > SIX:
            return False
        if k == ZERO:
            return True
        before = following[k - ONE]
        if place == ZERO and k > TWO:
            return False
        return before > FOUR or (before > THREE and link <= now + 1.0) if e == THREE else before > ZERO

    def run_one(place, k):
        nonlocal now, link
        e = following[k]
        now = max(now, arrives[k]) + 0.3
        plan[place].append((k, e))
        link = max(link, now) + per_tile[e] * tiles[k]
        arrives[k] = (link if e < FIVE else now) + late[e]
        following[k] = e + ONE

    for place in range(len(plan)):
        while True:
            ready = [k for k in range(SEVEN) if allowed(place, k) and arrives[k] <= now]
            if ready:
                run_one(place, ready[ZERO])
                continue
            must = [k for k in range(SEVEN) if following[k] < SEVEN and (due[k] <= place or place == len(plan) - ONE)]
            if not must:
                break
            waiting = [k for k in range(SEVEN) if allowed(place, k) and following[k] < SEVEN]
            run_one(place, min(waiting, key=lambda k: arrives[k]))
        if place < len(length):
            now += length[place]
    return plan


def forward_kernel(
    x_hbm, dy_hbm, w_gate, w_up, own_d,
    gu0, d0, gu1, gate0, up0, act0, a0, h1, a1, dact1, d1,
    x, a, big, wt, go, raw, wc, ho, dyt, own,
    ssem, rsem, csem, xsem, wsem, gsem, bsem, rawsem, hsem, asem, dsem, esem,
):
    load_x = pltpu.make_async_copy(x_hbm, x, xsem.at[ZERO])
    load_x.start()

    def own_tile(c, _):
        for layer in range(LAYERS):
            for k, w in enumerate((w_gate, w_up)):
                own[layer, k, c] = w[layer, :, pl.ds(pl.multiple_of(c * L, L), L)]
        return ZERO

    lax.fori_loop(ZERO, C, own_tile, ZERO)
    me = coords()
    barrier(me)

    def stream(k, shard, out, cols):
        g = Gather(me, shard, out, ssem.at[k], rsem.at[k], csem.at[k], cols)
        return g, g.events()

    todo = [(own.at[ZERO], gu0, cols) for cols in GU0] + [(own_d.at[n], d, DD) for n, d in enumerate((d0, d1))] + [(own.at[ONE], gu1, cols) for cols in GU1]
    streams = [stream(k, *one) for k, one in enumerate(todo)]
    plan = [[streams[k][ONE][e] for k, e in place] for place in plan_forward()]

    run(plan[ZERO][:TWO])
    load_x.wait()

    def norm0(t, _):
        rows = pl.ds(pl.multiple_of(t * M, M), M)
        a[rows, :] = norm_rows(x[rows, :])
        return ZERO

    lax.fori_loop(ZERO, N_T, norm0, ZERO)
    keep_a0 = pltpu.make_async_copy(a, a0, xsem.at[ONE])
    keep_a0.start()
    run(plan[ZERO][TWO:])

    def load_w(w, f, slot):
        return pltpu.make_async_copy(w.at[:, pl.ds(TWO * f, TWO)], wt.at[slot], wsem.at[slot])

    def put(f, slot):
        return (
            pltpu.make_async_copy(go.at[slot, ZERO], pair(gate0, f), gsem.at[slot, ZERO]),
            pltpu.make_async_copy(go.at[slot, ONE], pair(up0, f), gsem.at[slot, ONE]),
            pltpu.make_async_copy(pair(big, f), pair(act0, f), bsem.at[slot]),
        )

    def gate_up(f, events, w, finish):
        slot = lax.rem(f, TWO)
        load_w(w, f, slot).wait()

        @pl.when(f + ONE < N_F)
        def _():
            load_w(w, f + ONE, ONE - slot).start()

        finish(f, slot, [wide([wt[slot, k, e].reshape(D, L) for e in (ZERO, ONE)]) for k in (ZERO, ONE)])
        at_step(f, events)
        return ZERO

    def finish0(f, slot, w):
        @pl.when(f >= TWO)
        def _():
            for copy in put(f - TWO, slot):
                copy.wait()

        for t in range(N_T):
            rows = pl.ds(t * M, M)
            gate, up = dot(a[rows, :], w[ZERO]), dot(a[rows, :], w[ONE])
            act = (gate * jax.nn.sigmoid(gate) * up).astype(bf)
            for e in (ZERO, ONE):
                lanes = slice(L * e, L * e + L)
                go[slot, ZERO, e, rows, :] = gate[:, lanes]
                go[slot, ONE, e, rows, :] = up[:, lanes]
                big[TWO * f + e, rows, :] = act[:, lanes]
        for copy in put(f, slot):
            copy.start()

    load_raw = [pltpu.make_async_copy(d, raw, rawsem) for d in (d0, d1)]
    ev = {f: plan[ONE + f] for f in range(N_F)}
    load_w(gu0, ZERO, ZERO).start()
    lax.fori_loop(ZERO, N_F, lambda f, _: gate_up(f, ev, gu0, finish0), ZERO)
    load_raw[ZERO].start()
    for f in (N_F - TWO, N_F - ONE):
        for copy in put(f, f % TWO):
            copy.wait()
    keep_a0.wait()

    def convert():
        def four(g, _):
            blocks = [down_block([raw[c // ELEVEN, c % ELEVEN, g // FOUR, lax.rem(g, FOUR), z] for c in range(C)]) for z in range(FOUR)]
            wc[pl.ds(pl.multiple_of(176 * g, 176), 176), :] = jnp.concatenate(blocks, axis=ZERO)
            return ZERO

        lax.fori_loop(ZERO, ROWS, four, ZERO)

    load_raw[ZERO].wait()
    convert()

    def put_h(t, slot):
        return pltpu.make_async_copy(ho.at[slot], h1.at[pl.ds(pl.multiple_of(t * M, M), M)], hsem.at[slot])

    def load_dy(t, slot):
        return pltpu.make_async_copy(dy_hbm.at[pl.ds(pl.multiple_of(t * M, M), M)], dyt.at[slot], dsem.at[slot])

    def down(t, events):
        slot = lax.rem(t, TWO)

        @pl.when(t >= TWO)
        def _():
            put_h(t - TWO, slot).wait()

        rows = pl.ds(pl.multiple_of(t * M, M), M)
        h = (x[rows, :].astype(f32) + dot(wide([big[c, rows, :] for c in range(C)]), wc[...]).astype(bf).astype(f32)).astype(bf)
        ho[slot] = h
        a[rows, :] = norm_rows(h)
        put_h(t, slot).start()
        at_step(t, events)
        return ZERO

    lax.fori_loop(ZERO, N_T, lambda t, _: down(t, {ZERO: plan[ONE + N_F], ONE: [*plan[TWO + N_F], lambda: load_raw[ONE].start()], TWO: plan[THREE + N_F], THREE: plan[FOUR + N_F]}), ZERO)
    keep_a1 = pltpu.make_async_copy(a, a1, asem)
    keep_a1.start()
    load_dy(ZERO, ZERO).start()
    for t in (N_T - TWO, N_T - ONE):
        put_h(t, t % TWO).wait()
    load_raw[ONE].wait()
    convert()

    def put_dact(t):
        r = pl.ds(pl.multiple_of(t * M, M), M)
        return pltpu.make_async_copy(big.at[:, r], dact1.at[:, r], esem.at[t])

    def dact(t, events):
        slot = lax.rem(t, TWO)
        load_dy(t, slot).wait()

        @pl.when(t + ONE < N_T)
        def _():
            load_dy(t + ONE, ONE - slot).start()

        rows = pl.ds(pl.multiple_of(t * M, M), M)
        for half in (ZERO, ONE):
            v = dot(dyt[slot], wc[FF // TWO * half : FF // TWO * half + FF // TWO, :], NT).astype(bf)
            for c in range(ELEVEN):
                big[ELEVEN * half + c, rows, :] = v[:, L * c : L * c + L]
        put_dact(t).start()
        at_step(t, events)
        return ZERO

    lax.fori_loop(ZERO, N_T, lambda t, _: dact(t, {n: plan[FIVE + N_F + n] for n in range(N_T)}), ZERO)
    run(plan[-ONE])

    for t in range(N_T):
        put_dact(t).wait()
    keep_a1.wait()
    for g, _ in streams:
        g.finish()


def forward(x, dy, w_gate, w_up, own_d):
    sd = jax.ShapeDtypeStruct
    tall, tall32, narrow = sd((C, T, L), bf), sd((C, T, L), f32), sd((T, D), bf)
    blocks = sd((TWO, C, FOUR, FOUR, FOUR, ROWS, L), bf)
    half_blocks = sd((TWO, C // TWO, FOUR, FOUR, FOUR, ROWS, L), bf)
    dma = pltpu.SemaphoreType.DMA
    return pl.pallas_call(
        forward_kernel,
        in_specs=[HBM, HBM, VMEM, VMEM, VMEM],
        out_specs=[HBM] * ELEVEN,
        out_shape=[blocks, half_blocks, blocks, tall32, tall32, tall, narrow, narrow, narrow, tall, half_blocks],
        scratch_shapes=[
            pltpu.VMEM((T, D), bf), pltpu.VMEM((T, D), bf), pltpu.VMEM((C, T, L), bf),
            pltpu.VMEM((TWO, TWO, TWO, FOUR, FOUR, FOUR, ROWS, L), bf), pltpu.VMEM((TWO, TWO, TWO, T, L), f32),
            pltpu.VMEM((TWO, C // TWO, FOUR, FOUR, FOUR, ROWS, L), bf), pltpu.VMEM((FF, D), bf), pltpu.VMEM((TWO, M, D), bf),
            pltpu.VMEM((TWO, M, D), bf), pltpu.VMEM((LAYERS, TWO, C, ROWS, L), bf),
            dma((SEVEN, THREE, 15)), dma((SEVEN, THREE, 15)), dma((SEVEN, THREE)), dma((TWO,)), dma((TWO,)), dma((TWO, TWO)), dma((TWO,)), dma(()), dma((TWO,)), dma(()), dma((TWO,)), dma((FOUR,)),
        ],
        compiler_params=pltpu.CompilerParams(collective_id=ZERO, has_side_effects=True, vmem_limit_bytes=63 * TWO**20),
        name="forward",
    )(x, dy, w_gate, w_up, own_d)[:TEN]


HALF = FF // TWO
PARTS = ((ZERO, FOUR), (FOUR, FOUR), (EIGHT, THREE))
UNITS = TWELVE


class Scatter:
    @staticmethod
    def vw(p, v, w):
        return (slice(None), v, w) if PERM[p][ONE] < PERM[p][TWO] else (slice(None), w, v)

    @staticmethod
    def scratch():
        s = []
        for p, (_, n) in enumerate(PARTS):
            _, *h = Scatter.vw(p, TWO, FOUR)
            s += [
                pltpu.VMEM((TWO, SIX, n, *h, ROWS, L), bf),
                pltpu.VMEM((TWO, FOUR, n, *h, ROWS, L), bf),
                pltpu.VMEM((n, FOUR, FOUR, ROWS, L), f32), pltpu.VMEM((n, FOUR, FOUR, ROWS, L), bf),
                pltpu.VMEM((SIX, n, TWO, ROWS, L), bf), pltpu.VMEM((TWO, n, TWO, ROWS, L), bf),
                pltpu.VMEM((n, FOUR, ROWS, L), f32), pltpu.VMEM((n, FOUR, ROWS, L), bf),
                pltpu.VMEM((THREE, n, ROWS, L), bf),
            ]
        dma = pltpu.SemaphoreType.DMA
        regular = pltpu.SemaphoreType.REGULAR
        return s + [pltpu.VMEM((ROWS, FF // TWO), bf), dma((TWO, THREE, 15)), dma((TWO, THREE, 15)), dma((TWO, THREE, FOUR)), dma(()), regular((THREE, TWO)), regular((THREE, TWO)), regular((THREE, THREE))]

    def __init__(self, me, grads, out, bufs):
        self.me, self.grads, self.out = me, grads, out
        self.b = [bufs[NINE * p : NINE * p + NINE] for p in range(THREE)]
        self.res, self.ssem, self.rsem, self.lsem, self.osem, self.credit1, self.credit2, self.credit3 = bufs[27:]

    def m(self, p, k, d=ZERO):
        return self.me.plus[PERM[p][k]][d]

    def at_unit(self, k):
        self.k, self.slot = k, lax.rem(k, TWO)
        odd = lax.rem(k, TWO)
        self.grad = jnp.where(k < FOUR, ONE + odd, jnp.where(k < SIX, ZERO, jnp.where(k < EIGHT, THREE, k // TWO)))
        self.col0 = C // TWO * jnp.where(k < FOUR, k // TWO, odd)

    def cols(self, p):
        c, n = PARTS[p]
        return pl.ds(self.col0 + c, n)

    def term(self, p, u, half):
        i = [None] * THREE
        a, v, w = PERM[p]
        i[a], i[v], i[w] = u, pl.ds(TWO * half, TWO), slice(None)
        return self.grads.at[(self.grad, self.cols(p), *i)]

    def own(self, p, j):
        u, h = ((ONE, ZERO), (THREE, ONE), (ZERO, ZERO), (ZERO, ONE))[j]
        return pltpu.make_async_copy(self.term(p, self.m(p, ZERO, u), h), self.b[p][ONE].at[self.slot, j], self.lsem.at[self.slot, p, j])

    def cp(self, p, k):
        b, s = self.b[p], self.slot
        if k < SIX:
            ax, d = ZERO, (ONE, THREE, ONE, THREE, ONE, THREE)[k]
            if k < FOUR:
                u, h = ((TWO, ZERO), (TWO, ONE), (ONE, ONE), (THREE, ZERO))[k]
                src = self.term(p, self.m(p, ZERO, u), h)
            else:
                src = b[ONE].at[s, k - FOUR]
            dst = b[ZERO].at[s, k]
        elif k < TWELVE:
            j = k - SIX
            ax, d = ONE, (ONE, THREE, ONE, THREE, ONE, THREE)[j]
            if j < FOUR:
                v, h = ((TWO, ZERO), (TWO, ONE), (ONE, ONE), (THREE, ZERO))[j]
                src = b[THREE].at[self.vw(p, self.m(p, ONE, v), pl.ds(TWO * h, TWO))]
            else:
                src = b[FIVE].at[j - FOUR]
            dst, s = b[FOUR].at[j], ZERO
        else:
            ax, d = TWO, (ONE, THREE, TWO)[k - TWELVE]
            src, dst, s = b[SEVEN].at[:, self.m(p, TWO, d)], b[EIGHT].at[k - TWELVE], ZERO
        return pltpu.make_async_remote_copy(
            src_ref=src, dst_ref=dst, send_sem=self.ssem.at[s, p, k], recv_sem=self.rsem.at[s, p, k],
            device_id=shifted(self.me, PERM[p][ax], d), device_id_type=MESH,
        )

    def give(self, credit, axis, last):
        @pl.when(self.k < last)
        def _():
            for p in range(THREE):
                for j, d in enumerate((THREE, ONE, TWO)[: credit.shape[ONE]]):
                    pl.semaphore_signal(credit.at[p, j], inc=ONE, device_id=shifted(self.me, PERM[p][axis], d), device_id_type=MESH)

    def take(self, credit, first):
        @pl.when(self.k >= first)
        def _():
            for p in range(THREE):
                for j in range(credit.shape[ONE]):
                    pl.semaphore_wait(credit.at[p, j], ONE)

    def begin(self):
        self.take(self.credit1, TWO)
        for k in (ZERO, ONE, TWO, THREE):
            for p in range(THREE):
                self.cp(p, k).start()
        for p in range(THREE):
            for j in range(FOUR):
                self.own(p, j).start()

    def pass_on(self):
        s = self.slot
        for p in range(THREE):
            b = self.b[p]
            for k in (ZERO, ONE):
                self.own(p, k).wait()
                self.cp(p, k).wait_recv()
                for n in range(PARTS[p][ONE]):
                    b[ONE][s, k, n] = (b[ZERO][s, k, n].astype(f32) + b[ONE][s, k, n].astype(f32)).astype(bf)
        for k in (FOUR, FIVE):
            for p in range(THREE):
                self.cp(p, k).start()

    def first_sum(self):
        s = self.slot
        for p in range(THREE):
            b = self.b[p]
            for k in (TWO, THREE, FOUR, FIVE):
                self.cp(p, k).wait_recv()
            for j in (TWO, THREE):
                self.own(p, j).wait()
            for half in (ZERO, ONE):
                own, sums, raw = ((TWO, FOUR, THREE), (THREE, FIVE, TWO))[half]
                _, *ix = self.vw(p, slice(TWO * half, TWO * half + TWO), slice(None))
                for n in range(PARTS[p][ONE]):
                    t = b[ONE][s, own, n].astype(f32) + b[ZERO][s, sums, n].astype(f32) + b[ZERO][s, raw, n].astype(f32)
                    b[TWO][(n, *ix)] = t
                    b[THREE][(n, *ix)] = t.astype(bf)
        for p in range(THREE):
            for k in range(SIX):
                self.cp(p, k).wait_send()
        self.give(self.credit1, ZERO, UNITS - TWO)
        self.take(self.credit2, ONE)
        for k in (SIX, SEVEN, EIGHT, NINE):
            for p in range(THREE):
                self.cp(p, k).start()

    def pass_on2(self):
        for p in range(THREE):
            b = self.b[p]
            for half in (ZERO, ONE):
                self.cp(p, SIX + half).wait_recv()
                v = self.m(p, ONE, (ONE, THREE)[half])
                own = b[TWO][self.vw(p, v, slice(TWO * half, TWO * half + TWO))]
                b[FIVE][half] = (b[FOUR][half].astype(f32) + own).astype(bf)
        for k in (TEN, ELEVEN):
            for p in range(THREE):
                self.cp(p, k).start()

    def second_sum(self):
        for p in range(THREE):
            b, v = self.b[p], self.m(p, ONE)
            for k in (EIGHT, NINE, TEN, ELEVEN):
                self.cp(p, k).wait_recv()
            for half in (ZERO, ONE):
                sums, raw = ((FOUR, THREE), (FIVE, TWO))[half]
                part = slice(TWO * half, TWO * half + TWO)
                t = b[TWO][self.vw(p, v, part)] + b[FOUR][sums].astype(f32) + b[FOUR][raw].astype(f32)
                b[SIX][:, part] = t
                b[SEVEN][:, part] = t.astype(bf)
        for p in range(THREE):
            for k in range(SIX, TWELVE):
                self.cp(p, k).wait_send()
        self.give(self.credit2, ONE, UNITS - ONE)
        self.take(self.credit3, ONE)
        for k in (TWELVE, 13, 14):
            for p in range(THREE):
                self.cp(p, k).start()

    def total(self):
        for p in range(THREE):
            b, w = self.b[p], self.m(p, TWO)
            for k in (TWELVE, 13, 14):
                self.cp(p, k).wait_recv()
            t = b[SIX][:, w]
            for j in range(THREE):
                t = t + b[EIGHT][j].astype(f32)
            c, n = PARTS[p]
            for q in range(n):
                self.res[:, L * (c + q) : L * (c + q) + L] = t[q].astype(bf)
        layer, kind = ONE - self.grad // THREE, lax.rem(self.grad, THREE)
        for m, out in enumerate(self.out):

            @pl.when(kind == m)
            def _():
                pltpu.make_async_copy(self.res, out.at[layer, :, pl.ds(pl.multiple_of(self.col0 * L, L), FF // TWO)], self.osem).start()

        for p in range(THREE):
            for k in (TWELVE, 13, 14):
                self.cp(p, k).wait_send()
        self.give(self.credit3, TWO, UNITS - ONE)
        pltpu.make_async_copy(self.res, self.out[ZERO].at[ZERO, :, pl.ds(ZERO, FF // TWO)], self.osem).wait()

    def tick(self, j, plan):
        def due(steps):
            words = [sum(ONE << (n - 30 * w) for n in steps if n // 30 == w) for w in range(max(plan["total"]) // 30 + ONE)]
            word = functools.reduce(lambda have, w: jnp.where(j >= 30 * w, words[w], have), range(ONE, len(words)), words[ZERO])
            return (lax.shift_right_logical(jnp.int32(word), lax.rem(j, 30)) & ONE) == ONE

        @pl.when(due({n for steps in plan.values() for n in steps}))
        def _():
            for event in (self.total, self.second_sum, self.pass_on2, self.first_sum, self.pass_on, self.begin):
                steps = plan[event.__name__]

                @pl.when(due(steps))
                def _():
                    self.at_unit(sum(jnp.where(j > n, ONE, ZERO) for n in steps))
                    event()


S1, S2, S3, S6, S5, S7, S8, S9, TAIL = ZERO, ELEVEN, 19, 35, 43, 51, 63, 74, 90


def make_plan():
    length = [5.1] * ELEVEN + [2.2] * EIGHT + [1.95] * ROWS + [2.2] * EIGHT + [2.1] * EIGHT + [2.4] * TWELVE + [1.4] * ELEVEN + [1.95] * ROWS
    ready = [SEVEN, SEVEN, S2 + ONE, S2 + ONE, S3 + ONE, S3 + ONE, S5 + ONE, S5 + ONE, S7 + SEVEN, S8 + ONE, S8 + SEVEN, S9 + ONE]
    names = ("begin", "pass_on", "first_sum", "pass_on2", "second_sum", "total")
    sends = (6.1, 3.05, 1.6, 0.8, 1.1, 0.0)
    late = 2.5
    plan = {name: [] for name in names}
    arrives = [[0.0] * SEVEN for _ in range(UNITS)]
    now, link, step = 3.0, 0.0, ZERO

    def may_run(e, k):
        n = len(plan[names[e]])
        if n != k or (plan[names[e]] and plan[names[e]][-ONE] == step):
            return False
        if e == ZERO:
            return step >= ready[k] and (k < TWO or len(plan["first_sum"]) > k - TWO)
        if len(plan[names[e - ONE]]) <= k or plan[names[e - ONE]][k] == step:
            return False
        if e == TWO and len(plan["second_sum"]) < k:
            return False
        return not (e == FOUR and len(plan["total"]) < k)

    while len(plan["total"]) < UNITS:
        ran = False
        for e in (FIVE, FOUR, THREE, TWO, ONE, ZERO):
            k = len(plan[names[e]])
            if k < UNITS and may_run(e, k) and (arrives[k][e] <= now or step >= TAIL):
                if step >= TAIL and arrives[k][e] > now:
                    if ran or any(may_run(o, len(plan[names[o]])) and arrives[len(plan[names[o]])][o] < arrives[k][e] for o in range(SIX) if o != e and len(plan[names[o]]) < UNITS):
                        continue
                    now = arrives[k][e]
                plan[names[e]].append(step)
                ran = True
                now += 0.35
                link = max(link, now) + sends[e]
                if e == ZERO:
                    arrives[k][ONE], arrives[k][TWO] = link - sends[ONE] + late, link + late
                elif e < FIVE:
                    arrives[k][e + ONE] = max(arrives[k][e + ONE], link + late)
        now += length[step] if step < TAIL else 0.05
        step += ONE
    return plan


PLAN = make_plan()
N_STEPS = max(PLAN["total"]) + ONE


def backward_kernel(
    x, dy, gu0, d0, gu1, gate0, up0, act0, a0, h1, a1, dact1,
    dx, by_down, by_gate, by_up, grads, dup1,
    am, dh, r1, r2, r3, stg, tl, ob, gl, ht,
    lsem, r1sem, r2sem, r3sem, amsem, wsem, dasem, tlsem, obsem, glsem, flsem, hsem, dxsem, *bufs,
):
    me = coords()
    barrier(me, sib=False)
    scatter = Scatter(me, grads, (by_down, by_gate, by_up), bufs)

    def rows(t, n=M):
        return pl.ds(pl.multiple_of(t * n, n), n)

    def col(f, n=F):
        return pl.ds(pl.multiple_of(f * n, 128), n)

    load_dh = pltpu.make_async_copy(dy, dh, lsem)
    load_dup = pltpu.make_async_copy(dup1, r1, r1sem)
    load_act = pltpu.make_async_copy(act0, r2, r2sem)

    def load_am(src):
        return pltpu.make_async_copy(src, am, amsem)

    def load_wt(f, slot):
        return [
            pltpu.make_async_copy(gu1.at[k, pl.ds(TWO * f, TWO), pl.ds(TWO * h, TWO)], stg.at[pl.ds(EIGHT * slot + FOUR * k + TWO * h, TWO)], wsem.at[slot, k, h])
            for k in (ZERO, ONE) for h in (ZERO, ONE)
        ]

    def load_dact(f, slot):
        return pltpu.make_async_copy(pair(dact1, f), pair(r1, f), dasem.at[slot])

    def load_r3(src, h):
        return pltpu.make_async_copy(src.at[:, pl.ds(TWO * h, TWO)], r3.at[:, pl.ds(TWO * h, TWO)], r3sem.at[h])

    def flush(grad, half):
        return pltpu.make_async_copy(stg, grads.at[grad, :, pl.ds(TWO * half, TWO)], flsem)

    def put_tl(f, slot):
        return pltpu.make_async_copy(tl.at[slot], pair(dup1, f), tlsem.at[slot])

    def put_ob(grad, f, slot, kinds=(ZERO, ONE)):
        return [pltpu.make_async_copy(ob.at[slot, k], grads.at[grad + k, pl.ds(TWO * f, TWO)], obsem.at[slot, k]) for k in kinds]

    def load_gl(f, e):
        return [pltpu.make_async_copy(src.at[TWO * f + e], gl.at[e, k], glsem.at[e, k]) for k, src in enumerate((gate0, up0))]

    def load_h(src, t):
        return pltpu.make_async_copy(src.at[rows(t)], ht, hsem)

    def put_dx(t):
        return pltpu.make_async_copy(dh.at[rows(t)], dx.at[rows(t)], dxsem.at[t])

    def go(copies):
        for c in copies:
            c.start()

    def done(copies):
        for c in copies:
            c.wait()

    def when(condition, f):
        pl.when(condition)(f)

    def gate_up_grad(slot, tiles, parts=(ZERO, FOUR), kinds=(ZERO, ONE)):
        lo, hi = parts
        v = dot(am[:, F * lo : F * hi], wide(tiles), TN).astype(bf)
        for n, k in enumerate(kinds):
            for e in (ZERO, ONE):
                ob[slot, k, e, lo:hi] = v[:, F * n + L * e : F * n + L * e + L].reshape(hi - lo, FOUR, FOUR, ROWS, L)

    def layer1(f, slot):
        w = []
        for k in (ZERO, ONE):
            halves = [wide([stg[EIGHT * slot + FOUR * k + TWO * h + e].reshape(D // TWO, L) for e in (ZERO, ONE)]) for h in (ZERO, ONE)]
            w.append(jnp.concatenate(halves, axis=ZERO))
        for t in range(N_T):
            r = pl.ds(t * M, M)
            gate, up = dot(am[r, :], w[ZERO]), dot(am[r, :], w[ONE])
            by_act = wide([r1[TWO * f + e, r, :] for e in (ZERO, ONE)]).astype(f32)
            sig = jax.nn.sigmoid(gate)
            silu = gate * sig
            act, by_gate, by_up = silu * up, by_act * up * (sig + silu * (ONE - sig)), by_act * silu
            for e in (ZERO, ONE):
                lanes = slice(L * e, L * e + L)
                r1[TWO * f + e, r, :] = act[:, lanes].astype(bf)
                r2[TWO * f + e, r, :] = by_gate[:, lanes].astype(bf)
                tl[slot, e, r, :] = by_up[:, lanes].astype(bf)
        gate_up_grad(slot, [r2[TWO * f], r2[TWO * f + ONE], tl[slot, ZERO], tl[slot, ONE]])

    def down_grad(s, src, grad):
        half, c = s // FOUR, lax.rem(s, FOUR)
        lhs = wide([src[C // TWO * half + i] for i in range(C // TWO)])
        am[: FF // TWO, :F] = dot(lhs, dh[:, col(c)], TN).astype(bf)
        when(s == FOUR, lambda: flush(grad, ZERO).wait())
        lanes = [slice(L * e, L * e + L) for e in (ZERO, ONE)]

        def four(g, _):
            v = am[pl.ds(pl.multiple_of(176 * g, 176), 176), :F]
            x, y = g // FOUR, lax.rem(g, FOUR)
            for z in range(FOUR):
                for e in (ZERO, ONE):
                    stg[TWO * c + e, x, y, z] = v[44 * z : 44 * z + ROWS, lanes[e]]
                    stg[EIGHT + TWO * c + e, x, y, z] = v[44 * z + ROWS : 44 * z + 32, lanes[e]]
            for k in range(FOUR):

                @pl.when(c == k)
                def _():
                    for z in range(FOUR):
                        for n in range(THREE):
                            for e in (ZERO, ONE):
                                stg[ROWS + TWO * n + e, x, y, z, FOUR * k : FOUR * k + FOUR] = v[44 * z + 32 + FOUR * n : 44 * z + 36 + FOUR * n, lanes[e]]

            return ZERO

        lax.fori_loop(ZERO, EIGHT, four, ZERO)
        for h in (ZERO, ONE):
            when(s == FOUR * h + THREE, lambda: flush(grad, h).start())

    def silu_back(f, e, t):
        for q in range(t * M, t * M + M, L):
            r = slice(q, q + L)
            gate, up, by_act = gl[e, ZERO, r, :], gl[e, ONE, r, :], r1[TWO * f + e, r, :].astype(f32)
            sig = jax.nn.sigmoid(gate)
            silu = gate * sig
            r2[TWO * f + e, r, :] = (by_act * up * (sig + silu * (ONE - sig))).astype(bf)
            r1[TWO * f + e, r, :] = (by_act * silu).astype(bf)

    def by_input(src, n, t):
        w = wide([r3[c, pl.ds(TWO * n, TWO)].reshape(D // TWO, L) for c in range(C)])
        return dot(wide([src[c, rows(t), :] for c in range(C)]), w, NT).astype(bf)

    def norm_back(t):
        h = ht[...].astype(f32)
        by_a = am[rows(t), :].astype(f32)
        scale = lax.rsqrt(jnp.mean(h * h, -ONE, keepdims=True) + 1e-6)
        by_wide = scale * by_a - h * (scale * scale * scale * jnp.mean(h * by_a, -ONE, keepdims=True))
        dh[rows(t), :] = (dh[rows(t), :].astype(f32) + by_wide.astype(bf).astype(f32)).astype(bf)

    def down_rows(half):
        def four(g, _):
            blocks = [down_block([r3[c, TWO * half + g // FOUR, lax.rem(g, FOUR), z] for c in range(C)]) for z in range(FOUR)]
            am[pl.ds(pl.multiple_of(176 * g, 176), 176), :] = jnp.concatenate(blocks, axis=ZERO)
            return ZERO

        lax.fori_loop(ZERO, EIGHT, four, ZERO)

    def step(j, _):
        def within(a, b):
            return (j >= a) & (j < b)

        in1, in2, in3 = j < S2, within(S2, S3), within(S3, S6)
        in6, in5, in7, in8, in9 = within(S6, S5), within(S5, S7), within(S7, S8), within(S8, S9), within(S9, TAIL)

        def input_pre(s, w, src):
            when(s == ZERO, lambda: load_r3(w.at[ZERO], ZERO).wait())

            @pl.when(s == FOUR)
            def _():
                load_r3(w.at[ZERO], ONE).wait()
                load_r3(w.at[ONE], ZERO).start()

            @pl.when(s == EIGHT)
            def _():
                load_r3(w.at[ONE], ZERO).wait()
                load_r3(w.at[ONE], ONE).start()

            when(s == ELEVEN, lambda: load_h(src, ZERO).start())
            when(s == TWELVE, lambda: load_r3(w.at[ONE], ONE).wait())

        @pl.when(j < S6)
        def _():
            @pl.when(in1)
            def _():
                f = j - S1
                slot = lax.rem(f, TWO)

                @pl.when(f >= TWO)
                def _():
                    done(put_ob(ONE, f - TWO, slot))
                    put_tl(f - TWO, slot).wait()

                done(load_wt(f, slot))
                load_dact(f, slot).wait()

                @pl.when(f + ONE < N_F)
                def _():
                    go(load_wt(f + ONE, ONE - slot))
                    load_dact(f + ONE, ONE - slot).start()

                when(f == TWO, lambda: go([load_r3(gu1.at[ZERO], h) for h in (ZERO, ONE)]))

            @pl.when(in2)
            def _():
                @pl.when(j == S2)
                def _():
                    done(put_ob(ONE, N_F - TWO, ONE))
                    put_tl(N_F - TWO, ONE).wait()
                    load_dh.wait()

                @pl.when(j == S2 + ONE)
                def _():
                    done(put_ob(ONE, N_F - ONE, ZERO))
                    put_tl(N_F - ONE, ZERO).wait()

            @pl.when(in3)
            def _():
                s = j - S3
                input_pre(s, gu1, h1)
                when(s == ZERO, lambda: load_dup.start())
                when(s == ONE, lambda: flush(ZERO, ONE).wait())

                @pl.when(s == EIGHT)
                def _():
                    load_dup.wait()
                    load_act.start()

                when(s == TWELVE, lambda: load_r3(d0, ZERO).start())

        @pl.when((j >= S6) & (j < TAIL))
        def _():
            @pl.when(in9)
            def _():
                s = j - S9
                input_pre(s, gu0, x)
                when(s == ZERO, lambda: done(put_ob(FOUR, N_F - TWO, ONE, (ONE,))))
                when(s == ONE, lambda: done(put_ob(FOUR, N_F - ONE, ZERO, (ONE,))))

            @pl.when(j == S6)
            def _():
                load_act.wait()
                load_r3(d0, ONE).start()

            @pl.when(in5)
            def _():
                s = j - S5

                @pl.when(s == ZERO)
                def _():
                    load_r3(d0, ZERO).wait()
                    go(load_gl(ZERO, ZERO) + load_gl(ZERO, ONE))

                @pl.when(s == ONE)
                def _():
                    flush(THREE, ONE).wait()
                    load_r3(gu0.at[ZERO], ZERO).start()

                when(s == FOUR, lambda: load_r3(d0, ONE).wait())
                when(s == FIVE, lambda: load_r3(gu0.at[ZERO], ONE).start())

            @pl.when(in7)
            def _():
                when(j == S7 + ONE, lambda: load_am(a0).wait())
                i = j - S7
                when((i >= THREE) & (i != EIGHT), lambda: done(put_ob(FOUR, i - THREE, lax.rem(i - THREE, TWO), (ZERO,))))
                when(i == SEVEN, lambda: done(put_ob(FOUR, FIVE, ONE, (ZERO,))))

            @pl.when(in8)
            def _():
                f = j - S8
                when(f == ZERO, lambda: done(put_ob(FOUR, N_F - TWO, ONE, (ZERO,))))
                when(f == ONE, lambda: done(put_ob(FOUR, N_F - ONE, ZERO, (ZERO,))))
                when(f >= TWO, lambda: done(put_ob(FOUR, f - TWO, lax.rem(f, TWO), (ONE,))))

        scatter.tick(j, PLAN)

        @pl.when(j < S3)
        def _():
            @pl.when(in1)
            def _():
                f = j - S1
                slot = lax.rem(f, TWO)
                layer1(f, slot)
                go(put_ob(ONE, f, slot))
                put_tl(f, slot).start()

            when(in2, lambda: down_grad(j - S2, r1, ZERO))

        @pl.when(in3 | in9)
        def _():
            s = jnp.where(in3, j - S3, j - S9)
            n, t = lax.rem(s, EIGHT) // FOUR, lax.rem(s, FOUR)
            here = (rows(t), col(n, D // TWO))

            def more():
                am[here] = (am[here].astype(f32) + by_input(r1, n, t).astype(f32)).astype(bf)

            @pl.when(s < EIGHT)
            def _():
                am[here] = by_input(r2, n, t)

            when((s >= EIGHT) & (s < 13), more)

            @pl.when(s >= 13)
            def _():
                load_h(h1, t - ONE).wait()
                norm_back(t - ONE)
                more()
                when(in3, lambda: load_h(h1, t).start())
                when(in9, lambda: load_h(x, t).start())
                when(in9, lambda: put_dx(t - ONE).start())

            @pl.when(s == 15)
            def _():
                load_h(h1, THREE).wait()
                norm_back(THREE)
                when(in9, lambda: put_dx(THREE).start())

        @pl.when((j >= S6) & (j < S9))
        def _():
            when(in6, lambda: down_grad(j - S6, r2, THREE))

            @pl.when(in5)
            def _():
                s = j - S5
                half, t = s // FOUR, lax.rem(s, FOUR)
                when(t == ZERO, lambda: down_rows(half))
                v = dot(dh[rows(t), :], am[: FF // TWO, :], NT).astype(bf)
                for c in range(C // TWO):
                    r1[C // TWO * half + c, rows(t), :] = v[:, L * c : L * c + L]
                when(s == SEVEN, lambda: load_am(a0).start())

            @pl.when(in7)
            def _():
                i = j - S7
                before = i - ONE
                slot = lax.rem(i + ONE, TWO)
                tiles = lambda: [r2[TWO * before], r2[TWO * before + ONE]]

                @pl.when(i == ZERO)
                def _():
                    for e in (ZERO, ONE):
                        done(load_gl(ZERO, e))
                        for t in range(FOUR):
                            silu_back(ZERO, e, t)
                        go(load_gl(ONE, e))

                @pl.when((i > ZERO) & (i < N_F))
                def _():
                    for e in (ZERO, ONE):
                        done(load_gl(i, e))
                        for t in (ZERO, ONE):
                            gate_up_grad(slot, tiles(), (TWO * e + t, TWO * e + t + ONE), (ZERO,))
                            silu_back(i, e, TWO * t)
                            silu_back(i, e, TWO * t + ONE)
                        when(i + ONE < N_F, lambda: go(load_gl(i + ONE, e)))

                when(i == N_F, lambda: gate_up_grad(slot, tiles(), (ZERO, FOUR), (ZERO,)))
                when(i > ZERO, lambda: go(put_ob(FOUR, before, slot, (ZERO,))))

            @pl.when(in8)
            def _():
                f = j - S8
                slot = lax.rem(f, TWO)
                gate_up_grad(slot, [r1[TWO * f], r1[TWO * f + ONE]], (ZERO, FOUR), (ONE,))
                go(put_ob(FOUR, f, slot, (ONE,)))

        return ZERO

    load_am(a1).start()
    go(load_wt(ZERO, ZERO))
    load_dact(ZERO, ZERO).start()
    load_dh.start()
    load_am(a1).wait()
    lax.fori_loop(ZERO, N_STEPS, step, ZERO)
    done([put_dx(t) for t in range(FOUR)])


def backward(x, dy, gu0, d0, *args):
    sd = jax.ShapeDtypeStruct
    dma = pltpu.SemaphoreType.DMA
    return pl.pallas_call(
        backward_kernel,
        in_specs=[HBM] * TWELVE,
        out_specs=[HBM] * SIX,
        out_shape=[sd((T, D), bf), *[sd((LAYERS, ROWS, FF), bf)] * THREE, sd((SIX, C, FOUR, FOUR, FOUR, ROWS, L), bf), sd((C, T, L), bf)],
        scratch_shapes=[
            pltpu.VMEM((T, D), bf), pltpu.VMEM((T, D), bf), pltpu.VMEM((C, T, L), bf), pltpu.VMEM((C, T, L), bf),
            pltpu.VMEM((C, FOUR, FOUR, FOUR, ROWS, L), bf), pltpu.VMEM((C, TWO, FOUR, FOUR, ROWS, L), bf), pltpu.VMEM((TWO, TWO, T, L), bf),
            pltpu.VMEM((TWO, TWO, TWO, FOUR, FOUR, FOUR, ROWS, L), bf), pltpu.VMEM((TWO, TWO, T, L), f32), pltpu.VMEM((M, D), bf),
            dma(()), dma(()), dma(()), dma((TWO,)), dma(()), dma((TWO, TWO, TWO)), dma((TWO,)), dma((TWO,)), dma((TWO, TWO)), dma((TWO, TWO)), dma(()), dma(()), dma((FOUR,)),
            *Scatter.scratch(),
        ],
        compiler_params=pltpu.CompilerParams(collective_id=ONE, has_side_effects=True, vmem_limit_bytes=63 * TWO**20 + 900 * 1024),
        name="backward",
    )(x, dy, gu0, d0.reshape(C, FOUR, FOUR, FOUR, ROWS, L), *args)[:FOUR]


def pack_down(t):
    first = t[:, :32].reshape(-ONE, TWO, ROWS, EIGHT, L).transpose(ZERO, ONE, THREE, TWO, FOUR).reshape(-ONE, ROWS, ROWS, L)
    last = t[:, 32:].reshape(-ONE, THREE, FOUR, FOUR, TWO, L).transpose(ZERO, ONE, FOUR, THREE, TWO, FIVE).reshape(-ONE, SIX, ROWS, L)
    return jnp.concatenate([first, last], axis=ONE).reshape(-ONE, TWO, C // TWO, ROWS, L)


def unpack_down(t):
    last = t[:, :, TWO * D :].reshape(-ONE, FOUR, FOUR, THREE, F).transpose(ZERO, THREE, TWO, ONE, FOUR).reshape(-ONE, TWELVE, D)
    return jnp.concatenate([t[:, :, :D], t[:, :, D : TWO * D], last], axis=ONE)


def solution(mesh):
    def device(x, dy, w_gate, w_up, w_down):
        x, dy = x[ZERO], dy[ZERO]
        own_d = pack_down(w_down)
        gu0, d0, gu1, *rest = forward(x, dy, w_gate, w_up, own_d)
        by_x, by_down, by_gate, by_up = backward(x, dy, gu0, d0, gu1, *rest)
        return by_x[None], by_gate, by_up, unpack_down(by_down)

    return jax.shard_map(
        device,
        mesh=mesh,
        in_specs=(P(("rep", "dp")), P(("rep", "dp")), *(P(None, "dp"),) * THREE),
        out_specs=(P(("rep", "dp")), *(P("rep", "dp"),) * THREE),
        check_vma=False,
    )
```

```python
import functools
import jax, jax.numpy as jnp
from jax import lax
from jax.experimental import pallas as pl
from jax.experimental.pallas import tpu as pltpu
from jax.sharding import PartitionSpec as P
ZERO, ONE, TWO, THREE, FOUR, FIVE, SIX, SEVEN, EIGHT, NINE, TEN, ELEVEN, TWELVE = range(13)
ROWS = 1024 // 64
bf=jnp.bfloat16
MESH=pl.DeviceIdType.MESH
PERM=((ZERO,ONE,TWO),(ONE,TWO,ZERO),(TWO,ZERO,ONE))

class Place:
    def __init__(self):
        i=lax.axis_index("dp")
        self.plus=[[c,*((c+d)%FOUR for d in range(ONE,FOUR))] for c in (i//ROWS,(i//FOUR)%FOUR,i%FOUR)]
        self.near=[]
        for a in range(THREE):
            c=[self.plus[b][ZERO] for b in range(THREE)]
            self.near.append([{"dp":(c[:a]+[self.plus[a][d]]+c[a+ONE:])[ZERO]*ROWS+(c[:a]+[self.plus[a][d]]+c[a+ONE:])[ONE]*FOUR+(c[:a]+[self.plus[a][d]]+c[a+ONE:])[TWO]} for d in range(FOUR)])

def coords():
    return Place()

def shifted(me,axis,d):
    return me.near[axis][d]

def peers(me,far=True):
    return [shifted(me,a,d) for a in range(THREE) for d in ((ONE,THREE,TWO) if far else (ONE,THREE))]

def barrier(me,far=True,sib=True):
    b=pltpu.get_barrier_semaphore()
    n=ZERO
    for t in peers(me,far):
        pl.semaphore_signal(b,inc=ONE,device_id=t,device_id_type=MESH); n+=ONE
    if sib:
        pl.semaphore_signal(b,inc=ONE,device_id={"rep":ONE-lax.axis_index("rep")},device_id_type=MESH); n+=ONE
    pl.semaphore_wait(b,n)

class Gather:
    NSEM=15
    def __init__(self,me,own,out,ssem,rsem,lsem,cols):
        self.me,self.own,self.out,self.ssem,self.rsem,self.lsem,self.cols=me,own,out,ssem,rsem,lsem,cols
        self.r=lax.axis_index("rep"); self.sib={"rep":ONE-self.r}
    def at(self,p,r,u,v,w):
        i=[None]*THREE
        for a,k in zip(PERM[p],(u,v,w)): i[a]=k
        return self.out.at[(r,pl.ds(*self.cols[p]),*i)]
    def copy(self,p,k,src,dst,dev):
        return pltpu.make_async_remote_copy(src_ref=src,dst_ref=dst,send_sem=self.ssem.at[p,k],recv_sem=self.rsem.at[p,k],device_id=dev,device_id_type=MESH)
    def m(self,p,k,d=ZERO): return self.me.plus[PERM[p][k]][d]
    def sent(self,p,k):
        r=self.r; u,v,w=(self.m(p,j) for j in range(THREE)); A=slice(None); lo,hi=pl.ds(ZERO,TWO),pl.ds(TWO,TWO)
        near=[self.me.near[a] for a in PERM[p]]
        if k<THREE: return self.own.at[r,pl.ds(*self.cols[p])],self.at(p,r,u,v,w),near[ZERO][(ONE,THREE,TWO)[k]]
        if k<FIVE: ref,to=self.at(p,r,A,v,w),near[ONE][(ONE,THREE)[k-THREE]]
        elif k<SEVEN: ref,to=self.at(p,r,(lo,hi)[k-FIVE],self.m(p,ONE,(THREE,ONE)[k-FIVE]),w),near[ONE][(ONE,THREE)[k-FIVE]]
        elif k<NINE: ref,to=self.at(p,r,A,A,w),near[TWO][(ONE,THREE)[k-SEVEN]]
        elif k<ELEVEN: ref,to=self.at(p,r,(lo,hi)[k-NINE],A,self.m(p,TWO,(THREE,ONE)[k-NINE])),near[TWO][(ONE,THREE)[k-NINE]]
        else: ref,to=self.at(p,r,A,A,self.m(p,TWO,(ZERO,THREE,ONE,TWO)[k-ELEVEN])),self.sib
        return ref,ref,to
    def received(self,p,k):
        r=self.r; v,w=self.m(p,ONE),self.m(p,TWO); A=slice(None); lo,hi=pl.ds(ZERO,TWO),pl.ds(TWO,TWO)
        if k<THREE: return self.at(p,r,self.m(p,ZERO,(THREE,ONE,TWO)[k]),v,w)
        if k<FIVE: return self.at(p,r,A,self.m(p,ONE,(THREE,ONE)[k-THREE]),w)
        if k<SEVEN: return self.at(p,r,(lo,hi)[k-FIVE],self.m(p,ONE,TWO),w)
        if k<NINE: return self.at(p,r,A,A,self.m(p,TWO,(THREE,ONE)[k-SEVEN]))
        if k<ELEVEN: return self.at(p,r,(lo,hi)[k-NINE],A,self.m(p,TWO,TWO))
        return self.at(p,ONE-r,A,A,self.m(p,TWO,(ZERO,THREE,ONE,TWO)[k-ELEVEN]))
    def start(self,p,k):
        s,d,dev=self.sent(p,k); self.copy(p,k,s,d,dev).start()
    def wait_send(self,p,k):
        s,d,dev=self.sent(p,k); self.copy(p,k,s,d,dev).wait_send()
    def wait_recv(self,p,k):
        ref=self.received(p,k); self.copy(p,k,ref,ref,self.sib).wait_recv()
    def local(self,p):
        return pltpu.make_async_copy(self.own.at[self.r,pl.ds(*self.cols[p])],self.at(p,self.r,*(self.m(p,j) for j in range(THREE))),self.lsem.at[p])
    def events(self):
        P3=range(THREE)
        def e0():
            for p in P3:
                self.local(p).start()
                for k in (ZERO,ONE,TWO): self.start(p,k)
        def e1():
            for p in P3:
                self.local(p).wait()
                for k in (ZERO,ONE,TWO): self.wait_recv(p,k)
                for k in (THREE,FOUR): self.start(p,k)
        def e2():
            for p in P3:
                for k in (THREE,FOUR): self.wait_recv(p,k); self.start(p,k+TWO)
        def e3():
            for p in P3:
                for k in (FIVE,SIX): self.wait_recv(p,k)
                for k in (SEVEN,EIGHT,ELEVEN): self.start(p,k)
        def e4():
            for p in P3:
                for k in (SEVEN,EIGHT): self.wait_recv(p,k); self.start(p,k+TWO); self.start(p,k+FIVE)
        def e5():
            for p in P3:
                for k in (NINE,TEN): self.wait_recv(p,k)
                self.start(p,14)
        def e6():
            for p in P3:
                for k in range(ELEVEN,15): self.wait_recv(p,k)
        return [e0,e1,e2,e3,e4,e5,e6]
    def finish(self):
        for p in range(THREE):
            for k in range(15): self.wait_send(p,k)

f32=jnp.float32

T, D, FF, LAYERS = 2048, 1024, 2816, TWO
F = 256
N_F = FF // F
M = 512
N_T = T // M
NT = (((ONE,), (ONE,)), ((), ()))
TN = (((ZERO,), (ZERO,)), ((), ()))
L = 128
C = FF // L
GU0 = (((ZERO, TWO), (TWO, TWO), (FOUR, TWO)), ((SIX, THREE), (NINE, THREE), (TWELVE, TWO)), ((14, THREE), (17, THREE), (20, TWO)))
DD = ((ZERO, FOUR), (FOUR, FOUR), (EIGHT, THREE))
GU1 = (((ZERO, FOUR), (FOUR, THREE), (SEVEN, FOUR)), ((ELEVEN, THREE), (14, FOUR), (18, FOUR)))
HBM = pl.BlockSpec(memory_space=pltpu.HBM)
VMEM = pl.BlockSpec(memory_space=pltpu.VMEM)


def dot(a, b, dims=None):
    if dims is None:
        return jnp.dot(a, b, preferred_element_type=f32)
    return lax.dot_general(a, b, dims, preferred_element_type=f32)


def norm_rows(h):
    wide = h.astype(f32)
    return (wide * lax.rsqrt(jnp.mean(wide * wide, -ONE, keepdims=True) + 1e-6)).astype(bf)


def run(events):
    for event in events:
        event()


def at_step(i, events):
    for step, functions in events.items():
        pl.when(i == step)(functools.partial(run, functions))


def pair(ref, f):
    return ref.at[pl.ds(TWO * f, TWO)]


def wide(tiles):
    return jnp.concatenate(tiles, axis=ONE)


def down_block(tiles):
    last = []
    for q in range(EIGHT):
        tile, row = ROWS + TWELVE * q // ROWS, TWELVE * q % ROWS
        parts = [tiles[tile][row : min(row + TWELVE, ROWS)]]
        if row + TWELVE > ROWS:
            parts.append(tiles[tile + ONE][: row - FOUR])
        last.append(jnp.concatenate(parts, axis=ZERO))
    return jnp.concatenate([wide(tiles[:EIGHT]), wide(tiles[EIGHT:ROWS]), wide(last)], axis=ZERO)


def plan_forward():
    tiles = [max(n for _, n in cols) for cols in (*GU0, DD, DD, *GU1)]
    per_tile = (0.27, 0.36, 0.18, 1.43, 0.72, 0.0, 0.0)
    due = {ZERO: ZERO, ONE: TWO, TWO: SIX, THREE: N_F, FOUR: N_F + TWO, FIVE: 99, SIX: 99}
    length = [3.0] * N_F + [3.8] * (TWO * N_T)
    late = (2.7, 2.7, 2.7, 2.7, 2.7, 1.5, 0.0)
    following = [ZERO] * SEVEN
    arrives = [0.0] * SEVEN
    plan = [[] for _ in range(N_F + TWO * N_T + TWO)]
    now, link = 0.0, 0.0

    def allowed(place, k):
        e = following[k]
        if e > SIX:
            return False
        if k == ZERO:
            return True
        before = following[k - ONE]
        if place == ZERO and k > TWO:
            return False
        return before > FOUR or (before > THREE and link <= now + 1.0) if e == THREE else before > ZERO

    def run_one(place, k):
        nonlocal now, link
        e = following[k]
        now = max(now, arrives[k]) + 0.3
        plan[place].append((k, e))
        link = max(link, now) + per_tile[e] * tiles[k]
        arrives[k] = (link if e < FIVE else now) + late[e]
        following[k] = e + ONE

    for place in range(len(plan)):
        while True:
            ready = [k for k in range(SEVEN) if allowed(place, k) and arrives[k] <= now]
            if ready:
                run_one(place, ready[ZERO])
                continue
            must = [k for k in range(SEVEN) if following[k] < SEVEN and (due[k] <= place or place == len(plan) - ONE)]
            if not must:
                break
            waiting = [k for k in range(SEVEN) if allowed(place, k) and following[k] < SEVEN]
            run_one(place, min(waiting, key=lambda k: arrives[k]))
        if place < len(length):
            now += length[place]
    return plan


def forward_kernel(
    x_hbm, dy_hbm, w_gate, w_up, own_d,
    gu0, d0, gu1, gate0, up0, act0, a0, h1, a1, dact1, d1,
    x, a, big, wt, go, raw, wc, ho, dyt, own,
    ssem, rsem, csem, xsem, wsem, gsem, bsem, rawsem, hsem, asem, dsem, esem,
):
    load_x = pltpu.make_async_copy(x_hbm, x, xsem.at[ZERO])
    load_x.start()

    def own_tile(c, _):
        for layer in range(LAYERS):
            for k, w in enumerate((w_gate, w_up)):
                own[layer, k, c] = w[layer, :, pl.ds(pl.multiple_of(c * L, L), L)]
        return ZERO

    lax.fori_loop(ZERO, C, own_tile, ZERO)
    me = coords()
    barrier(me)

    def stream(k, shard, out, cols):
        g = Gather(me, shard, out, ssem.at[k], rsem.at[k], csem.at[k], cols)
        return g, g.events()

    todo = [(own.at[ZERO], gu0, cols) for cols in GU0] + [(own_d.at[n], d, DD) for n, d in enumerate((d0, d1))] + [(own.at[ONE], gu1, cols) for cols in GU1]
    streams = [stream(k, *one) for k, one in enumerate(todo)]
    plan = [[streams[k][ONE][e] for k, e in place] for place in plan_forward()]

    run(plan[ZERO][:TWO])
    load_x.wait()

    def norm0(t, _):
        rows = pl.ds(pl.multiple_of(t * M, M), M)
        a[rows, :] = norm_rows(x[rows, :])
        return ZERO

    lax.fori_loop(ZERO, N_T, norm0, ZERO)
    keep_a0 = pltpu.make_async_copy(a, a0, xsem.at[ONE])
    keep_a0.start()
    run(plan[ZERO][TWO:])

    def load_w(w, f, slot):
        return pltpu.make_async_copy(w.at[:, pl.ds(TWO * f, TWO)], wt.at[slot], wsem.at[slot])

    def put(f, slot):
        return (
            pltpu.make_async_copy(go.at[slot, ZERO], pair(gate0, f), gsem.at[slot, ZERO]),
            pltpu.make_async_copy(go.at[slot, ONE], pair(up0, f), gsem.at[slot, ONE]),
            pltpu.make_async_copy(pair(big, f), pair(act0, f), bsem.at[slot]),
        )

    def gate_up(f, events, w, finish):
        slot = lax.rem(f, TWO)
        load_w(w, f, slot).wait()

        @pl.when(f + ONE < N_F)
        def _():
            load_w(w, f + ONE, ONE - slot).start()

        finish(f, slot, [wide([wt[slot, k, e].reshape(D, L) for e in (ZERO, ONE)]) for k in (ZERO, ONE)])
        at_step(f, events)
        return ZERO

    def finish0(f, slot, w):
        @pl.when(f >= TWO)
        def _():
            for copy in put(f - TWO, slot):
                copy.wait()

        for t in range(N_T):
            rows = pl.ds(t * M, M)
            gate, up = dot(a[rows, :], w[ZERO]), dot(a[rows, :], w[ONE])
            act = (gate * jax.nn.sigmoid(gate) * up).astype(bf)
            for e in (ZERO, ONE):
                lanes = slice(L * e, L * e + L)
                go[slot, ZERO, e, rows, :] = gate[:, lanes]
                go[slot, ONE, e, rows, :] = up[:, lanes]
                big[TWO * f + e, rows, :] = act[:, lanes]
        for copy in put(f, slot):
            copy.start()

    load_raw = [pltpu.make_async_copy(d, raw, rawsem) for d in (d0, d1)]
    ev = {f: plan[ONE + f] for f in range(N_F)}
    load_w(gu0, ZERO, ZERO).start()
    lax.fori_loop(ZERO, N_F, lambda f, _: gate_up(f, ev, gu0, finish0), ZERO)
    load_raw[ZERO].start()
    for f in (N_F - TWO, N_F - ONE):
        for copy in put(f, f % TWO):
            copy.wait()
    keep_a0.wait()

    def convert():
        def four(g, _):
            blocks = [down_block([raw[c // ELEVEN, c % ELEVEN, g // FOUR, lax.rem(g, FOUR), z] for c in range(C)]) for z in range(FOUR)]
            wc[pl.ds(pl.multiple_of(176 * g, 176), 176), :] = jnp.concatenate(blocks, axis=ZERO)
            return ZERO

        lax.fori_loop(ZERO, ROWS, four, ZERO)

    load_raw[ZERO].wait()
    convert()

    def put_h(t, slot):
        return pltpu.make_async_copy(ho.at[slot], h1.at[pl.ds(pl.multiple_of(t * M, M), M)], hsem.at[slot])

    def load_dy(t, slot):
        return pltpu.make_async_copy(dy_hbm.at[pl.ds(pl.multiple_of(t * M, M), M)], dyt.at[slot], dsem.at[slot])

    def down(t, events):
        slot = lax.rem(t, TWO)

        @pl.when(t >= TWO)
        def _():
            put_h(t - TWO, slot).wait()

        rows = pl.ds(pl.multiple_of(t * M, M), M)
        h = (x[rows, :].astype(f32) + dot(wide([big[c, rows, :] for c in range(C)]), wc[...]).astype(bf).astype(f32)).astype(bf)
        ho[slot] = h
        a[rows, :] = norm_rows(h)
        put_h(t, slot).start()
        at_step(t, events)
        return ZERO

    lax.fori_loop(ZERO, N_T, lambda t, _: down(t, {ZERO: plan[ONE + N_F], ONE: [*plan[TWO + N_F], lambda: load_raw[ONE].start()], TWO: plan[THREE + N_F], THREE: plan[FOUR + N_F]}), ZERO)
    keep_a1 = pltpu.make_async_copy(a, a1, asem)
    keep_a1.start()
    load_dy(ZERO, ZERO).start()
    for t in (N_T - TWO, N_T - ONE):
        put_h(t, t % TWO).wait()
    load_raw[ONE].wait()
    convert()

    def put_dact(t):
        r = pl.ds(pl.multiple_of(t * M, M), M)
        return pltpu.make_async_copy(big.at[:, r], dact1.at[:, r], esem.at[t])

    def dact(t, events):
        slot = lax.rem(t, TWO)
        load_dy(t, slot).wait()

        @pl.when(t + ONE < N_T)
        def _():
            load_dy(t + ONE, ONE - slot).start()

        rows = pl.ds(pl.multiple_of(t * M, M), M)
        for half in (ZERO, ONE):
            v = dot(dyt[slot], wc[FF // TWO * half : FF // TWO * half + FF // TWO, :], NT).astype(bf)
            for c in range(ELEVEN):
                big[ELEVEN * half + c, rows, :] = v[:, L * c : L * c + L]
        put_dact(t).start()
        at_step(t, events)
        return ZERO

    lax.fori_loop(ZERO, N_T, lambda t, _: dact(t, {n: plan[FIVE + N_F + n] for n in range(N_T)}), ZERO)
    run(plan[-ONE])

    for t in range(N_T):
        put_dact(t).wait()
    keep_a1.wait()
    for g, _ in streams:
        g.finish()


def forward(x, dy, w_gate, w_up, own_d):
    sd = jax.ShapeDtypeStruct
    tall, tall32, narrow = sd((C, T, L), bf), sd((C, T, L), f32), sd((T, D), bf)
    blocks = sd((TWO, C, FOUR, FOUR, FOUR, ROWS, L), bf)
    half_blocks = sd((TWO, C // TWO, FOUR, FOUR, FOUR, ROWS, L), bf)
    dma = pltpu.SemaphoreType.DMA
    return pl.pallas_call(
        forward_kernel,
        in_specs=[HBM, HBM, VMEM, VMEM, VMEM],
        out_specs=[HBM] * ELEVEN,
        out_shape=[blocks, half_blocks, blocks, tall32, tall32, tall, narrow, narrow, narrow, tall, half_blocks],
        scratch_shapes=[
            pltpu.VMEM((T, D), bf), pltpu.VMEM((T, D), bf), pltpu.VMEM((C, T, L), bf),
            pltpu.VMEM((TWO, TWO, TWO, FOUR, FOUR, FOUR, ROWS, L), bf), pltpu.VMEM((TWO, TWO, TWO, T, L), f32),
            pltpu.VMEM((TWO, C // TWO, FOUR, FOUR, FOUR, ROWS, L), bf), pltpu.VMEM((FF, D), bf), pltpu.VMEM((TWO, M, D), bf),
            pltpu.VMEM((TWO, M, D), bf), pltpu.VMEM((LAYERS, TWO, C, ROWS, L), bf),
            dma((SEVEN, THREE, 15)), dma((SEVEN, THREE, 15)), dma((SEVEN, THREE)), dma((TWO,)), dma((TWO,)), dma((TWO, TWO)), dma((TWO,)), dma(()), dma((TWO,)), dma(()), dma((TWO,)), dma((FOUR,)),
        ],
        compiler_params=pltpu.CompilerParams(collective_id=ZERO, has_side_effects=True, vmem_limit_bytes=63 * TWO**20),
        name="forward",
    )(x, dy, w_gate, w_up, own_d)[:TEN]


HALF = FF // TWO
PARTS = ((ZERO, FOUR), (FOUR, FOUR), (EIGHT, THREE))
UNITS = TWELVE


class Scatter:
    @staticmethod
    def vw(p, v, w):
        return (slice(None), v, w) if PERM[p][ONE] < PERM[p][TWO] else (slice(None), w, v)

    @staticmethod
    def scratch():
        s = []
        for p, (_, n) in enumerate(PARTS):
            _, *h = Scatter.vw(p, TWO, FOUR)
            s += [
                pltpu.VMEM((TWO, SIX, n, *h, ROWS, L), bf),
                pltpu.VMEM((TWO, FOUR, n, *h, ROWS, L), bf),
                pltpu.VMEM((n, FOUR, FOUR, ROWS, L), f32), pltpu.VMEM((n, FOUR, FOUR, ROWS, L), bf),
                pltpu.VMEM((SIX, n, TWO, ROWS, L), bf), pltpu.VMEM((TWO, n, TWO, ROWS, L), bf),
                pltpu.VMEM((n, FOUR, ROWS, L), f32), pltpu.VMEM((n, FOUR, ROWS, L), bf),
                pltpu.VMEM((THREE, n, ROWS, L), bf),
            ]
        dma = pltpu.SemaphoreType.DMA
        regular = pltpu.SemaphoreType.REGULAR
        return s + [pltpu.VMEM((ROWS, FF // TWO), bf), dma((TWO, THREE, 15)), dma((TWO, THREE, 15)), dma((TWO, THREE, FOUR)), dma(()), regular((THREE, TWO)), regular((THREE, TWO)), regular((THREE, THREE))]

    def __init__(self, me, grads, out, bufs):
        self.me, self.grads, self.out = me, grads, out
        self.b = [bufs[NINE * p : NINE * p + NINE] for p in range(THREE)]
        self.res, self.ssem, self.rsem, self.lsem, self.osem, self.credit1, self.credit2, self.credit3 = bufs[27:]

    def m(self, p, k, d=ZERO):
        return self.me.plus[PERM[p][k]][d]

    def at_unit(self, k):
        self.k, self.slot = k, lax.rem(k, TWO)
        odd = lax.rem(k, TWO)
        self.grad = jnp.where(k < FOUR, ONE + odd, jnp.where(k < SIX, ZERO, jnp.where(k < EIGHT, THREE, k // TWO)))
        self.col0 = C // TWO * jnp.where(k < FOUR, k // TWO, odd)

    def cols(self, p):
        c, n = PARTS[p]
        return pl.ds(self.col0 + c, n)

    def term(self, p, u, half):
        i = [None] * THREE
        a, v, w = PERM[p]
        i[a], i[v], i[w] = u, pl.ds(TWO * half, TWO), slice(None)
        return self.grads.at[(self.grad, self.cols(p), *i)]

    def own(self, p, j):
        u, h = ((ONE, ZERO), (THREE, ONE), (ZERO, ZERO), (ZERO, ONE))[j]
        return pltpu.make_async_copy(self.term(p, self.m(p, ZERO, u), h), self.b[p][ONE].at[self.slot, j], self.lsem.at[self.slot, p, j])

    def cp(self, p, k):
        b, s = self.b[p], self.slot
        if k < SIX:
            ax, d = ZERO, (ONE, THREE, ONE, THREE, ONE, THREE)[k]
            if k < FOUR:
                u, h = ((TWO, ZERO), (TWO, ONE), (ONE, ONE), (THREE, ZERO))[k]
                src = self.term(p, self.m(p, ZERO, u), h)
            else:
                src = b[ONE].at[s, k - FOUR]
            dst = b[ZERO].at[s, k]
        elif k < TWELVE:
            j = k - SIX
            ax, d = ONE, (ONE, THREE, ONE, THREE, ONE, THREE)[j]
            if j < FOUR:
                v, h = ((TWO, ZERO), (TWO, ONE), (ONE, ONE), (THREE, ZERO))[j]
                src = b[THREE].at[self.vw(p, self.m(p, ONE, v), pl.ds(TWO * h, TWO))]
            else:
                src = b[FIVE].at[j - FOUR]
            dst, s = b[FOUR].at[j], ZERO
        else:
            ax, d = TWO, (ONE, THREE, TWO)[k - TWELVE]
            src, dst, s = b[SEVEN].at[:, self.m(p, TWO, d)], b[EIGHT].at[k - TWELVE], ZERO
        return pltpu.make_async_remote_copy(
            src_ref=src, dst_ref=dst, send_sem=self.ssem.at[s, p, k], recv_sem=self.rsem.at[s, p, k],
            device_id=shifted(self.me, PERM[p][ax], d), device_id_type=MESH,
        )

    def give(self, credit, axis, last):
        @pl.when(self.k < last)
        def _():
            for p in range(THREE):
                for j, d in enumerate((THREE, ONE, TWO)[: credit.shape[ONE]]):
                    pl.semaphore_signal(credit.at[p, j], inc=ONE, device_id=shifted(self.me, PERM[p][axis], d), device_id_type=MESH)

    def take(self, credit, first):
        @pl.when(self.k >= first)
        def _():
            for p in range(THREE):
                for j in range(credit.shape[ONE]):
                    pl.semaphore_wait(credit.at[p, j], ONE)

    def begin(self):
        self.take(self.credit1, TWO)
        for k in (ZERO, ONE, TWO, THREE):
            for p in range(THREE):
                self.cp(p, k).start()
        for p in range(THREE):
            for j in range(FOUR):
                self.own(p, j).start()

    def pass_on(self):
        s = self.slot
        for p in range(THREE):
            b = self.b[p]
            for k in (ZERO, ONE):
                self.own(p, k).wait()
                self.cp(p, k).wait_recv()
                for n in range(PARTS[p][ONE]):
                    b[ONE][s, k, n] = (b[ZERO][s, k, n].astype(f32) + b[ONE][s, k, n].astype(f32)).astype(bf)
        for k in (FOUR, FIVE):
            for p in range(THREE):
                self.cp(p, k).start()

    def first_sum(self):
        s = self.slot
        for p in range(THREE):
            b = self.b[p]
            for k in (TWO, THREE, FOUR, FIVE):
                self.cp(p, k).wait_recv()
            for j in (TWO, THREE):
                self.own(p, j).wait()
            for half in (ZERO, ONE):
                own, sums, raw = ((TWO, FOUR, THREE), (THREE, FIVE, TWO))[half]
                _, *ix = self.vw(p, slice(TWO * half, TWO * half + TWO), slice(None))
                for n in range(PARTS[p][ONE]):
                    t = b[ONE][s, own, n].astype(f32) + b[ZERO][s, sums, n].astype(f32) + b[ZERO][s, raw, n].astype(f32)
                    b[TWO][(n, *ix)] = t
                    b[THREE][(n, *ix)] = t.astype(bf)
        for p in range(THREE):
            for k in range(SIX):
                self.cp(p, k).wait_send()
        self.give(self.credit1, ZERO, UNITS - TWO)
        self.take(self.credit2, ONE)
        for k in (SIX, SEVEN, EIGHT, NINE):
            for p in range(THREE):
                self.cp(p, k).start()

    def pass_on2(self):
        for p in range(THREE):
            b = self.b[p]
            for half in (ZERO, ONE):
                self.cp(p, SIX + half).wait_recv()
                v = self.m(p, ONE, (ONE, THREE)[half])
                own = b[TWO][self.vw(p, v, slice(TWO * half, TWO * half + TWO))]
                b[FIVE][half] = (b[FOUR][half].astype(f32) + own).astype(bf)
        for k in (TEN, ELEVEN):
            for p in range(THREE):
                self.cp(p, k).start()

    def second_sum(self):
        for p in range(THREE):
            b, v = self.b[p], self.m(p, ONE)
            for k in (EIGHT, NINE, TEN, ELEVEN):
                self.cp(p, k).wait_recv()
            for half in (ZERO, ONE):
                sums, raw = ((FOUR, THREE), (FIVE, TWO))[half]
                part = slice(TWO * half, TWO * half + TWO)
                t = b[TWO][self.vw(p, v, part)] + b[FOUR][sums].astype(f32) + b[FOUR][raw].astype(f32)
                b[SIX][:, part] = t
                b[SEVEN][:, part] = t.astype(bf)
        for p in range(THREE):
            for k in range(SIX, TWELVE):
                self.cp(p, k).wait_send()
        self.give(self.credit2, ONE, UNITS - ONE)
        self.take(self.credit3, ONE)
        for k in (TWELVE, 13, 14):
            for p in range(THREE):
                self.cp(p, k).start()

    def total(self):
        for p in range(THREE):
            b, w = self.b[p], self.m(p, TWO)
            for k in (TWELVE, 13, 14):
                self.cp(p, k).wait_recv()
            t = b[SIX][:, w]
            for j in range(THREE):
                t = t + b[EIGHT][j].astype(f32)
            c, n = PARTS[p]
            for q in range(n):
                self.res[:, L * (c + q) : L * (c + q) + L] = t[q].astype(bf)
        layer, kind = ONE - self.grad // THREE, lax.rem(self.grad, THREE)
        for m, out in enumerate(self.out):

            @pl.when(kind == m)
            def _():
                pltpu.make_async_copy(self.res, out.at[layer, :, pl.ds(pl.multiple_of(self.col0 * L, L), FF // TWO)], self.osem).start()

        for p in range(THREE):
            for k in (TWELVE, 13, 14):
                self.cp(p, k).wait_send()
        self.give(self.credit3, TWO, UNITS - ONE)
        pltpu.make_async_copy(self.res, self.out[ZERO].at[ZERO, :, pl.ds(ZERO, FF // TWO)], self.osem).wait()

    def tick(self, j, plan):
        def due(steps):
            words = [sum(ONE << (n - 30 * w) for n in steps if n // 30 == w) for w in range(max(plan["total"]) // 30 + ONE)]
            word = functools.reduce(lambda have, w: jnp.where(j >= 30 * w, words[w], have), range(ONE, len(words)), words[ZERO])
            return (lax.shift_right_logical(jnp.int32(word), lax.rem(j, 30)) & ONE) == ONE

        @pl.when(due({n for steps in plan.values() for n in steps}))
        def _():
            for event in (self.total, self.second_sum, self.pass_on2, self.first_sum, self.pass_on, self.begin):
                steps = plan[event.__name__]

                @pl.when(due(steps))
                def _():
                    self.at_unit(sum(jnp.where(j > n, ONE, ZERO) for n in steps))
                    event()


S1, S2, S3, S6, S5, S7, S8, S9, TAIL = ZERO, ELEVEN, 19, 35, 43, 51, 63, 74, 90


def make_plan():
    length = [5.1] * ELEVEN + [2.2] * EIGHT + [1.95] * ROWS + [2.2] * EIGHT + [2.1] * EIGHT + [2.4] * TWELVE + [1.4] * ELEVEN + [1.95] * ROWS
    ready = [SEVEN, SEVEN, S2 + ONE, S2 + ONE, S3 + ONE, S3 + ONE, S5 + ONE, S5 + ONE, S7 + SEVEN, S8 + ONE, S8 + SEVEN, S9 + ONE]
    names = ("begin", "pass_on", "first_sum", "pass_on2", "second_sum", "total")
    sends = (6.1, 3.05, 1.6, 0.8, 1.1, 0.0)
    late = 2.5
    plan = {name: [] for name in names}
    arrives = [[0.0] * SEVEN for _ in range(UNITS)]
    now, link, step = 3.0, 0.0, ZERO

    def may_run(e, k):
        n = len(plan[names[e]])
        if n != k or (plan[names[e]] and plan[names[e]][-ONE] == step):
            return False
        if e == ZERO:
            return step >= ready[k] and (k < TWO or len(plan["first_sum"]) > k - TWO)
        if len(plan[names[e - ONE]]) <= k or plan[names[e - ONE]][k] == step:
            return False
        if e == TWO and len(plan["second_sum"]) < k:
            return False
        return not (e == FOUR and len(plan["total"]) < k)

    while len(plan["total"]) < UNITS:
        ran = False
        for e in (FIVE, FOUR, THREE, TWO, ONE, ZERO):
            k = len(plan[names[e]])
            if k < UNITS and may_run(e, k) and (arrives[k][e] <= now or step >= TAIL):
                if step >= TAIL and arrives[k][e] > now:
                    if ran or any(may_run(o, len(plan[names[o]])) and arrives[len(plan[names[o]])][o] < arrives[k][e] for o in range(SIX) if o != e and len(plan[names[o]]) < UNITS):
                        continue
                    now = arrives[k][e]
                plan[names[e]].append(step)
                ran = True
                now += 0.35
                link = max(link, now) + sends[e]
                if e == ZERO:
                    arrives[k][ONE], arrives[k][TWO] = link - sends[ONE] + late, link + late
                elif e < FIVE:
                    arrives[k][e + ONE] = max(arrives[k][e + ONE], link + late)
        now += length[step] if step < TAIL else 0.05
        step += ONE
    return plan


PLAN = make_plan()
N_STEPS = max(PLAN["total"]) + ONE


def backward_kernel(
    x, dy, gu0, d0, gu1, gate0, up0, act0, a0, h1, a1, dact1,
    dx, by_down, by_gate, by_up, grads, dup1,
    am, dh, r1, r2, r3, stg, tl, ob, gl, ht,
    lsem, r1sem, r2sem, r3sem, amsem, wsem, dasem, tlsem, obsem, glsem, flsem, hsem, dxsem, *bufs,
):
    me = coords()
    barrier(me, sib=False)
    scatter = Scatter(me, grads, (by_down, by_gate, by_up), bufs)

    def rows(t, n=M):
        return pl.ds(pl.multiple_of(t * n, n), n)

    def col(f, n=F):
        return pl.ds(pl.multiple_of(f * n, 128), n)

    load_dh = pltpu.make_async_copy(dy, dh, lsem)
    load_dup = pltpu.make_async_copy(dup1, r1, r1sem)
    load_act = pltpu.make_async_copy(act0, r2, r2sem)

    def load_am(src):
        return pltpu.make_async_copy(src, am, amsem)

    def load_wt(f, slot):
        return [
            pltpu.make_async_copy(gu1.at[k, pl.ds(TWO * f, TWO), pl.ds(TWO * h, TWO)], stg.at[pl.ds(EIGHT * slot + FOUR * k + TWO * h, TWO)], wsem.at[slot, k, h])
            for k in (ZERO, ONE) for h in (ZERO, ONE)
        ]

    def load_dact(f, slot):
        return pltpu.make_async_copy(pair(dact1, f), pair(r1, f), dasem.at[slot])

    def load_r3(src, h):
        return pltpu.make_async_copy(src.at[:, pl.ds(TWO * h, TWO)], r3.at[:, pl.ds(TWO * h, TWO)], r3sem.at[h])

    def flush(grad, half):
        return pltpu.make_async_copy(stg, grads.at[grad, :, pl.ds(TWO * half, TWO)], flsem)

    def put_tl(f, slot):
        return pltpu.make_async_copy(tl.at[slot], pair(dup1, f), tlsem.at[slot])

    def put_ob(grad, f, slot, kinds=(ZERO, ONE)):
        return [pltpu.make_async_copy(ob.at[slot, k], grads.at[grad + k, pl.ds(TWO * f, TWO)], obsem.at[slot, k]) for k in kinds]

    def load_gl(f, e):
        return [pltpu.make_async_copy(src.at[TWO * f + e], gl.at[e, k], glsem.at[e, k]) for k, src in enumerate((gate0, up0))]

    def load_h(src, t):
        return pltpu.make_async_copy(src.at[rows(t)], ht, hsem)

    def put_dx(t):
        return pltpu.make_async_copy(dh.at[rows(t)], dx.at[rows(t)], dxsem.at[t])

    def go(copies):
        for c in copies:
            c.start()

    def done(copies):
        for c in copies:
            c.wait()

    def when(condition, f):
        pl.when(condition)(f)

    def gate_up_grad(slot, tiles, parts=(ZERO, FOUR), kinds=(ZERO, ONE)):
        lo, hi = parts
        v = dot(am[:, F * lo : F * hi], wide(tiles), TN).astype(bf)
        for n, k in enumerate(kinds):
            for e in (ZERO, ONE):
                ob[slot, k, e, lo:hi] = v[:, F * n + L * e : F * n + L * e + L].reshape(hi - lo, FOUR, FOUR, ROWS, L)

    def layer1(f, slot):
        w = []
        for k in (ZERO, ONE):
            halves = [wide([stg[EIGHT * slot + FOUR * k + TWO * h + e].reshape(D // TWO, L) for e in (ZERO, ONE)]) for h in (ZERO, ONE)]
            w.append(jnp.concatenate(halves, axis=ZERO))
        for t in range(N_T):
            r = pl.ds(t * M, M)
            gate, up = dot(am[r, :], w[ZERO]), dot(am[r, :], w[ONE])
            by_act = wide([r1[TWO * f + e, r, :] for e in (ZERO, ONE)]).astype(f32)
            sig = jax.nn.sigmoid(gate)
            silu = gate * sig
            act, by_gate, by_up = silu * up, by_act * up * (sig + silu * (ONE - sig)), by_act * silu
            for e in (ZERO, ONE):
                lanes = slice(L * e, L * e + L)
                r1[TWO * f + e, r, :] = act[:, lanes].astype(bf)
                r2[TWO * f + e, r, :] = by_gate[:, lanes].astype(bf)
                tl[slot, e, r, :] = by_up[:, lanes].astype(bf)
        gate_up_grad(slot, [r2[TWO * f], r2[TWO * f + ONE], tl[slot, ZERO], tl[slot, ONE]])

    def down_grad(s, src, grad):
        half, c = s // FOUR, lax.rem(s, FOUR)
        lhs = wide([src[C // TWO * half + i] for i in range(C // TWO)])
        am[: FF // TWO, :F] = dot(lhs, dh[:, col(c)], TN).astype(bf)
        when(s == FOUR, lambda: flush(grad, ZERO).wait())
        lanes = [slice(L * e, L * e + L) for e in (ZERO, ONE)]

        def four(g, _):
            v = am[pl.ds(pl.multiple_of(176 * g, 176), 176), :F]
            x, y = g // FOUR, lax.rem(g, FOUR)
            for z in range(FOUR):
                for e in (ZERO, ONE):
                    stg[TWO * c + e, x, y, z] = v[44 * z : 44 * z + ROWS, lanes[e]]
                    stg[EIGHT + TWO * c + e, x, y, z] = v[44 * z + ROWS : 44 * z + 32, lanes[e]]
            for z in range(FOUR):
                one, two = (v[44 * z + 32 : 44 * z + 44, lanes[e]] for e in (ZERO, ONE))
                for k, part in enumerate((one[:EIGHT], jnp.concatenate([one[EIGHT:], two[:FOUR]], axis=ZERO), two[FOUR:])):
                    n = THREE * c + k
                    stg[ROWS + n // TWO, x, y, z, pl.ds(pl.multiple_of(EIGHT * lax.rem(n, TWO), EIGHT), EIGHT)] = part

            return ZERO

        lax.fori_loop(ZERO, EIGHT, four, ZERO)
        for h in (ZERO, ONE):
            when(s == FOUR * h + THREE, lambda: flush(grad, h).start())

    def silu_back(f, e, t):
        for q in range(t * M, t * M + M, L):
            r = slice(q, q + L)
            gate, up, by_act = gl[e, ZERO, r, :], gl[e, ONE, r, :], r1[TWO * f + e, r, :].astype(f32)
            sig = jax.nn.sigmoid(gate)
            silu = gate * sig
            r2[TWO * f + e, r, :] = (by_act * up * (sig + silu * (ONE - sig))).astype(bf)
            r1[TWO * f + e, r, :] = (by_act * silu).astype(bf)

    def by_input(src, n, t):
        w = wide([r3[c, pl.ds(TWO * n, TWO)].reshape(D // TWO, L) for c in range(C)])
        return dot(wide([src[c, rows(t), :] for c in range(C)]), w, NT).astype(bf)

    def norm_back(t):
        h = ht[...].astype(f32)
        by_a = am[rows(t), :].astype(f32)
        scale = lax.rsqrt(jnp.mean(h * h, -ONE, keepdims=True) + 1e-6)
        by_wide = scale * by_a - h * (scale * scale * scale * jnp.mean(h * by_a, -ONE, keepdims=True))
        dh[rows(t), :] = (dh[rows(t), :].astype(f32) + by_wide.astype(bf).astype(f32)).astype(bf)

    def down_rows(half):
        def four(g, _):
            blocks = [down_block([r3[c, TWO * half + g // FOUR, lax.rem(g, FOUR), z] for c in range(C)]) for z in range(FOUR)]
            am[pl.ds(pl.multiple_of(176 * g, 176), 176), :] = jnp.concatenate(blocks, axis=ZERO)
            return ZERO

        lax.fori_loop(ZERO, EIGHT, four, ZERO)

    def step(j, _):
        def within(a, b):
            return (j >= a) & (j < b)

        in1, in2, in3 = j < S2, within(S2, S3), within(S3, S6)
        in6, in5, in7, in8, in9 = within(S6, S5), within(S5, S7), within(S7, S8), within(S8, S9), within(S9, TAIL)

        def input_pre(s, w, src):
            when(s == ZERO, lambda: load_r3(w.at[ZERO], ZERO).wait())

            @pl.when(s == FOUR)
            def _():
                load_r3(w.at[ZERO], ONE).wait()
                load_r3(w.at[ONE], ZERO).start()

            @pl.when(s == EIGHT)
            def _():
                load_r3(w.at[ONE], ZERO).wait()
                load_r3(w.at[ONE], ONE).start()

            when(s == ELEVEN, lambda: load_h(src, ZERO).start())
            when(s == TWELVE, lambda: load_r3(w.at[ONE], ONE).wait())

        @pl.when(j < S6)
        def _():
            @pl.when(in1)
            def _():
                f = j - S1
                slot = lax.rem(f, TWO)

                @pl.when(f >= TWO)
                def _():
                    done(put_ob(ONE, f - TWO, slot))
                    put_tl(f - TWO, slot).wait()

                done(load_wt(f, slot))
                load_dact(f, slot).wait()

                @pl.when(f + ONE < N_F)
                def _():
                    go(load_wt(f + ONE, ONE - slot))
                    load_dact(f + ONE, ONE - slot).start()

                when(f == TWO, lambda: go([load_r3(gu1.at[ZERO], h) for h in (ZERO, ONE)]))

            @pl.when(in2)
            def _():
                @pl.when(j == S2)
                def _():
                    done(put_ob(ONE, N_F - TWO, ONE))
                    put_tl(N_F - TWO, ONE).wait()
                    load_dh.wait()

                @pl.when(j == S2 + ONE)
                def _():
                    done(put_ob(ONE, N_F - ONE, ZERO))
                    put_tl(N_F - ONE, ZERO).wait()

            @pl.when(in3)
            def _():
                s = j - S3
                input_pre(s, gu1, h1)
                when(s == ZERO, lambda: load_dup.start())
                when(s == ONE, lambda: flush(ZERO, ONE).wait())

                @pl.when(s == EIGHT)
                def _():
                    load_dup.wait()
                    load_act.start()

                when(s == TWELVE, lambda: load_r3(d0, ZERO).start())

        @pl.when((j >= S6) & (j < TAIL))
        def _():
            @pl.when(in9)
            def _():
                s = j - S9
                input_pre(s, gu0, x)
                when(s == ZERO, lambda: done(put_ob(FOUR, N_F - TWO, ONE, (ONE,))))
                when(s == ONE, lambda: done(put_ob(FOUR, N_F - ONE, ZERO, (ONE,))))

            @pl.when(j == S6)
            def _():
                load_act.wait()
                load_r3(d0, ONE).start()

            @pl.when(in5)
            def _():
                s = j - S5

                @pl.when(s == ZERO)
                def _():
                    load_r3(d0, ZERO).wait()
                    go(load_gl(ZERO, ZERO) + load_gl(ZERO, ONE))

                @pl.when(s == ONE)
                def _():
                    flush(THREE, ONE).wait()
                    load_r3(gu0.at[ZERO], ZERO).start()

                when(s == FOUR, lambda: load_r3(d0, ONE).wait())
                when(s == FIVE, lambda: load_r3(gu0.at[ZERO], ONE).start())

            @pl.when(in7)
            def _():
                when(j == S7 + ONE, lambda: load_am(a0).wait())
                i = j - S7
                when((i >= THREE) & (i != EIGHT), lambda: done(put_ob(FOUR, i - THREE, lax.rem(i - THREE, TWO), (ZERO,))))
                when(i == SEVEN, lambda: done(put_ob(FOUR, FIVE, ONE, (ZERO,))))

            @pl.when(in8)
            def _():
                f = j - S8
                when(f == ZERO, lambda: done(put_ob(FOUR, N_F - TWO, ONE, (ZERO,))))
                when(f == ONE, lambda: done(put_ob(FOUR, N_F - ONE, ZERO, (ZERO,))))
                when(f >= TWO, lambda: done(put_ob(FOUR, f - TWO, lax.rem(f, TWO), (ONE,))))

        scatter.tick(j, PLAN)

        @pl.when(j < S3)
        def _():
            @pl.when(in1)
            def _():
                f = j - S1
                slot = lax.rem(f, TWO)
                layer1(f, slot)
                go(put_ob(ONE, f, slot))
                put_tl(f, slot).start()

            when(in2, lambda: down_grad(j - S2, r1, ZERO))

        @pl.when(in3 | in9)
        def _():
            s = jnp.where(in3, j - S3, j - S9)
            n, t = lax.rem(s, EIGHT) // FOUR, lax.rem(s, FOUR)
            here = (rows(t), col(n, D // TWO))

            def more():
                am[here] = (am[here].astype(f32) + by_input(r1, n, t).astype(f32)).astype(bf)

            @pl.when(s < EIGHT)
            def _():
                am[here] = by_input(r2, n, t)

            when((s >= EIGHT) & (s < 13), more)

            @pl.when(s >= 13)
            def _():
                load_h(h1, t - ONE).wait()
                norm_back(t - ONE)
                more()
                when(in3, lambda: load_h(h1, t).start())
                when(in9, lambda: load_h(x, t).start())
                when(in9, lambda: put_dx(t - ONE).start())

            @pl.when(s == 15)
            def _():
                load_h(h1, THREE).wait()
                norm_back(THREE)
                when(in9, lambda: put_dx(THREE).start())

        @pl.when((j >= S6) & (j < S9))
        def _():
            when(in6, lambda: down_grad(j - S6, r2, THREE))

            @pl.when(in5)
            def _():
                s = j - S5
                half, t = s // FOUR, lax.rem(s, FOUR)
                when(t == ZERO, lambda: down_rows(half))
                v = dot(dh[rows(t), :], am[: FF // TWO, :], NT).astype(bf)
                for c in range(C // TWO):
                    r1[C // TWO * half + c, rows(t), :] = v[:, L * c : L * c + L]
                when(s == SEVEN, lambda: load_am(a0).start())

            @pl.when(in7)
            def _():
                i = j - S7
                before = i - ONE
                slot = lax.rem(i + ONE, TWO)
                tiles = lambda: [r2[TWO * before], r2[TWO * before + ONE]]

                @pl.when(i == ZERO)
                def _():
                    for e in (ZERO, ONE):
                        done(load_gl(ZERO, e))
                        for t in range(FOUR):
                            silu_back(ZERO, e, t)
                        go(load_gl(ONE, e))

                @pl.when((i > ZERO) & (i < N_F))
                def _():
                    for e in (ZERO, ONE):
                        done(load_gl(i, e))
                        for t in (ZERO, ONE):
                            gate_up_grad(slot, tiles(), (TWO * e + t, TWO * e + t + ONE), (ZERO,))
                            silu_back(i, e, TWO * t)
                            silu_back(i, e, TWO * t + ONE)
                        when(i + ONE < N_F, lambda: go(load_gl(i + ONE, e)))

                when(i == N_F, lambda: gate_up_grad(slot, tiles(), (ZERO, FOUR), (ZERO,)))
                when(i > ZERO, lambda: go(put_ob(FOUR, before, slot, (ZERO,))))

            @pl.when(in8)
            def _():
                f = j - S8
                slot = lax.rem(f, TWO)
                gate_up_grad(slot, [r1[TWO * f], r1[TWO * f + ONE]], (ZERO, FOUR), (ONE,))
                go(put_ob(FOUR, f, slot, (ONE,)))

        return ZERO

    load_am(a1).start()
    go(load_wt(ZERO, ZERO))
    load_dact(ZERO, ZERO).start()
    load_dh.start()
    load_am(a1).wait()
    lax.fori_loop(ZERO, N_STEPS, step, ZERO)
    done([put_dx(t) for t in range(FOUR)])


def backward(x, dy, gu0, d0, *args):
    sd = jax.ShapeDtypeStruct
    dma = pltpu.SemaphoreType.DMA
    return pl.pallas_call(
        backward_kernel,
        in_specs=[HBM] * TWELVE,
        out_specs=[HBM] * SIX,
        out_shape=[sd((T, D), bf), *[sd((LAYERS, ROWS, FF), bf)] * THREE, sd((SIX, C, FOUR, FOUR, FOUR, ROWS, L), bf), sd((C, T, L), bf)],
        scratch_shapes=[
            pltpu.VMEM((T, D), bf), pltpu.VMEM((T, D), bf), pltpu.VMEM((C, T, L), bf), pltpu.VMEM((C, T, L), bf),
            pltpu.VMEM((C, FOUR, FOUR, FOUR, ROWS, L), bf), pltpu.VMEM((C, TWO, FOUR, FOUR, ROWS, L), bf), pltpu.VMEM((TWO, TWO, T, L), bf),
            pltpu.VMEM((TWO, TWO, TWO, FOUR, FOUR, FOUR, ROWS, L), bf), pltpu.VMEM((TWO, TWO, T, L), f32), pltpu.VMEM((M, D), bf),
            dma(()), dma(()), dma(()), dma((TWO,)), dma(()), dma((TWO, TWO, TWO)), dma((TWO,)), dma((TWO,)), dma((TWO, TWO)), dma((TWO, TWO)), dma(()), dma(()), dma((FOUR,)),
            *Scatter.scratch(),
        ],
        compiler_params=pltpu.CompilerParams(collective_id=ONE, has_side_effects=True, vmem_limit_bytes=63 * TWO**20 + 900 * 1024),
        name="backward",
    )(x, dy, gu0, d0.reshape(C, FOUR, FOUR, FOUR, ROWS, L), *args)[:FOUR]


def pack_down(t):
    first = t[:, :32].reshape(-ONE, TWO, ROWS, EIGHT, L).transpose(ZERO, ONE, THREE, TWO, FOUR).reshape(-ONE, ROWS, ROWS, L)
    last = t[:, 32:].reshape(-ONE, TWELVE, EIGHT, L).transpose(ZERO, TWO, ONE, THREE).reshape(-ONE, SIX, ROWS, L)
    return jnp.concatenate([first, last], axis=ONE).reshape(-ONE, TWO, C // TWO, ROWS, L)


def unpack_down(t):
    last = t[:, :, TWO * D :].reshape(-ONE, ROWS, SIX, L).transpose(ZERO, TWO, ONE, THREE).reshape(-ONE, EIGHT, TWELVE, L).transpose(ZERO, TWO, ONE, THREE).reshape(-ONE, TWELVE, D)
    return jnp.concatenate([t[:, :, :D], t[:, :, D : TWO * D], last], axis=ONE)


def solution(mesh):
    def device(x, dy, w_gate, w_up, w_down):
        x, dy = x[ZERO], dy[ZERO]
        own_d = pack_down(w_down)
        gu0, d0, gu1, *rest = forward(x, dy, w_gate, w_up, own_d)
        by_x, by_down, by_gate, by_up = backward(x, dy, gu0, d0, gu1, *rest)
        return by_x[None], by_gate, by_up, unpack_down(by_down)

    return jax.shard_map(
        device,
        mesh=mesh,
        in_specs=(P(("rep", "dp")), P(("rep", "dp")), *(P(None, "dp"),) * THREE),
        out_specs=(P(("rep", "dp")), *(P("rep", "dp"),) * THREE),
        check_vma=False,
    )
```
